8 devices in a mesh: dp: 2 (over z, y), cp: 4 (over x, core).
Axes of the slice: x: 2, y: 2, z: 1, core: 2. Of those that a mesh axis runs over, the one named last changes fastest.
Arguments:
- latent: bfloat16 [16, 4, 128, 512], P(('dp', 'cp')), parts along dimension 0
- conv_w: bfloat16 [4, 3, 3, 3, 512, 512], replicated
- conv_b: float32 [4, 512], replicated
- norm_in_scale: float32 [2, 512], replicated
- norm_in_shift: float32 [2, 512], replicated
- norm_mid_scale: float32 [2, 16, 512], P(None, ('dp', 'cp')), parts along dimension 1
- norm_mid_shift: float32 [2, 16, 512], P(None, ('dp', 'cp')), parts along dimension 1
Outputs:
- output: bfloat16 [16, 4, 128, 512], P(('dp', 'cp')), parts along dimension 0
There are 2 independent parts. The reference program is written for one: setup_inputs(seed, part) draws one part's arguments, and reference() takes and returns one part's arrays. A program takes and returns all parts, laid end to end along the dimension named above; an argument that names none is the same for every part.
All inputs are finite; a program needn't handle non-finite values.
Results may differ from the reference program's by a relative error of at most 0.0134452.
Values are sent between devices in bfloat16 or wider.
A program may use at most 1 GiB of HBM per device.

```python
import jax
import jax.numpy as jnp
from jax import lax

FRAMES = 8
HEIGHT = 4
WIDTH = 128
CHANNELS = 512
GROUPS = 32
EPSILON = 1e-6


def setup_inputs(seed: int = 0, part: int = 0) -> dict:
    base_key = jax.random.key(seed)
    shared_keys = jax.random.split(base_key, 4)
    part_keys = jax.random.split(jax.random.fold_in(base_key, part), 8)
    frame_pos = (2.0 * jnp.arange(FRAMES, dtype=jnp.float32) - (FRAMES - 1)) / FRAMES
    gain_slope = 0.6 * jax.random.uniform(part_keys[0], (), jnp.float32, -1.0, 1.0)
    log_gain = gain_slope * frame_pos + 0.15 * jax.random.normal(part_keys[1], (FRAMES,), jnp.float32)
    chan_trend = jax.random.normal(part_keys[2], (CHANNELS,), jnp.float32) + jnp.repeat(jax.random.normal(part_keys[3], (GROUPS,), jnp.float32), CHANNELS // GROUPS)
    frame_offset = 0.7 * chan_trend[None, :] * frame_pos[:, None] + 0.2 * jax.random.normal(part_keys[4], (FRAMES, CHANNELS), jnp.float32)
    base_noise = jax.random.normal(part_keys[5], (FRAMES, HEIGHT, WIDTH, CHANNELS), jnp.float32)
    latent = (base_noise * jnp.exp(log_gain)[:, None, None, None] + frame_offset[:, None, None, :]).astype(jnp.bfloat16)
    conv_scale = (27 * CHANNELS) ** -0.5
    conv_w = (jax.random.normal(shared_keys[0], (4, 3, 3, 3, CHANNELS, CHANNELS), jnp.float32) * conv_scale).astype(jnp.bfloat16)
    conv_b = 0.3 * jax.random.normal(shared_keys[1], (4, CHANNELS), jnp.float32)
    norm_in_scale = 1.0 + 0.3 * jax.random.normal(shared_keys[2], (2, CHANNELS), jnp.float32)
    norm_in_shift = 0.4 * jax.random.normal(shared_keys[3], (2, CHANNELS), jnp.float32)
    norm_mid_scale = 1.0 + 0.3 * jax.random.normal(part_keys[6], (2, FRAMES, CHANNELS), jnp.float32)
    norm_mid_shift = 0.4 * jax.random.normal(part_keys[7], (2, FRAMES, CHANNELS), jnp.float32)
    return {"latent": latent, "conv_w": conv_w, "conv_b": conv_b, "norm_in_scale": norm_in_scale, "norm_in_shift": norm_in_shift, "norm_mid_scale": norm_mid_scale, "norm_mid_shift": norm_mid_shift}


def group_norm_silu(x_frames, norm_scale, norm_shift):
    per_group = CHANNELS // GROUPS
    norm_count = FRAMES * HEIGHT * WIDTH * per_group
    x_wide = x_frames.astype(jnp.float32)
    sum_one = jnp.sum(x_wide, axis=(0, 1, 2))
    sum_two = jnp.sum(jnp.square(x_wide), axis=(0, 1, 2))
    grp_mean = jnp.sum(sum_one.reshape(GROUPS, per_group), axis=1) / norm_count
    grp_var = jnp.sum(sum_two.reshape(GROUPS, per_group), axis=1) / norm_count - grp_mean * grp_mean
    grp_rstd = lax.rsqrt(grp_var + EPSILON)
    chan_mean = jnp.repeat(grp_mean, per_group)
    chan_rstd = jnp.repeat(grp_rstd, per_group)
    normed = ((x_wide - chan_mean) * (chan_rstd * norm_scale) + norm_shift).astype(jnp.bfloat16)
    return jax.nn.silu(normed.astype(jnp.float32)).astype(jnp.bfloat16)


def causal_conv(act_in, kernel, conv_bias):
    frame_zero = act_in[:1]
    padded = jnp.concatenate([frame_zero, frame_zero, act_in], axis=0)
    conv_out = lax.conv_general_dilated(padded[None].astype(jnp.float32), kernel.astype(jnp.float32), (1, 1, 1), ((0, 0), (1, 1), (1, 1)), dimension_numbers=("NDHWC", "DHWIO", "NDHWC"))[0]
    return (conv_out + conv_bias).astype(jnp.bfloat16)


def reference(latent, conv_w, conv_b, norm_in_scale, norm_in_shift, norm_mid_scale, norm_mid_shift):
    residual = latent
    for block_idx in range(2):
        act_in = group_norm_silu(residual, norm_in_scale[block_idx], norm_in_shift[block_idx])
        hidden = causal_conv(act_in, conv_w[2 * block_idx], conv_b[2 * block_idx])
        act_mid = group_norm_silu(hidden, norm_mid_scale[block_idx][:, None, None, :], norm_mid_shift[block_idx][:, None, None, :])
        hidden = causal_conv(act_mid, conv_w[2 * block_idx + 1], conv_b[2 * block_idx + 1])
        residual = (residual.astype(jnp.float32) + hidden.astype(jnp.float32)).astype(jnp.bfloat16)
    return residual
```

```python
import functools

import jax
import jax.numpy as jnp
from jax import lax
from jax.experimental import pallas as pl
from jax.experimental.pallas import tpu as pltpu
from jax.sharding import PartitionSpec as P

NUM_GROUPS = 32
EPSILON = 1e-6
EXPLICIT = False
MESH = pl.DeviceIdType.MESH
F32 = jnp.float32
BF16 = jnp.bfloat16

N_CONV = 4
N_FR = 2
N_ROW = 4
N_COL = 128
N_CH = 512
TILE = 16
N_TILE = N_COL // TILE
PAD_COL = N_COL + 2 * TILE
HALF = 256


def kernel(
    cp_size,
    x_hbm, w_hbm, bias_ref, in_scale, in_shift, mid_scale, mid_shift,
    out_hbm,
    x_in, raw, halo, act, wts, part, tx, rx, gains, shifts, h_scale, h_shift, mean_ref, rstd_ref, tmp,
    x_sem, w_sem, st_send, st_recv, h_send, h_recv, p_send, p_recv, o_sem,
    *extra,
):
    if EXPLICIT:
        pl.run_scoped(
            functools.partial(
                body, cp_size, x_hbm, w_hbm, bias_ref, in_scale, in_shift, mid_scale, mid_shift, out_hbm,
                x_in, raw, halo, act, wts, part, tx, rx, gains, shifts, h_scale, h_shift, mean_ref, rstd_ref, tmp,
                x_sem, w_sem, st_send, st_recv, h_send, h_recv, p_send, p_recv, o_sem,
            ),
            *[pltpu.ACC(m)((N_COL, HALF), F32) for m in range(2) for _ in range(N_FR * N_ROW)],
        )
    else:
        body(
            cp_size, x_hbm, w_hbm, bias_ref, in_scale, in_shift, mid_scale, mid_shift, out_hbm,
            x_in, raw, halo, act, wts, part, tx, rx, gains, shifts, h_scale, h_shift, mean_ref, rstd_ref, tmp,
            x_sem, w_sem, st_send, st_recv, h_send, h_recv, p_send, p_recv, o_sem, *extra,
        )


def body(
    cp_size, x_hbm, w_hbm, bias_ref, in_scale, in_shift, mid_scale, mid_shift, out_hbm,
    x_in, raw, halo, act, wts, part, tx, rx, gains, shifts, h_scale, h_shift, mean_ref, rstd_ref, tmp,
    x_sem, w_sem, st_send, st_recv, h_send, h_recv, p_send, p_recv, o_sem,
    *accs,
):
    cp = lax.axis_index("cp")
    count = float(N_FR * cp_size * N_ROW * N_COL * (N_CH // NUM_GROUPS))
    first, last = cp == 0, cp == cp_size - 1
    peers = [lax.rem(cp + d, cp_size) for d in range(1, cp_size)]
    right = lax.rem(cp + 1, cp_size)

    def acc_of(m, t, p):
        return accs[(m * N_FR + t) * N_ROW + p]

    def mm_push(slot, k, dp, dq, kt, m, reg):
        off = ((dp + 1) * 3 + dq + 1) * N_CH + kt * HALF
        w = wts[slot, k, off : off + HALF, m * HALF : (m + 1) * HALF]
        pltpu.matmul_push_rhs(w, staging_register=reg, mxu_index=m)

    def mm_step(slot, t, k, dp, dq, kt, rows, reg):
        rows = [p for p in rows if 0 <= p + dp < N_ROW]
        if EXPLICIT:
            for m in range(2):
                mm_push(slot, k, dp, dq, kt, m, reg)
        for i, p in enumerate(rows):
            lhs = act[t + k, p + dp, TILE * (1 + dq) : TILE * (1 + dq) + N_COL, kt * HALF : (kt + 1) * HALF]
            for m in range(2):
                if EXPLICIT:
                    pltpu.matmul_acc_lhs(acc_of(m, t, p), lhs, load_staged_rhs=reg if i == 0 else None)
                else:
                    off = ((dp + 1) * 3 + dq + 1) * N_CH + kt * HALF
                    w = wts[slot, k, off : off + HALF, m * HALF : (m + 1) * HALF]
                    accs[0][t, p, m] += jnp.dot(lhs, w, preferred_element_type=F32)

    def pop(m, t, p):
        if EXPLICIT:
            return pltpu.matmul_pop(acc_of(m, t, p))
        val = accs[0][t, p, m]
        accs[0][t, p, m] = jnp.zeros((N_COL, HALF), F32)
        return val

    def steps_of(t, k, kts=(0, 1), rows=range(N_ROW)):
        return [(t, k, dp, dq, kt, tuple(rows)) for kt in kts for dp in (0, -1, 1) for dq in (0, -1, 1)]

    def run(slot, steps, thunks=(), upto=1.0):
        done, span = 0, max(1, int(len(steps) * upto))
        for i, (t, k, dp, dq, kt, rows) in enumerate(steps):
            mm_step(slot, t, k, dp, dq, kt, rows, i % 2)
            want = min(len(thunks), -(-len(thunks) * (i + 1) // span))
            for thunk in thunks[done:want]:
                thunk()
            done = want

    def add_moments(val, half):
        cut = slice(half * HALF, (half + 1) * HALF)
        rows = val.reshape(N_COL // 8, 8, HALF)
        part[0, :, cut] += jnp.sum(rows, axis=0)
        part[1, :, cut] += jnp.sum(rows * rows, axis=0)

    def norm(read, c, f, p, half):
        cut = slice(half * HALF, (half + 1) * HALF)
        gain = rstd_ref[0:1, cut] * gains[c, f : f + 1, cut]
        val = (read(p, cut).astype(F32) - mean_ref[0:1, cut]) * gain + shifts[c, f : f + 1, cut]
        val = 0.5 * val.astype(BF16).astype(F32)
        val = val + val * jnp.tanh(val)
        act[f, p, TILE : TILE + N_COL, cut] = val.astype(BF16)
        row = lax.broadcasted_iota(jnp.int32, (TILE, HALF), 0)
        low = jnp.where(row == 0, 0.0, pltpu.roll(val[N_COL - TILE :], 1, 0))
        act[f, p, 0:TILE, cut] = low.astype(BF16)
        high = jnp.where(row == TILE - 1, 0.0, pltpu.roll(val[:TILE], TILE - 1, 0))
        act[f, p, TILE + N_COL :, cut] = high.astype(BF16)

    def epilogue(c, par, t, p, m):
        cut = slice(m * HALF, (m + 1) * HALF)
        flag = par.astype(F32)
        conv = (pop(m, t, p) + bias_ref[pl.ds(c, 1), cut]).astype(BF16).astype(F32)
        val = (raw[0, t, p, :, cut].astype(F32) * flag + conv).astype(BF16)
        raw[1 - par, t, p, :, cut] = val
        add_moments(val.astype(F32), m)

    def finish_moments(slot):
        for i in range(2):
            total = jnp.sum(part[i], axis=0, keepdims=True)
            for j in range(4):
                tx[slot, 4 * i + j : 4 * i + j + 1, :] = total[:, j * 128 : (j + 1) * 128]
        part[...] = jnp.zeros_like(part)

    def statistics(slot):
        total = tx[slot]
        for d in range(cp_size - 1):
            total = total + rx[slot, d]
        lane = lax.broadcasted_iota(jnp.int32, total.shape, 1)
        for shift in (1, 2, 4, 8):
            total = total + jnp.where(
                (lane & shift) == 0, pltpu.roll(total, 128 - shift, 1), pltpu.roll(total, shift, 1)
            )
        mean = total[0:4] / count
        var = total[4:8] / count - mean * mean
        rstd = lax.rsqrt(var + EPSILON)
        for j in range(4):
            mean_ref[0:1, j * 128 : (j + 1) * 128] = mean[j : j + 1]
            rstd_ref[0:1, j * 128 : (j + 1) * 128] = rstd[j : j + 1]

    def w_copy(c, k):
        slot = lax.rem(c, 2)
        return pltpu.make_async_copy(w_hbm.at[c, k], wts.at[slot, k], w_sem.at[slot, k])

    def st_copy(slot, d):
        return pltpu.make_async_remote_copy(
            src_ref=tx.at[slot], dst_ref=rx.at[slot, d], send_sem=st_send.at[slot, d], recv_sem=st_recv.at[slot, d],
            device_id={"cp": peers[d]}, device_id_type=MESH,
        )

    def halo_copy(par, hs, t):
        return pltpu.make_async_remote_copy(
            src_ref=raw.at[par, t], dst_ref=halo.at[hs, t], send_sem=h_send.at[t], recv_sem=h_recv.at[hs, t],
            device_id={"cp": right}, device_id_type=MESH,
        )

    def own_copy(par, hs, t):
        return pltpu.make_async_copy(raw.at[par, 0], halo.at[hs, t], h_recv.at[hs, t])

    def param_copy(i):
        src, dst = ((mid_scale, h_scale), (mid_shift, h_shift))[i]
        return pltpu.make_async_remote_copy(
            src_ref=src, dst_ref=dst, send_sem=p_send.at[i], recv_sem=p_recv.at[i],
            device_id={"cp": right}, device_id_type=MESH,
        )

    def send_halo(par, hs, t):
        @pl.when(jnp.logical_not(last))
        def _():
            halo_copy(par, hs, t).start()

        if t == 0:

            @pl.when(first)
            def _():
                own_copy(par, hs, 0).start()
                own_copy(par, hs, 1).start()

    barrier = pltpu.get_barrier_semaphore()
    for peer in peers:
        pl.semaphore_signal(barrier, inc=1, device_id={"cp": peer}, device_id_type=MESH)
    x_copies = [pltpu.make_async_copy(x_hbm.at[t], x_in.at[t], x_sem.at[t]) for t in range(N_FR)]
    for t in (1, 0):
        x_copies[t].start()
    for k in (2, 1, 0):
        w_copy(0, k).start()

    part[...] = jnp.zeros_like(part)
    if EXPLICIT:
        for acc in accs:
            pltpu.matmul_pop(acc)
    else:
        accs[0][...] = jnp.zeros_like(accs[0])
    for b in range(2):
        for f in range(4):
            gains[2 * b, f : f + 1, :] = in_scale[b : b + 1, :]
            shifts[2 * b, f : f + 1, :] = in_shift[b : b + 1, :]
        gains[2 * b + 1, 2:4, :] = mid_scale[b]
        shifts[2 * b + 1, 2:4, :] = mid_shift[b]
    for t in (1, 0):
        x_copies[t].wait()
        for p in range(N_ROW):
            val = x_in[t, p].astype(F32)
            for half in range(2):
                add_moments(val[:, half * HALF : (half + 1) * HALF], half)
    finish_moments(0)
    pl.semaphore_wait(barrier, cp_size - 1)
    for d in range(cp_size - 1):
        st_copy(0, d).start()

    for t in (1, 0):
        for p in range(N_ROW):
            val = x_in[t, p].astype(F32)
            for j in range(4):
                tmp[p % 2, j] = val[:, j * 128 : (j + 1) * 128]
            for j in range(4):
                for v in range(N_TILE):
                    raw[0, t, p, v * TILE : (v + 1) * TILE, j * 128 : (j + 1) * 128] = tmp[
                        p % 2, j, pl.ds(v, TILE, stride=N_TILE), :
                    ].astype(BF16)
        if t == 1:

            @pl.when(jnp.logical_not(last))
            def _():
                for i in range(2):
                    param_copy(i).start()

        send_halo(0, 0, t)

    def conv(c, carry):
        par = lax.rem(c, 2)
        nxt = 1 - par

        @pl.when(c < N_CONV - 1)
        def _():
            for k in (2, 1, 0):
                w_copy(c + 1, k).start()

        for d in range(cp_size - 1):
            st_copy(par, d).wait()
        statistics(par)

        def own(t):
            return lambda p, cut: raw[par, t, p, :, cut]

        def received(t):
            return lambda p, cut: halo[par, t, p, :, cut]

        def norms(read, f, halves=(0, 1)):
            return [functools.partial(norm, read, c, f, p, h) for h in halves for p in range(N_ROW)]

        def epilogues(t, rows):
            return [functools.partial(epilogue, c, par, t, p, m) for p in rows for m in range(2)]

        for thunk in norms(own(1), 3, (0,)):
            thunk()
        w_copy(c, 2).wait()
        run(par, steps_of(1, 2, (0,)), norms(own(1), 3, (1,)), 0.9)
        run(par, steps_of(1, 2, (1,)), norms(own(0), 2))
        w_copy(c, 1).wait()

        @pl.when(c == 0)
        def _():
            @pl.when(jnp.logical_not(first))
            def _():
                for i in range(2):
                    param_copy(i).wait_recv()
                for b in range(2):
                    gains[2 * b + 1, 0:2, :] = h_scale[b]
                    shifts[2 * b + 1, 0:2, :] = h_shift[b]

            @pl.when(first)
            def _():
                for b in range(2):
                    for f in range(2):
                        gains[2 * b + 1, f : f + 1, :] = mid_scale[b, 0:1]
                        shifts[2 * b + 1, f : f + 1, :] = mid_shift[b, 0:1]

            @pl.when(jnp.logical_not(last))
            def _():
                for i in range(2):
                    param_copy(i).wait_send()

        own_copy(par, par, 1).wait()
        run(par, steps_of(1, 1), norms(received(1), 1))
        w_copy(c, 0).wait()
        run(par, steps_of(1, 0))
        steps = steps_of(0, 2)
        run(par, steps[:6], epilogues(1, range(N_ROW)))

        @pl.when(jnp.logical_not(last))
        def _():
            halo_copy(par, par, 1).wait_send()
            halo_copy(par, par, 0).wait_send()

        @pl.when(c < N_CONV - 1)
        def _():
            send_halo(nxt, nxt, 1)

        run(par, steps[6:])
        own_copy(par, par, 0).wait()
        run(par, steps_of(0, 1), norms(received(0), 0))
        run(par, steps_of(0, 0, rows=(0, 1)))
        run(par, steps_of(0, 0, rows=(2, 3)), epilogues(0, (0, 1)), 0.8)
        for thunk in epilogues(0, (2, 3)):
            thunk()
        finish_moments(nxt)

        @pl.when(c < N_CONV - 1)
        def _():
            for d in range(cp_size - 1):
                st_copy(nxt, d).start()
            send_halo(nxt, nxt, 0)

        return carry

    lax.fori_loop(0, N_CONV, conv, 0)

    copies = []
    for t in (1, 0):
        for p in range(N_ROW):
            for j in range(4):
                for v in range(N_TILE):
                    tmp[p % 2, j, pl.ds(v, TILE, stride=N_TILE), :] = raw[
                        0, t, p, v * TILE : (v + 1) * TILE, j * 128 : (j + 1) * 128
                    ].astype(F32)
                x_in[t, p, :, j * 128 : (j + 1) * 128] = tmp[p % 2, j].astype(BF16)
            copies.append(pltpu.make_async_copy(x_in.at[t, p], out_hbm.at[t, p], o_sem.at[t, p]))
            copies[-1].start()
    for copy in copies:
        copy.wait()


def solution(mesh):
    cp_size = mesh.shape["cp"]

    def local_decode(latent, conv_w, conv_b, in_scale, in_shift, mid_scale, mid_shift):
        any_spec, vmem = pl.BlockSpec(memory_space=pl.ANY), pl.BlockSpec(memory_space=pltpu.VMEM)
        dma = pltpu.SemaphoreType.DMA
        frame = (N_ROW, N_COL, N_CH)
        extra = [] if EXPLICIT else [pltpu.VMEM((N_FR, N_ROW, 2, N_COL, HALF), F32)]
        return pl.pallas_call(
            functools.partial(kernel, cp_size),
            out_shape=jax.ShapeDtypeStruct(latent.shape, BF16),
            in_specs=[any_spec, any_spec, vmem, vmem, vmem, vmem, vmem],
            out_specs=any_spec,
            scratch_shapes=[
                pltpu.VMEM((N_FR, *frame), BF16),
                pltpu.VMEM((2, N_FR, *frame), BF16),
                pltpu.VMEM((2, N_FR, *frame), BF16),
                pltpu.VMEM((4, N_ROW, PAD_COL, N_CH), BF16),
                pltpu.VMEM((2, 3, 9 * N_CH, N_CH), BF16),
                pltpu.VMEM((2, 8, N_CH), F32),
                pltpu.VMEM((2, 8, 128), F32),
                pltpu.VMEM((2, cp_size - 1, 8, 128), F32),
                pltpu.VMEM((N_CONV, 4, N_CH), F32),
                pltpu.VMEM((N_CONV, 4, N_CH), F32),
                pltpu.VMEM((2, N_FR, N_CH), F32),
                pltpu.VMEM((2, N_FR, N_CH), F32),
                pltpu.VMEM((1, N_CH), F32),
                pltpu.VMEM((1, N_CH), F32),
                pltpu.VMEM((2, 4, N_COL, 128), F32),
                dma((N_FR,)),
                dma((2, 3)),
                dma((2, cp_size - 1)),
                dma((2, cp_size - 1)),
                dma((N_FR,)),
                dma((2, N_FR)),
                dma((2,)),
                dma((2,)),
                dma((N_FR, N_ROW)),
                *extra,
            ],
            compiler_params=pltpu.CompilerParams(
                collective_id=0, has_side_effects=True, vmem_limit_bytes=60 * 1024 * 1024
            ),
        )(latent, conv_w.reshape(N_CONV, 3, 9 * N_CH, N_CH), conv_b, in_scale, in_shift, mid_scale, mid_shift)

    time_spec = P(("dp", "cp"))
    param_spec = P(None, ("dp", "cp"))
    return jax.shard_map(
        local_decode,
        mesh=mesh,
        in_specs=(time_spec, P(), P(), P(), P(), param_spec, param_spec),
        out_specs=time_spec,
        check_vma=False,
    )
```

```python
import functools

import jax
import jax.numpy as jnp
from jax import lax
from jax.experimental import pallas as pl
from jax.experimental.pallas import tpu as pltpu
from jax.sharding import PartitionSpec as P

NUM_GROUPS = 32
EPSILON = 1e-6
MESH = pl.DeviceIdType.MESH
F32 = jnp.float32
BF16 = jnp.bfloat16

N_CONV = 4
N_FR = 2
N_ROW = 4
N_COL = 128
N_CH = 512
TILE = 16
N_TILE = N_COL // TILE
PAD_COL = N_COL + 2 * TILE
HALF = 256


def kernel(
    cp_size, x_hbm, w_hbm, bias_ref, in_scale, in_shift, mid_scale, mid_shift, out_hbm,
    x_in, raw, halo, act, wts, acc, part, tx, rx, gains, shifts, h_scale, h_shift, coef, tmp,
    x_sem, w_sem, st_send, st_recv, h_send, h_recv, p_send, p_recv, o_sem,
):
    cp = lax.axis_index("cp")
    count = float(N_FR * cp_size * N_ROW * N_COL * (N_CH // NUM_GROUPS))
    first, last = cp == 0, cp == cp_size - 1
    peers = [lax.rem(cp + d, cp_size) for d in range(1, cp_size)]
    right = lax.rem(cp + 1, cp_size)

    def mm_step(slot, t, k, p, dp, dq, kt):
        lhs = act[t + k, p + dp, TILE * (1 + dq) : TILE * (1 + dq) + N_COL, kt * HALF : (kt + 1) * HALF]
        off = ((dp + 1) * 3 + dq + 1) * N_CH + kt * HALF
        for m in range(2):
            w = wts[slot, k, off : off + HALF, m * HALF : (m + 1) * HALF]
            acc[t, p, m] += jnp.dot(lhs, w, preferred_element_type=F32)

    def pop(m, t, p):
        val = acc[t, p, m]
        acc[t, p, m] = jnp.zeros((N_COL, HALF), F32)
        return val

    def steps_of(t, k, kts=(0, 1), rows=range(N_ROW)):
        return [
            (t, k, p, dp, dq, kt)
            for kt in kts
            for p in rows
            for dp in (0, 1, -1)
            if 0 <= p + dp < N_ROW
            for dq in (0, -1, 1)
        ]

    def run(slot, steps, thunks=(), upto=1.0):
        done, span = 0, max(1, int(len(steps) * upto))
        for i, step in enumerate(steps):
            mm_step(slot, *step)
            want = min(len(thunks), -(-len(thunks) * (i + 1) // span))
            for thunk in thunks[done:want]:
                thunk()
            done = want

    def add_moments(val, half):
        cut = slice(half * HALF, (half + 1) * HALF)
        rows = val.reshape(N_COL // 8, 8, HALF)
        part[0, :, cut] += jnp.sum(rows, axis=0)
        part[1, :, cut] += jnp.sum(rows * rows, axis=0)

    def norm(read, f, p, half):
        cut = slice(half * HALF, (half + 1) * HALF)
        val = read(p, cut).astype(F32) * coef[0, f : f + 1, cut] + coef[1, f : f + 1, cut]
        val = val.astype(BF16).astype(F32)
        val = val + val * jnp.tanh(val)
        act[f, p, TILE : TILE + N_COL, cut] = val.astype(BF16)
        row = lax.broadcasted_iota(jnp.int32, (TILE, HALF), 0)
        low = jnp.where(row == 0, 0.0, pltpu.roll(val[N_COL - TILE :], 1, 0))
        act[f, p, 0:TILE, cut] = low.astype(BF16)
        high = jnp.where(row == TILE - 1, 0.0, pltpu.roll(val[:TILE], TILE - 1, 0))
        act[f, p, TILE + N_COL :, cut] = high.astype(BF16)

    def epilogue(c, par, t, p, m):
        cut = slice(m * HALF, (m + 1) * HALF)
        conv = (pop(m, t, p) + bias_ref[pl.ds(c, 1), cut]).astype(BF16).astype(F32)
        val = (raw[2 - 2 * par, t, p, :, cut].astype(F32) + conv).astype(BF16)
        raw[1 - par, t, p, :, cut] = val
        add_moments(val.astype(F32), m)

    def finish_moments(slot):
        for i in range(2):
            total = jnp.sum(part[i], axis=0, keepdims=True)
            for j in range(4):
                tx[slot, 4 * i + j : 4 * i + j + 1, :] = total[:, j * 128 : (j + 1) * 128]
        part[...] = jnp.zeros_like(part)

    def statistics(slot):
        total = tx[slot]
        for d in range(cp_size - 1):
            total = total + rx[slot, d]
        lane = lax.broadcasted_iota(jnp.int32, total.shape, 1)
        for unit in (1, 4):
            spot = (lane // unit) % 4
            terms = [total]
            for d in range(1, 4):
                up, down = pltpu.roll(total, 128 - d * unit, 1), pltpu.roll(total, d * unit, 1)
                terms.append(jnp.where(spot < 4 - d, up, 0.0))
                terms.append(jnp.where(spot >= d, down, 0.0))
            while len(terms) > 1:
                terms = [terms[i] + terms[i + 1] for i in range(0, len(terms) - 1, 2)] + terms[len(terms) & ~1 :]
            total = terms[0]
        mean = total[0:4] * (1.0 / count)
        var = total[4:8] * (1.0 / count) - mean * mean
        return mean, lax.rsqrt(var + EPSILON)

    def coefficients(c, mean, rstd, frames):
        for j in range(4):
            cut = slice(j * 128, (j + 1) * 128)
            for f in frames:
                gain = 0.5 * (rstd[j : j + 1] * gains[c, f : f + 1, cut])
                coef[0, f : f + 1, cut] = gain
                coef[1, f : f + 1, cut] = 0.5 * shifts[c, f : f + 1, cut] - mean[j : j + 1] * gain

    def w_copy(c, k):
        slot = lax.rem(c, 2)
        return pltpu.make_async_copy(w_hbm.at[c, k], wts.at[slot, k], w_sem.at[slot, k])

    def st_copy(slot, d):
        return pltpu.make_async_remote_copy(
            src_ref=tx.at[slot], dst_ref=rx.at[slot, d], send_sem=st_send.at[slot, d], recv_sem=st_recv.at[slot, d],
            device_id={"cp": peers[d]}, device_id_type=MESH,
        )

    def halo_copy(par, hs, t):
        return pltpu.make_async_remote_copy(
            src_ref=raw.at[par, t], dst_ref=halo.at[hs, t], send_sem=h_send.at[t], recv_sem=h_recv.at[hs, t],
            device_id={"cp": right}, device_id_type=MESH,
        )

    def own_copy(par, hs, t):
        return pltpu.make_async_copy(raw.at[par, 0], halo.at[hs, t], h_recv.at[hs, t])

    def param_copy(i):
        src, dst = ((mid_scale, h_scale), (mid_shift, h_shift))[i]
        return pltpu.make_async_remote_copy(
            src_ref=src, dst_ref=dst, send_sem=p_send.at[i], recv_sem=p_recv.at[i],
            device_id={"cp": right}, device_id_type=MESH,
        )

    def send_halo(par, hs, t):
        @pl.when(jnp.logical_not(last))
        def _():
            halo_copy(par, hs, t).start()

        if t == 0:

            @pl.when(first)
            def _():
                own_copy(par, hs, 0).start()
                own_copy(par, hs, 1).start()

    barrier = pltpu.get_barrier_semaphore()
    for peer in peers:
        pl.semaphore_signal(barrier, inc=1, device_id={"cp": peer}, device_id_type=MESH)
    x_copies = [pltpu.make_async_copy(x_hbm.at[t], x_in.at[t], x_sem.at[t]) for t in range(N_FR)]
    for t in (1, 0):
        x_copies[t].start()
    for k in (2, 1, 0):
        w_copy(0, k).start()

    part[...] = jnp.zeros_like(part)
    acc[...] = jnp.zeros_like(acc)
    raw[2] = jnp.zeros((N_FR, N_ROW, N_COL, N_CH), BF16)
    for b in range(2):
        for f in range(4):
            gains[2 * b, f : f + 1, :] = in_scale[b : b + 1, :]
            shifts[2 * b, f : f + 1, :] = in_shift[b : b + 1, :]
        gains[2 * b + 1, 2:4, :] = mid_scale[b]
        shifts[2 * b + 1, 2:4, :] = mid_shift[b]
    for t in (1, 0):
        x_copies[t].wait()
        for p in range(N_ROW):
            val = x_in[t, p].astype(F32)
            for half in range(2):
                add_moments(val[:, half * HALF : (half + 1) * HALF], half)
    finish_moments(0)
    pl.semaphore_wait(barrier, cp_size - 1)
    for d in range(cp_size - 1):
        st_copy(0, d).start()

    for t in (1, 0):
        for p in range(N_ROW):
            val = x_in[t, p].astype(F32)
            for j in range(4):
                tmp[p % 2, j] = val[:, j * 128 : (j + 1) * 128]
            for j in range(4):
                for v in range(N_TILE):
                    raw[0, t, p, v * TILE : (v + 1) * TILE, j * 128 : (j + 1) * 128] = tmp[
                        p % 2, j, pl.ds(v, TILE, stride=N_TILE), :
                    ].astype(BF16)
        if t == 1:

            @pl.when(jnp.logical_not(last))
            def _():
                for i in range(2):
                    param_copy(i).start()

        send_halo(0, 0, t)

    def conv(c, carry):
        par = lax.rem(c, 2)
        nxt = 1 - par

        @pl.when(c < N_CONV - 1)
        def _():
            for k in (2, 1, 0):
                w_copy(c + 1, k).start()

        for d in range(cp_size - 1):
            st_copy(par, d).wait()
        mean, rstd = statistics(par)
        coefficients(c, mean, rstd, (3, 2))

        def own(t):
            return lambda p, cut: raw[par, t, p, :, cut]

        def received(t):
            return lambda p, cut: halo[par, t, p, :, cut]

        def norms(read, f, halves=(0, 1)):
            return [functools.partial(norm, read, f, p, h) for h in halves for p in range(N_ROW)]

        def epilogues(t, rows):
            return [functools.partial(epilogue, c, par, t, p, m) for p in rows for m in range(2)]

        for thunk in norms(own(1), 3, (0,)):
            thunk()

        @pl.when(c == 0)
        def _():
            @pl.when(jnp.logical_not(first))
            def _():
                for i in range(2):
                    param_copy(i).wait_recv()
                for b in range(2):
                    gains[2 * b + 1, 0:2, :] = h_scale[b]
                    shifts[2 * b + 1, 0:2, :] = h_shift[b]

            @pl.when(first)
            def _():
                for b in range(2):
                    for f in range(2):
                        gains[2 * b + 1, f : f + 1, :] = mid_scale[b, 0:1]
                        shifts[2 * b + 1, f : f + 1, :] = mid_shift[b, 0:1]

            @pl.when(jnp.logical_not(last))
            def _():
                for i in range(2):
                    param_copy(i).wait_send()

        coefficients(c, mean, rstd, (1, 0))
        w_copy(c, 2).wait()
        run(par, steps_of(1, 2, (0,)), norms(own(1), 3, (1,)), 0.9)
        run(par, steps_of(1, 2, (1,)), norms(own(0), 2))
        w_copy(c, 1).wait()
        steps = steps_of(1, 1)
        run(par, steps[:44])
        own_copy(par, par, 1).wait()
        run(par, steps[44:], norms(received(1), 1))
        w_copy(c, 0).wait()
        for p in range(N_ROW):
            run(par, steps_of(1, 0, rows=(p,)), epilogues(1, (p - 1,)) if p else ())
        steps = steps_of(0, 2)
        run(par, steps[:10], epilogues(1, (N_ROW - 1,)))

        @pl.when(jnp.logical_not(last))
        def _():
            halo_copy(par, par, 1).wait_send()
            halo_copy(par, par, 0).wait_send()

        @pl.when(c < N_CONV - 1)
        def _():
            send_halo(nxt, nxt, 1)

        run(par, steps[10:])
        steps = steps_of(0, 1)
        run(par, steps[:40])
        own_copy(par, par, 0).wait()
        run(par, steps[40:], norms(received(0), 0))
        for p in range(N_ROW):
            run(par, steps_of(0, 0, rows=(p,)), epilogues(0, (p - 1,)) if p else ())
        for thunk in epilogues(0, (N_ROW - 1,)):
            thunk()
        finish_moments(nxt)

        @pl.when(c < N_CONV - 1)
        def _():
            for d in range(cp_size - 1):
                st_copy(nxt, d).start()
            send_halo(nxt, nxt, 0)

        return carry

    lax.fori_loop(0, N_CONV, conv, 0)

    copies = []
    for t in (1, 0):
        for p in range(N_ROW):
            for j in range(4):
                for v in range(N_TILE):
                    tmp[p % 2, j, pl.ds(v, TILE, stride=N_TILE), :] = raw[
                        0, t, p, v * TILE : (v + 1) * TILE, j * 128 : (j + 1) * 128
                    ].astype(F32)
                x_in[t, p, :, j * 128 : (j + 1) * 128] = tmp[p % 2, j].astype(BF16)
            copies.append(pltpu.make_async_copy(x_in.at[t, p], out_hbm.at[t, p], o_sem.at[t, p]))
            copies[-1].start()
    for copy in copies:
        copy.wait()


def solution(mesh):
    cp_size = mesh.shape["cp"]

    def local_decode(latent, conv_w, conv_b, in_scale, in_shift, mid_scale, mid_shift):
        any_spec, vmem = pl.BlockSpec(memory_space=pl.ANY), pl.BlockSpec(memory_space=pltpu.VMEM)
        dma = pltpu.SemaphoreType.DMA
        frame = (N_ROW, N_COL, N_CH)
        return pl.pallas_call(
            functools.partial(kernel, cp_size),
            out_shape=jax.ShapeDtypeStruct(latent.shape, BF16),
            in_specs=[any_spec, any_spec, vmem, vmem, vmem, vmem, vmem],
            out_specs=any_spec,
            scratch_shapes=[
                pltpu.VMEM((N_FR, *frame), BF16),
                pltpu.VMEM((3, N_FR, *frame), BF16),
                pltpu.VMEM((2, N_FR, *frame), BF16),
                pltpu.VMEM((4, N_ROW, PAD_COL, N_CH), BF16),
                pltpu.VMEM((2, 3, 9 * N_CH, N_CH), BF16),
                pltpu.VMEM((N_FR, N_ROW, 2, N_COL, HALF), F32),
                pltpu.VMEM((2, 8, N_CH), F32),
                pltpu.VMEM((2, 8, 128), F32),
                pltpu.VMEM((2, cp_size - 1, 8, 128), F32),
                pltpu.VMEM((N_CONV, 4, N_CH), F32),
                pltpu.VMEM((N_CONV, 4, N_CH), F32),
                pltpu.VMEM((2, N_FR, N_CH), F32),
                pltpu.VMEM((2, N_FR, N_CH), F32),
                pltpu.VMEM((2, 4, N_CH), F32),
                pltpu.VMEM((2, 4, N_COL, 128), F32),
                dma((N_FR,)),
                dma((2, 3)),
                dma((2, cp_size - 1)),
                dma((2, cp_size - 1)),
                dma((N_FR,)),
                dma((2, N_FR)),
                dma((2,)),
                dma((2,)),
                dma((N_FR, N_ROW)),
            ],
            compiler_params=pltpu.CompilerParams(
                collective_id=0, has_side_effects=True, vmem_limit_bytes=60 * 1024 * 1024
            ),
        )(latent, conv_w.reshape(N_CONV, 3, 9 * N_CH, N_CH), conv_b, in_scale, in_shift, mid_scale, mid_shift)

    time_spec = P(("dp", "cp"))
    param_spec = P(None, ("dp", "cp"))
    return jax.shard_map(
        local_decode,
        mesh=mesh,
        in_specs=(time_spec, P(), P(), P(), P(), param_spec, param_spec),
        out_specs=time_spec,
        check_vma=False,
    )
```

```python
import functools

import jax
import jax.numpy as jnp
from jax import lax
from jax.experimental import pallas as pl
from jax.experimental.pallas import tpu as pltpu
from jax.sharding import PartitionSpec as P

NUM_GROUPS = 32
EPSILON = 1e-6
MESH = pl.DeviceIdType.MESH
F32 = jnp.float32
BF16 = jnp.bfloat16

N_CONV = 4
N_FR = 2
N_ROW = 4
N_COL = 128
N_CH = 512
TILE = 16
PIECES = ((1, slice(0, 2)), (1, slice(2, 4)), (0, slice(0, 4)))
N_TILE = N_COL // TILE
PAD_COL = N_COL + 2 * TILE
HALF = 256


def kernel(
    cp_size, x_hbm, w_hbm, bias_hbm, in_scale_hbm, in_shift_hbm, mid_scale_hbm, mid_shift_hbm, out_ref,
    bias_ref, in_scale, in_shift, mid_scale, mid_shift,
    x_in, raw, halo, act, wts, acc, part, tx, rx, gains, shifts, h_scale, h_shift, coef, tmp,
    x_sem, s_sem, w_sem, st_send, st_recv, h_send, h_recv, p_send, p_recv,
):
    cp = lax.axis_index("cp")
    count = float(N_FR * cp_size * N_ROW * N_COL * (N_CH // NUM_GROUPS))
    first, last = cp == 0, cp == cp_size - 1
    peers = [lax.rem(cp + d, cp_size) for d in range(1, cp_size)]
    right = lax.rem(cp + 1, cp_size)

    def mm_step(slot, t, k, p, dp, dq, kt):
        lhs = act[t + k, p + dp, TILE * (1 + dq) : TILE * (1 + dq) + N_COL, kt * HALF : (kt + 1) * HALF]
        off = ((dp + 1) * 3 + dq + 1) * N_CH + kt * HALF
        for m in range(2):
            w = wts[slot, k, off : off + HALF, m * HALF : (m + 1) * HALF]
            acc[t, p, m] += jnp.dot(lhs, w, preferred_element_type=F32)

    def pop(m, t, p):
        val = acc[t, p, m]
        acc[t, p, m] = jnp.zeros((N_COL, HALF), F32)
        return val

    def steps_of(t, k, kts=(0, 1), rows=range(N_ROW)):
        return [
            (t, k, p, dp, dq, kt)
            for kt in kts
            for p in rows
            for dp in (0, 1, -1)
            if 0 <= p + dp < N_ROW
            for dq in (0, -1, 1)
        ]

    def run(slot, steps, thunks=(), upto=1.0):
        done, span = 0, max(1, int(len(steps) * upto))
        for i, step in enumerate(steps):
            mm_step(slot, *step)
            want = min(len(thunks), -(-len(thunks) * (i + 1) // span))
            for thunk in thunks[done:want]:
                thunk()
            done = want

    def add_moments(val, half):
        cut = slice(half * HALF, (half + 1) * HALF)
        rows = val.reshape(N_COL // 8, 8, HALF)
        part[0, :, cut] += jnp.sum(rows, axis=0)
        part[1, :, cut] += jnp.sum(rows * rows, axis=0)

    def norm(read, f, p, half):
        cut = slice(half * HALF, (half + 1) * HALF)
        val = read(p, cut).astype(F32) * coef[0, f : f + 1, cut] + coef[1, f : f + 1, cut]
        val = val.astype(BF16).astype(F32)
        val = val + val * jnp.tanh(val)
        act[f, p, TILE : TILE + N_COL, cut] = val.astype(BF16)
        row = lax.broadcasted_iota(jnp.int32, (TILE, HALF), 0)
        low = jnp.where(row == 0, 0.0, pltpu.roll(val[N_COL - TILE :], 1, 0))
        act[f, p, 0:TILE, cut] = low.astype(BF16)
        high = jnp.where(row == TILE - 1, 0.0, pltpu.roll(val[:TILE], TILE - 1, 0))
        act[f, p, TILE + N_COL :, cut] = high.astype(BF16)

    def epilogue(c, par, t, p, m):
        cut = slice(m * HALF, (m + 1) * HALF)
        conv = (pop(m, t, p) + bias_ref[pl.ds(c, 1), cut]).astype(BF16).astype(F32)
        val = (raw[2 - 2 * par, t, p, :, cut].astype(F32) + conv).astype(BF16)
        raw[1 - par, t, p, :, cut] = val
        add_moments(val.astype(F32), m)

    def finish_moments(slot):
        for i in range(2):
            total = jnp.sum(part[i], axis=0, keepdims=True)
            for j in range(4):
                tx[slot, 4 * i + j : 4 * i + j + 1, :] = total[:, j * 128 : (j + 1) * 128]
        part[...] = jnp.zeros_like(part)

    def statistics(slot):
        total = tx[slot]
        for d in range(cp_size - 1):
            total = total + rx[slot, d]
        lane = lax.broadcasted_iota(jnp.int32, total.shape, 1)
        for unit in (1, 4):
            spot = (lane // unit) % 4
            terms = [total]
            for d in range(1, 4):
                up, down = pltpu.roll(total, 128 - d * unit, 1), pltpu.roll(total, d * unit, 1)
                terms.append(jnp.where(spot < 4 - d, up, 0.0))
                terms.append(jnp.where(spot >= d, down, 0.0))
            while len(terms) > 1:
                terms = [terms[i] + terms[i + 1] for i in range(0, len(terms) - 1, 2)] + terms[len(terms) & ~1 :]
            total = terms[0]
        mean = total[0:4] * (1.0 / count)
        var = total[4:8] * (1.0 / count) - mean * mean
        return mean, lax.rsqrt(var + EPSILON)

    def coefficients(c, mean, rstd, frames):
        for j in range(4):
            cut = slice(j * 128, (j + 1) * 128)
            for f in frames:
                gain = 0.5 * (rstd[j : j + 1] * gains[c, f : f + 1, cut])
                coef[0, f : f + 1, cut] = gain
                coef[1, f : f + 1, cut] = 0.5 * shifts[c, f : f + 1, cut] - mean[j : j + 1] * gain

    def w_copy(c, k):
        slot = lax.rem(c, 2)
        return pltpu.make_async_copy(w_hbm.at[c, k], wts.at[slot, k], w_sem.at[slot, k])

    def st_copy(slot, d):
        return pltpu.make_async_remote_copy(
            src_ref=tx.at[slot], dst_ref=rx.at[slot, d], send_sem=st_send.at[slot, d], recv_sem=st_recv.at[slot, d],
            device_id={"cp": peers[d]}, device_id_type=MESH,
        )

    def halo_copy(par, hs, i):
        t, rows = PIECES[i]
        return pltpu.make_async_remote_copy(
            src_ref=raw.at[par, t, rows], dst_ref=halo.at[hs, t, rows],
            send_sem=h_send.at[hs, i], recv_sem=h_recv.at[hs, i],
            device_id={"cp": right}, device_id_type=MESH,
        )

    def own_copy(par, hs, i):
        t, rows = PIECES[i]
        return pltpu.make_async_copy(raw.at[par, 0, rows], halo.at[hs, t, rows], h_recv.at[hs, i])

    def param_copy(i):
        src, dst = ((mid_scale, h_scale), (mid_shift, h_shift))[i]
        return pltpu.make_async_remote_copy(
            src_ref=src, dst_ref=dst, send_sem=p_send.at[i], recv_sem=p_recv.at[i],
            device_id={"cp": right}, device_id_type=MESH,
        )

    barrier = pltpu.get_barrier_semaphore()
    for peer in peers:
        pl.semaphore_signal(barrier, inc=1, device_id={"cp": peer}, device_id_type=MESH)
    x_copies = [pltpu.make_async_copy(x_hbm.at[t], x_in.at[t], x_sem.at[t]) for t in range(N_FR)]
    for t in (1, 0):
        x_copies[t].start()
    small = ((bias_hbm, bias_ref), (in_scale_hbm, in_scale), (in_shift_hbm, in_shift),
             (mid_scale_hbm, mid_scale), (mid_shift_hbm, mid_shift))
    small_copies = [pltpu.make_async_copy(src, dst, s_sem.at[i]) for i, (src, dst) in enumerate(small)]
    for copy in small_copies:
        copy.start()
    for k in (2, 1, 0):
        w_copy(0, k).start()

    part[...] = jnp.zeros_like(part)
    acc[...] = jnp.zeros_like(acc)
    raw[2] = jnp.zeros((N_FR, N_ROW, N_COL, N_CH), BF16)
    for t in (1, 0):
        x_copies[t].wait()
        for p in range(N_ROW):
            val = x_in[t, p].astype(F32)
            for half in range(2):
                add_moments(val[:, half * HALF : (half + 1) * HALF], half)
    finish_moments(0)
    pl.semaphore_wait(barrier, cp_size - 1)
    for d in range(cp_size - 1):
        st_copy(0, d).start()

    for copy in small_copies:
        copy.wait()
    for b in range(2):
        for f in range(4):
            gains[2 * b, f : f + 1, :] = in_scale[b : b + 1, :]
            shifts[2 * b, f : f + 1, :] = in_shift[b : b + 1, :]
        gains[2 * b + 1, 2:4, :] = mid_scale[b]
        shifts[2 * b + 1, 2:4, :] = mid_shift[b]
    for t in (1, 0):
        for p in range(N_ROW):
            val = x_in[t, p].astype(F32)
            for j in range(4):
                tmp[p % 2, j] = val[:, j * 128 : (j + 1) * 128]
            for j in range(4):
                for v in range(N_TILE):
                    raw[0, t, p, v * TILE : (v + 1) * TILE, j * 128 : (j + 1) * 128] = tmp[
                        p % 2, j, pl.ds(v, TILE, stride=N_TILE), :
                    ].astype(BF16)
            if (t, p) in ((1, 1), (1, 3), (0, 3)):
                piece = {(1, 1): 0, (1, 3): 1, (0, 3): 2}[t, p]

                @pl.when(jnp.logical_not(last))
                def _():
                    if piece == 0:
                        for i in range(2):
                            param_copy(i).start()
                    halo_copy(0, 0, piece).start()

    @pl.when(first)
    def _():
        for i in range(3):
            own_copy(0, 0, i).start()

    def conv(c, carry):
        par = lax.rem(c, 2)
        nxt = 1 - par

        @pl.when(c < N_CONV - 1)
        def _():
            for k in (2, 1, 0):
                w_copy(c + 1, k).start()

        for d in range(cp_size - 1):
            st_copy(par, d).wait()
        mean, rstd = statistics(par)
        coefficients(c, mean, rstd, (3, 2))

        def own(t):
            return lambda p, cut: raw[par, t, p, :, cut]

        def received(t):
            return lambda p, cut: halo[par, t, p, :, cut]

        def norms(read, f, halves=(0, 1), rows=range(N_ROW)):
            return [functools.partial(norm, read, f, p, h) for h in halves for p in rows]

        def epilogues(t, rows):
            return [functools.partial(epilogue, c, par, t, p, m) for p in rows for m in range(2)]

        for thunk in norms(own(1), 3, (0,)):
            thunk()

        @pl.when(c == 0)
        def _():
            @pl.when(jnp.logical_not(first))
            def _():
                for i in range(2):
                    param_copy(i).wait_recv()
                for b in range(2):
                    gains[2 * b + 1, 0:2, :] = h_scale[b]
                    shifts[2 * b + 1, 0:2, :] = h_shift[b]

            @pl.when(first)
            def _():
                for b in range(2):
                    for f in range(2):
                        gains[2 * b + 1, f : f + 1, :] = mid_scale[b, 0:1]
                        shifts[2 * b + 1, f : f + 1, :] = mid_shift[b, 0:1]

            @pl.when(jnp.logical_not(last))
            def _():
                for i in range(2):
                    param_copy(i).wait_send()

        coefficients(c, mean, rstd, (1, 0))
        w_copy(c, 2).wait()
        w_copy(c, 1).wait()
        run(par, steps_of(1, 2, (0,)), norms(own(1), 3, (1,)), 0.9)
        run(par, steps_of(1, 2, (1,)), norms(own(0), 2))
        run(par, steps_of(1, 1))
        w_copy(c, 0).wait()
        own_copy(par, par, 0).wait()
        run(par, steps_of(0, 2, (0,)), norms(received(1), 1, rows=(0, 1)))
        own_copy(par, par, 1).wait()
        run(par, steps_of(1, 0, rows=(0,)), norms(received(1), 1, rows=(2, 3)), 0.7)
        for p in (1, 2):
            run(par, steps_of(1, 0, rows=(p,)), epilogues(1, (p - 1,)), 0.6)

        @pl.when(jnp.logical_and(c < N_CONV - 1, jnp.logical_not(last)))
        def _():
            halo_copy(nxt, nxt, 0).start()

        run(par, steps_of(1, 0, rows=(3,)), epilogues(1, (2,)))
        run(par, steps_of(0, 2, (1,)), epilogues(1, (3,)))
        steps = steps_of(0, 1)
        run(par, steps[:40])
        own_copy(par, par, 2).wait()
        run(par, steps[40:], norms(received(0), 0))
        for p in range(N_ROW):
            run(par, steps_of(0, 0, rows=(p,)), epilogues(0, (p - 1,)) if p else ())
        for thunk in epilogues(0, (N_ROW - 1,)):
            thunk()
        finish_moments(nxt)

        @pl.when(c < N_CONV - 1)
        def _():
            for d in range(cp_size - 1):
                st_copy(nxt, d).start()

            @pl.when(jnp.logical_not(last))
            def _():
                for i in (1, 2):
                    halo_copy(nxt, nxt, i).start()

            @pl.when(first)
            def _():
                for i in range(3):
                    own_copy(nxt, nxt, i).start()

        @pl.when(jnp.logical_not(last))
        def _():
            for i in range(3):
                halo_copy(par, par, i).wait_send()

        return carry

    lax.fori_loop(0, N_CONV, conv, 0)

    out_ref[...] = raw[0]


def reorder(val_ref, out_hbm, tmp, buf, sem):
    copies = []
    for t in range(N_FR):
        for p in range(N_ROW):
            for j in range(4):
                cut = slice(j * 128, (j + 1) * 128)
                for v in range(N_TILE):
                    tmp[p % 2, j, pl.ds(v, TILE, stride=N_TILE), :] = val_ref[
                        t, p, v * TILE : (v + 1) * TILE, cut
                    ].astype(F32)
                buf[t, p, :, cut] = tmp[p % 2, j].astype(BF16)
            copies.append(pltpu.make_async_copy(buf.at[t, p], out_hbm.at[t, p], sem.at[t, p]))
            copies[-1].start()
    for copy in copies:
        copy.wait()


def solution(mesh):
    cp_size = mesh.shape["cp"]

    def local_decode(latent, conv_w, conv_b, in_scale, in_shift, mid_scale, mid_shift):
        any_spec, vmem = pl.BlockSpec(memory_space=pl.ANY), pl.BlockSpec(memory_space=pltpu.VMEM)
        dma = pltpu.SemaphoreType.DMA
        frame = (N_ROW, N_COL, N_CH)
        blocks = pl.pallas_call(
            functools.partial(kernel, cp_size),
            out_shape=jax.ShapeDtypeStruct(latent.shape, BF16),
            in_specs=[any_spec] * 7,
            out_specs=vmem,
            scratch_shapes=[
                pltpu.VMEM((N_CONV, N_CH), F32),
                pltpu.VMEM((2, N_CH), F32),
                pltpu.VMEM((2, N_CH), F32),
                pltpu.VMEM((2, N_FR, N_CH), F32),
                pltpu.VMEM((2, N_FR, N_CH), F32),
                pltpu.VMEM((N_FR, *frame), BF16),
                pltpu.VMEM((3, N_FR, *frame), BF16),
                pltpu.VMEM((2, N_FR, *frame), BF16),
                pltpu.VMEM((4, N_ROW, PAD_COL, N_CH), BF16),
                pltpu.VMEM((2, 3, 9 * N_CH, N_CH), BF16),
                pltpu.VMEM((N_FR, N_ROW, 2, N_COL, HALF), F32),
                pltpu.VMEM((2, 8, N_CH), F32),
                pltpu.VMEM((2, 8, 128), F32),
                pltpu.VMEM((2, cp_size - 1, 8, 128), F32),
                pltpu.VMEM((N_CONV, 4, N_CH), F32),
                pltpu.VMEM((N_CONV, 4, N_CH), F32),
                pltpu.VMEM((2, N_FR, N_CH), F32),
                pltpu.VMEM((2, N_FR, N_CH), F32),
                pltpu.VMEM((2, 4, N_CH), F32),
                pltpu.VMEM((2, 4, N_COL, 128), F32),
                dma((N_FR,)),
                dma((5,)),
                dma((2, 3)),
                dma((2, cp_size - 1)),
                dma((2, cp_size - 1)),
                dma((2, 3)),
                dma((2, 3)),
                dma((2,)),
                dma((2,)),
            ],
            compiler_params=pltpu.CompilerParams(
                collective_id=0, has_side_effects=True, vmem_limit_bytes=46 * 1024 * 1024
            ),
        )(*[
            pltpu.with_memory_space_constraint(arg, pltpu.HBM)
            for arg in (
                latent, conv_w.reshape(N_CONV, 3, 9 * N_CH, N_CH), conv_b, in_scale, in_shift, mid_scale, mid_shift
            )
        ])
        return pl.pallas_call(
            reorder,
            out_shape=jax.ShapeDtypeStruct(latent.shape, BF16),
            in_specs=[vmem],
            out_specs=any_spec,
            scratch_shapes=[
                pltpu.VMEM((2, 4, N_COL, 128), F32),
                pltpu.VMEM((N_FR, *frame), BF16),
                dma((N_FR, N_ROW)),
            ],
            compiler_params=pltpu.CompilerParams(vmem_limit_bytes=6 * 1024 * 1024),
        )(blocks)

    time_spec = P(("dp", "cp"))
    param_spec = P(None, ("dp", "cp"))
    return jax.shard_map(
        local_decode,
        mesh=mesh,
        in_specs=(time_spec, P(), P(), P(), P(), param_spec, param_spec),
        out_specs=time_spec,
        check_vma=False,
    )
```

```python
import functools

import jax
import jax.numpy as jnp
from jax import lax
from jax.experimental import pallas as pl
from jax.experimental.pallas import tpu as pltpu
from jax.sharding import PartitionSpec as P

NUM_GROUPS = 32
EPSILON = 1e-6
MESH = pl.DeviceIdType.MESH
F32 = jnp.float32
BF16 = jnp.bfloat16

N_CONV = 4
N_FR = 2
N_ROW = 4
N_COL = 128
N_CH = 512
TILE = 16
PIECES = ((1, slice(0, 2)), (1, slice(2, 4)), (0, slice(0, 2)), (0, slice(2, 4)))
N_TILE = N_COL // TILE
PAD_COL = N_COL + 2 * TILE
HALF = 256


def kernel(
    cp_size, x_hbm, w_hbm, bias_hbm, in_scale_hbm, in_shift_hbm, mid_scale_hbm, mid_shift_hbm, out_ref,
    bias_ref, in_scale, in_shift, mid_scale, mid_shift,
    x_in, raw, halo, act, wts, acc, part, tx, rx, gains, shifts, h_scale, h_shift, coef, tmp,
    x_sem, s_sem, w_sem, st_send, st_recv, h_send, h_recv, p_send, p_recv,
):
    cp = lax.axis_index("cp")
    count = float(N_FR * cp_size * N_ROW * N_COL * (N_CH // NUM_GROUPS))
    first, last = cp == 0, cp == cp_size - 1
    peers = [lax.rem(cp + d, cp_size) for d in range(1, cp_size)]
    right = lax.rem(cp + 1, cp_size)

    def mm_step(slot, t, k, p, dp, dq, kt):
        lhs = act[t + k, p + dp, TILE * (1 + dq) : TILE * (1 + dq) + N_COL, kt * HALF : (kt + 1) * HALF]
        off = ((dp + 1) * 3 + dq + 1) * N_CH + kt * HALF
        for m in range(2):
            w = wts[slot, k, off : off + HALF, m * HALF : (m + 1) * HALF]
            acc[t, p, m] += jnp.dot(lhs, w, preferred_element_type=F32)

    def pop(m, t, p):
        val = acc[t, p, m]
        acc[t, p, m] = jnp.zeros((N_COL, HALF), F32)
        return val

    def steps_of(t, k, kts=(0, 1), rows=range(N_ROW), dps=(0, 1, -1)):
        return [
            (t, k, p, dp, dq, kt)
            for kt in kts
            for p in rows
            for dp in dps
            if 0 <= p + dp < N_ROW
            for dq in (0, -1, 1)
        ]

    def run(slot, steps, thunks=(), upto=1.0):
        done, span = 0, max(1, int(len(steps) * upto))
        for i, step in enumerate(steps):
            mm_step(slot, *step)
            want = min(len(thunks), -(-len(thunks) * (i + 1) // span))
            for thunk in thunks[done:want]:
                thunk()
            done = want

    def add_moments(val, half):
        cut = slice(half * HALF, (half + 1) * HALF)
        rows = val.reshape(N_COL // 8, 8, HALF)
        part[0, :, cut] += jnp.sum(rows, axis=0)
        part[1, :, cut] += jnp.sum(rows * rows, axis=0)

    def norm(read, f, p, half):
        cut = slice(half * HALF, (half + 1) * HALF)
        val = read(p, cut).astype(F32) * coef[0, f : f + 1, cut] + coef[1, f : f + 1, cut]
        val = val.astype(BF16).astype(F32)
        val = val + val * jnp.tanh(val)
        act[f, p, TILE : TILE + N_COL, cut] = val.astype(BF16)
        row = lax.broadcasted_iota(jnp.int32, (TILE, HALF), 0)
        low = jnp.where(row == 0, 0.0, pltpu.roll(val[N_COL - TILE :], 1, 0))
        act[f, p, 0:TILE, cut] = low.astype(BF16)
        high = jnp.where(row == TILE - 1, 0.0, pltpu.roll(val[:TILE], TILE - 1, 0))
        act[f, p, TILE + N_COL :, cut] = high.astype(BF16)

    def epilogue(c, par, t, p, m):
        cut = slice(m * HALF, (m + 1) * HALF)
        conv = (pop(m, t, p) + bias_ref[pl.ds(c, 1), cut]).astype(BF16).astype(F32)
        val = (raw[2 - 2 * par, t, p, :, cut].astype(F32) + conv).astype(BF16)
        raw[1 - par, t, p, :, cut] = val
        add_moments(val.astype(F32), m)

    def finish_moments(slot):
        for i in range(2):
            total = jnp.sum(part[i], axis=0, keepdims=True)
            for j in range(4):
                tx[slot, 4 * i + j : 4 * i + j + 1, :] = total[:, j * 128 : (j + 1) * 128]
        part[...] = jnp.zeros_like(part)

    def statistics(slot):
        total = tx[slot]
        for d in range(cp_size - 1):
            total = total + rx[slot, d]
        lane = lax.broadcasted_iota(jnp.int32, total.shape, 1)
        for unit in (1, 4):
            spot = (lane // unit) % 4
            terms = [total]
            for d in range(1, 4):
                up, down = pltpu.roll(total, 128 - d * unit, 1), pltpu.roll(total, d * unit, 1)
                terms.append(jnp.where(spot < 4 - d, up, 0.0))
                terms.append(jnp.where(spot >= d, down, 0.0))
            while len(terms) > 1:
                terms = [terms[i] + terms[i + 1] for i in range(0, len(terms) - 1, 2)] + terms[len(terms) & ~1 :]
            total = terms[0]
        mean = total[0:4] * (1.0 / count)
        var = total[4:8] * (1.0 / count) - mean * mean
        return mean, lax.rsqrt(var + EPSILON)

    def coefficients(c, mean, rstd, frames):
        for j in range(4):
            cut = slice(j * 128, (j + 1) * 128)
            for f in frames:
                gain = 0.5 * (rstd[j : j + 1] * gains[c, f : f + 1, cut])
                coef[0, f : f + 1, cut] = gain
                coef[1, f : f + 1, cut] = 0.5 * shifts[c, f : f + 1, cut] - mean[j : j + 1] * gain

    def w_copy(c, k):
        slot = lax.rem(c, 2)
        return pltpu.make_async_copy(w_hbm.at[c, k], wts.at[slot, k], w_sem.at[slot, k])

    def st_copy(slot, d):
        return pltpu.make_async_remote_copy(
            src_ref=tx.at[slot], dst_ref=rx.at[slot, d], send_sem=st_send.at[slot, d], recv_sem=st_recv.at[slot, d],
            device_id={"cp": peers[d]}, device_id_type=MESH,
        )

    def halo_copy(par, hs, i):
        t, rows = PIECES[i]
        return pltpu.make_async_remote_copy(
            src_ref=raw.at[par, t, rows], dst_ref=halo.at[hs, t, rows],
            send_sem=h_send.at[hs, i], recv_sem=h_recv.at[hs, i],
            device_id={"cp": right}, device_id_type=MESH,
        )

    def own_copy(par, hs, i):
        t, rows = PIECES[i]
        return pltpu.make_async_copy(raw.at[par, 0, rows], halo.at[hs, t, rows], h_recv.at[hs, i])

    def param_copy(i):
        src, dst = ((mid_scale, h_scale), (mid_shift, h_shift))[i]
        return pltpu.make_async_remote_copy(
            src_ref=src, dst_ref=dst, send_sem=p_send.at[i], recv_sem=p_recv.at[i],
            device_id={"cp": right}, device_id_type=MESH,
        )

    barrier = pltpu.get_barrier_semaphore()
    for peer in peers:
        pl.semaphore_signal(barrier, inc=1, device_id={"cp": peer}, device_id_type=MESH)
    x_copies = [pltpu.make_async_copy(x_hbm.at[t], x_in.at[t], x_sem.at[t]) for t in range(N_FR)]
    for t in (1, 0):
        x_copies[t].start()
    small = ((bias_hbm, bias_ref), (in_scale_hbm, in_scale), (in_shift_hbm, in_shift),
             (mid_scale_hbm, mid_scale), (mid_shift_hbm, mid_shift))
    small_copies = [pltpu.make_async_copy(src, dst, s_sem.at[i]) for i, (src, dst) in enumerate(small)]
    for copy in small_copies:
        copy.start()
    for k in (2, 1, 0):
        w_copy(0, k).start()

    part[...] = jnp.zeros_like(part)
    acc[...] = jnp.zeros_like(acc)
    raw[2] = jnp.zeros((N_FR, N_ROW, N_COL, N_CH), BF16)
    for t in (1, 0):
        x_copies[t].wait()
        for p in range(N_ROW):
            val = x_in[t, p].astype(F32)
            for half in range(2):
                add_moments(val[:, half * HALF : (half + 1) * HALF], half)
    finish_moments(0)
    pl.semaphore_wait(barrier, cp_size - 1)
    for d in range(cp_size - 1):
        st_copy(0, d).start()

    for copy in small_copies:
        copy.wait()
    for b in range(2):
        for f in range(4):
            gains[2 * b, f : f + 1, :] = in_scale[b : b + 1, :]
            shifts[2 * b, f : f + 1, :] = in_shift[b : b + 1, :]
        gains[2 * b + 1, 2:4, :] = mid_scale[b]
        shifts[2 * b + 1, 2:4, :] = mid_shift[b]
    for t in (1, 0):
        for p in range(N_ROW):
            val = x_in[t, p].astype(F32)
            for j in range(4):
                tmp[p % 2, j] = val[:, j * 128 : (j + 1) * 128]
            for j in range(4):
                for v in range(N_TILE):
                    raw[0, t, p, v * TILE : (v + 1) * TILE, j * 128 : (j + 1) * 128] = tmp[
                        p % 2, j, pl.ds(v, TILE, stride=N_TILE), :
                    ].astype(BF16)
            if p % 2:
                piece = 2 * (1 - t) + p // 2

                @pl.when(jnp.logical_not(last))
                def _():
                    if piece == 0:
                        for i in range(2):
                            param_copy(i).start()
                    halo_copy(0, 0, piece).start()

    @pl.when(first)
    def _():
        for i in range(len(PIECES)):
            own_copy(0, 0, i).start()

    def conv(c, carry):
        par = lax.rem(c, 2)
        nxt = 1 - par

        @pl.when(c < N_CONV - 1)
        def _():
            for k in (2, 1, 0):
                w_copy(c + 1, k).start()

        for d in range(cp_size - 1):
            st_copy(par, d).wait()
        mean, rstd = statistics(par)
        coefficients(c, mean, rstd, (3, 2))

        def own(t):
            return lambda p, cut: raw[par, t, p, :, cut]

        def received(t):
            return lambda p, cut: halo[par, t, p, :, cut]

        def norms(read, f, halves=(0, 1), rows=range(N_ROW)):
            return [functools.partial(norm, read, f, p, h) for h in halves for p in rows]

        def epilogues(t, rows):
            return [functools.partial(epilogue, c, par, t, p, m) for p in rows for m in range(2)]

        for thunk in norms(own(1), 3, (0,), (0, 1)):
            thunk()

        @pl.when(c == 0)
        def _():
            @pl.when(jnp.logical_not(first))
            def _():
                for i in range(2):
                    param_copy(i).wait_recv()
                for b in range(2):
                    gains[2 * b + 1, 0:2, :] = h_scale[b]
                    shifts[2 * b + 1, 0:2, :] = h_shift[b]

            @pl.when(first)
            def _():
                for b in range(2):
                    for f in range(2):
                        gains[2 * b + 1, f : f + 1, :] = mid_scale[b, 0:1]
                        shifts[2 * b + 1, f : f + 1, :] = mid_shift[b, 0:1]

            @pl.when(jnp.logical_not(last))
            def _():
                for i in range(2):
                    param_copy(i).wait_send()

        coefficients(c, mean, rstd, (1, 0))
        w_copy(c, 2).wait()
        w_copy(c, 1).wait()
        run(par, steps_of(1, 2, (0,)), norms(own(1), 3, (0,), (2, 3)) + norms(own(1), 3, (1,)), 0.9)
        run(par, steps_of(1, 2, (1,)), norms(own(0), 2))
        run(par, steps_of(1, 1))
        w_copy(c, 0).wait()
        own_copy(par, par, 0).wait()
        steps = steps_of(0, 2)
        run(par, steps[:40], norms(received(1), 1, rows=(0, 1)), 0.9)
        own_copy(par, par, 1).wait()
        run(par, steps[40:], norms(received(1), 1, rows=(2, 3)), 0.9)
        run(par, steps_of(1, 0, dps=(1, -1)))
        for p in range(N_ROW):
            run(par, steps_of(1, 0, rows=(p,), dps=(0,)), epilogues(1, (p - 1,)) if p else ())
        steps = steps_of(0, 1)
        run(par, steps[:8], epilogues(1, (3,)))

        @pl.when(jnp.logical_and(c < N_CONV - 1, jnp.logical_not(last)))
        def _():
            halo_copy(nxt, nxt, 0).start()

        own_copy(par, par, 2).wait()
        run(par, steps[8:52], norms(received(0), 0, rows=(0, 1)), 0.9)
        own_copy(par, par, 3).wait()
        run(par, steps[52:], norms(received(0), 0, rows=(2, 3)), 0.9)
        run(par, steps_of(0, 0, dps=(1, -1)))
        for p in range(N_ROW):
            run(par, steps_of(0, 0, rows=(p,), dps=(0,)), epilogues(0, (p - 1,)) if p else ())
        for thunk in epilogues(0, (N_ROW - 1,)):
            thunk()
        finish_moments(nxt)

        @pl.when(c < N_CONV - 1)
        def _():
            for d in range(cp_size - 1):
                st_copy(nxt, d).start()

            @pl.when(jnp.logical_not(last))
            def _():
                for i in range(1, len(PIECES)):
                    halo_copy(nxt, nxt, i).start()

            @pl.when(first)
            def _():
                for i in range(len(PIECES)):
                    own_copy(nxt, nxt, i).start()

        @pl.when(jnp.logical_not(last))
        def _():
            for i in range(len(PIECES)):
                halo_copy(par, par, i).wait_send()

        return carry

    lax.fori_loop(0, N_CONV, conv, 0)

    out_ref[...] = raw[0]


def reorder(val_ref, out_hbm, tmp, buf, sem):
    copies = []
    for t in range(N_FR):
        for p in range(N_ROW):
            for j in range(4):
                cut = slice(j * 128, (j + 1) * 128)
                for v in range(N_TILE):
                    tmp[p % 2, j, pl.ds(v, TILE, stride=N_TILE), :] = val_ref[
                        t, p, v * TILE : (v + 1) * TILE, cut
                    ].astype(F32)
                buf[t, p, :, cut] = tmp[p % 2, j].astype(BF16)
            copies.append(pltpu.make_async_copy(buf.at[t, p], out_hbm.at[t, p], sem.at[t, p]))
            copies[-1].start()
    for copy in copies:
        copy.wait()


def solution(mesh):
    cp_size = mesh.shape["cp"]

    def local_decode(latent, conv_w, conv_b, in_scale, in_shift, mid_scale, mid_shift):
        any_spec, vmem = pl.BlockSpec(memory_space=pl.ANY), pl.BlockSpec(memory_space=pltpu.VMEM)
        dma = pltpu.SemaphoreType.DMA
        frame = (N_ROW, N_COL, N_CH)
        blocks = pl.pallas_call(
            functools.partial(kernel, cp_size),
            out_shape=jax.ShapeDtypeStruct(latent.shape, BF16),
            in_specs=[any_spec] * 7,
            out_specs=vmem,
            scratch_shapes=[
                pltpu.VMEM((N_CONV, N_CH), F32),
                pltpu.VMEM((2, N_CH), F32),
                pltpu.VMEM((2, N_CH), F32),
                pltpu.VMEM((2, N_FR, N_CH), F32),
                pltpu.VMEM((2, N_FR, N_CH), F32),
                pltpu.VMEM((N_FR, *frame), BF16),
                pltpu.VMEM((3, N_FR, *frame), BF16),
                pltpu.VMEM((2, N_FR, *frame), BF16),
                pltpu.VMEM((4, N_ROW, PAD_COL, N_CH), BF16),
                pltpu.VMEM((2, 3, 9 * N_CH, N_CH), BF16),
                pltpu.VMEM((N_FR, N_ROW, 2, N_COL, HALF), F32),
                pltpu.VMEM((2, 8, N_CH), F32),
                pltpu.VMEM((2, 8, 128), F32),
                pltpu.VMEM((2, cp_size - 1, 8, 128), F32),
                pltpu.VMEM((N_CONV, 4, N_CH), F32),
                pltpu.VMEM((N_CONV, 4, N_CH), F32),
                pltpu.VMEM((2, N_FR, N_CH), F32),
                pltpu.VMEM((2, N_FR, N_CH), F32),
                pltpu.VMEM((2, 4, N_CH), F32),
                pltpu.VMEM((2, 4, N_COL, 128), F32),
                dma((N_FR,)),
                dma((5,)),
                dma((2, 3)),
                dma((2, cp_size - 1)),
                dma((2, cp_size - 1)),
                dma((2, len(PIECES))),
                dma((2, len(PIECES))),
                dma((2,)),
                dma((2,)),
            ],
            compiler_params=pltpu.CompilerParams(
                collective_id=0, has_side_effects=True, vmem_limit_bytes=46 * 1024 * 1024
            ),
        )(*[
            pltpu.with_memory_space_constraint(arg, pltpu.HBM)
            for arg in (
                latent, conv_w.reshape(N_CONV, 3, 9 * N_CH, N_CH), conv_b, in_scale, in_shift, mid_scale, mid_shift
            )
        ])
        return pl.pallas_call(
            reorder,
            out_shape=jax.ShapeDtypeStruct(latent.shape, BF16),
            in_specs=[vmem],
            out_specs=any_spec,
            scratch_shapes=[
                pltpu.VMEM((2, 4, N_COL, 128), F32),
                pltpu.VMEM((N_FR, *frame), BF16),
                dma((N_FR, N_ROW)),
            ],
            compiler_params=pltpu.CompilerParams(vmem_limit_bytes=6 * 1024 * 1024),
        )(blocks)

    time_spec = P(("dp", "cp"))
    param_spec = P(None, ("dp", "cp"))
    return jax.shard_map(
        local_decode,
        mesh=mesh,
        in_specs=(time_spec, P(), P(), P(), P(), param_spec, param_spec),
        out_specs=time_spec,
        check_vma=False,
    )
```

```python
import functools

import jax
import jax.numpy as jnp
from jax import lax
from jax.experimental import pallas as pl
from jax.experimental.pallas import tpu as pltpu
from jax.sharding import PartitionSpec as P

NUM_GROUPS = 32
EPSILON = 1e-6
MESH = pl.DeviceIdType.MESH
F32 = jnp.float32
BF16 = jnp.bfloat16

N_CONV = 4
N_FR = 2
N_ROW = 4
N_COL = 128
N_CH = 512
TILE = 16
PIECES = ((1, slice(0, 2)), (1, slice(2, 4)), (0, slice(0, 2)), (0, slice(2, 4)))
N_TILE = N_COL // TILE
PAD_COL = N_COL + 2 * TILE
HALF = 256


def kernel(
    cp_size, x_hbm, w_hbm, bias_hbm, in_scale_hbm, in_shift_hbm, mid_scale_hbm, mid_shift_hbm, out_ref,
    bias_ref, in_scale, in_shift, mid_scale, mid_shift,
    x_in, raw, halo, act, wts, acc, part, tx, rx, gains, shifts, h_scale, h_shift, coef, tmp,
    x_sem, s_sem, w_sem, st_send, st_recv, h_send, h_recv, p_send, p_recv,
):
    cp = lax.axis_index("cp")
    count = float(N_FR * cp_size * N_ROW * N_COL * (N_CH // NUM_GROUPS))
    first, last = cp == 0, cp == cp_size - 1
    peers = [lax.rem(cp + d, cp_size) for d in range(1, cp_size)]
    right = lax.rem(cp + 1, cp_size)

    def mm_step(slot, t, k, low, high, dp, dq, kt):
        cut = slice(TILE * (1 + dq), TILE * (1 + dq) + N_COL)
        lhs = act[t + k, low + dp : high + dp, cut, kt * HALF : (kt + 1) * HALF].reshape((high - low) * N_COL, HALF)
        off = ((dp + 1) * 3 + dq + 1) * N_CH + kt * HALF
        for m in range(2):
            w = wts[slot, k, off : off + HALF, m * HALF : (m + 1) * HALF]
            out = jnp.dot(lhs, w, preferred_element_type=F32)
            for p in range(low, high):
                acc[t, p, m] += out[(p - low) * N_COL : (p - low + 1) * N_COL]

    def pop(m, t, p):
        val = acc[t, p, m]
        acc[t, p, m] = jnp.zeros((N_COL, HALF), F32)
        return val

    def steps_of(t, k, kts=(0, 1), rows=(0, N_ROW), dps=(0, 1, -1), size=N_ROW):
        return [
            (t, k, max(low, -dp), min(low + size, N_ROW - dp, rows[1]), dp, dq, kt)
            for kt in kts
            for low in range(rows[0], rows[1], size)
            for dp in dps
            if max(low, -dp) < min(low + size, N_ROW - dp, rows[1])
            for dq in (0, -1, 1)
        ]

    def run(slot, steps, thunks=(), upto=1.0):
        done, span = 0, max(1, int(len(steps) * upto))
        for i, step in enumerate(steps):
            mm_step(slot, *step)
            want = min(len(thunks), -(-len(thunks) * (i + 1) // span))
            for thunk in thunks[done:want]:
                thunk()
            done = want

    def add_moments(val, half):
        cut = slice(half * HALF, (half + 1) * HALF)
        rows = val.reshape(N_COL // 8, 8, HALF)
        part[0, :, cut] += jnp.sum(rows, axis=0)
        part[1, :, cut] += jnp.sum(rows * rows, axis=0)

    def norm(read, f, p, half):
        cut = slice(half * HALF, (half + 1) * HALF)
        val = read(p, cut).astype(F32) * coef[0, f : f + 1, cut] + coef[1, f : f + 1, cut]
        val = val.astype(BF16).astype(F32)
        val = val + val * jnp.tanh(val)
        act[f, p, TILE : TILE + N_COL, cut] = val.astype(BF16)
        row = lax.broadcasted_iota(jnp.int32, (TILE, HALF), 0)
        low = jnp.where(row == 0, 0.0, pltpu.roll(val[N_COL - TILE :], 1, 0))
        act[f, p, 0:TILE, cut] = low.astype(BF16)
        high = jnp.where(row == TILE - 1, 0.0, pltpu.roll(val[:TILE], TILE - 1, 0))
        act[f, p, TILE + N_COL :, cut] = high.astype(BF16)

    def epilogue(c, par, t, p, m):
        cut = slice(m * HALF, (m + 1) * HALF)
        conv = (pop(m, t, p) + bias_ref[pl.ds(c, 1), cut]).astype(BF16).astype(F32)
        val = (raw[2 - 2 * par, t, p, :, cut].astype(F32) + conv).astype(BF16)
        raw[1 - par, t, p, :, cut] = val
        add_moments(val.astype(F32), m)

    def finish_moments(slot):
        for i in range(2):
            total = jnp.sum(part[i], axis=0, keepdims=True)
            for j in range(4):
                tx[slot, 4 * i + j : 4 * i + j + 1, :] = total[:, j * 128 : (j + 1) * 128]
        part[...] = jnp.zeros_like(part)

    def statistics(slot):
        total = tx[slot]
        for d in range(cp_size - 1):
            total = total + rx[slot, d]
        lane = lax.broadcasted_iota(jnp.int32, total.shape, 1)
        for unit in (1, 4):
            spot = (lane // unit) % 4
            terms = [total]
            for d in range(1, 4):
                up, down = pltpu.roll(total, 128 - d * unit, 1), pltpu.roll(total, d * unit, 1)
                terms.append(jnp.where(spot < 4 - d, up, 0.0))
                terms.append(jnp.where(spot >= d, down, 0.0))
            while len(terms) > 1:
                terms = [terms[i] + terms[i + 1] for i in range(0, len(terms) - 1, 2)] + terms[len(terms) & ~1 :]
            total = terms[0]
        mean = total[0:4] * (1.0 / count)
        var = total[4:8] * (1.0 / count) - mean * mean
        return mean, lax.rsqrt(var + EPSILON)

    def coefficients(c, mean, rstd, frames):
        for j in range(4):
            cut = slice(j * 128, (j + 1) * 128)
            for f in frames:
                gain = 0.5 * (rstd[j : j + 1] * gains[c, f : f + 1, cut])
                coef[0, f : f + 1, cut] = gain
                coef[1, f : f + 1, cut] = 0.5 * shifts[c, f : f + 1, cut] - mean[j : j + 1] * gain

    def w_copy(c, k):
        slot = lax.rem(c, 2)
        return pltpu.make_async_copy(w_hbm.at[c, k], wts.at[slot, k], w_sem.at[slot, k])

    def st_copy(slot, d):
        return pltpu.make_async_remote_copy(
            src_ref=tx.at[slot], dst_ref=rx.at[slot, d], send_sem=st_send.at[slot, d], recv_sem=st_recv.at[slot, d],
            device_id={"cp": peers[d]}, device_id_type=MESH,
        )

    def halo_copy(par, hs, i):
        t, rows = PIECES[i]
        return pltpu.make_async_remote_copy(
            src_ref=raw.at[par, t, rows], dst_ref=halo.at[hs, t, rows],
            send_sem=h_send.at[hs, i], recv_sem=h_recv.at[hs, i],
            device_id={"cp": right}, device_id_type=MESH,
        )

    def own_copy(par, hs, i):
        t, rows = PIECES[i]
        return pltpu.make_async_copy(raw.at[par, 0, rows], halo.at[hs, t, rows], h_recv.at[hs, i])

    def param_copy(i):
        src, dst = ((mid_scale, h_scale), (mid_shift, h_shift))[i]
        return pltpu.make_async_remote_copy(
            src_ref=src, dst_ref=dst, send_sem=p_send.at[i], recv_sem=p_recv.at[i],
            device_id={"cp": right}, device_id_type=MESH,
        )

    barrier = pltpu.get_barrier_semaphore()
    for peer in peers:
        pl.semaphore_signal(barrier, inc=1, device_id={"cp": peer}, device_id_type=MESH)
    x_copies = [pltpu.make_async_copy(x_hbm.at[t], x_in.at[t], x_sem.at[t]) for t in range(N_FR)]
    for t in (1, 0):
        x_copies[t].start()
    small = ((bias_hbm, bias_ref), (in_scale_hbm, in_scale), (in_shift_hbm, in_shift),
             (mid_scale_hbm, mid_scale), (mid_shift_hbm, mid_shift))
    small_copies = [pltpu.make_async_copy(src, dst, s_sem.at[i]) for i, (src, dst) in enumerate(small)]
    for copy in small_copies:
        copy.start()
    for k in (2, 1, 0):
        w_copy(0, k).start()

    part[...] = jnp.zeros_like(part)
    acc[...] = jnp.zeros_like(acc)
    raw[2] = jnp.zeros((N_FR, N_ROW, N_COL, N_CH), BF16)
    for t in (1, 0):
        x_copies[t].wait()
        for p in range(N_ROW):
            val = x_in[t, p].astype(F32)
            for half in range(2):
                add_moments(val[:, half * HALF : (half + 1) * HALF], half)
    finish_moments(0)
    pl.semaphore_wait(barrier, cp_size - 1)
    for d in range(cp_size - 1):
        st_copy(0, d).start()

    for copy in small_copies:
        copy.wait()
    for b in range(2):
        for f in range(4):
            gains[2 * b, f : f + 1, :] = in_scale[b : b + 1, :]
            shifts[2 * b, f : f + 1, :] = in_shift[b : b + 1, :]
        gains[2 * b + 1, 2:4, :] = mid_scale[b]
        shifts[2 * b + 1, 2:4, :] = mid_shift[b]
    for t in (1, 0):
        for p in range(N_ROW):
            val = x_in[t, p].astype(F32)
            for j in range(4):
                tmp[p % 2, j] = val[:, j * 128 : (j + 1) * 128]
            for j in range(4):
                for v in range(N_TILE):
                    raw[0, t, p, v * TILE : (v + 1) * TILE, j * 128 : (j + 1) * 128] = tmp[
                        p % 2, j, pl.ds(v, TILE, stride=N_TILE), :
                    ].astype(BF16)
            if p % 2:
                piece = 2 * (1 - t) + p // 2

                @pl.when(jnp.logical_not(last))
                def _():
                    halo_copy(0, 0, piece).start()
                    if piece == len(PIECES) - 1:
                        for i in range(2):
                            param_copy(i).start()

    @pl.when(first)
    def _():
        for i in range(len(PIECES)):
            own_copy(0, 0, i).start()

    def conv(c, carry):
        par = lax.rem(c, 2)
        nxt = 1 - par

        @pl.when(c < N_CONV - 1)
        def _():
            for k in (2, 1, 0):
                w_copy(c + 1, k).start()

        for d in range(cp_size - 1):
            st_copy(par, d).wait()
        mean, rstd = statistics(par)
        coefficients(c, mean, rstd, (3,))

        def own(t):
            return lambda p, cut: raw[par, t, p, :, cut]

        def received(t):
            return lambda p, cut: halo[par, t, p, :, cut]

        def norms(read, f, halves=(0, 1), rows=range(N_ROW)):
            return [functools.partial(norm, read, f, p, h) for h in halves for p in rows]

        def epilogues(t, rows):
            return [functools.partial(epilogue, c, par, t, p, m) for p in rows for m in range(2)]

        for thunk in norms(own(1), 3, (0,), (0, 1)):
            thunk()

        @pl.when(c == 1)
        def _():
            @pl.when(jnp.logical_not(first))
            def _():
                for i in range(2):
                    param_copy(i).wait_recv()
                for b in range(2):
                    gains[2 * b + 1, 0:2, :] = h_scale[b]
                    shifts[2 * b + 1, 0:2, :] = h_shift[b]

            @pl.when(first)
            def _():
                for b in range(2):
                    for f in range(2):
                        gains[2 * b + 1, f : f + 1, :] = mid_scale[b, 0:1]
                        shifts[2 * b + 1, f : f + 1, :] = mid_shift[b, 0:1]

            @pl.when(jnp.logical_not(last))
            def _():
                for i in range(2):
                    param_copy(i).wait_send()

        coefficients(c, mean, rstd, (2, 1, 0))
        w_copy(c, 2).wait()
        w_copy(c, 1).wait()
        run(par, steps_of(1, 2, (0,), size=1), norms(own(1), 3, (0,), (2, 3)) + norms(own(1), 3, (1,)), 0.9)
        run(par, steps_of(1, 2, (1,)), norms(own(0), 2))
        run(par, steps_of(1, 1))
        w_copy(c, 0).wait()
        own_copy(par, par, 0).wait()
        steps = steps_of(0, 2)
        run(par, steps[:12], norms(received(1), 1, rows=(0, 1)), 0.9)
        own_copy(par, par, 1).wait()
        run(par, steps[12:], norms(received(1), 1, rows=(2, 3)), 0.9)
        run(par, steps_of(1, 0, dps=(1, -1)))
        for p in range(N_ROW):
            run(par, steps_of(1, 0, rows=(p, p + 1), dps=(0,)), epilogues(1, (p - 1,)) if p else ())
        steps = steps_of(0, 1)
        run(par, steps[:3], epilogues(1, (3,)))

        @pl.when(jnp.logical_and(c < N_CONV - 1, jnp.logical_not(last)))
        def _():
            halo_copy(nxt, nxt, 0).start()

        own_copy(par, par, 2).wait()
        run(par, steps[3:15], norms(received(0), 0, rows=(0, 1)), 0.9)
        own_copy(par, par, 3).wait()
        run(par, steps[15:], norms(received(0), 0, rows=(2, 3)), 0.9)
        run(par, steps_of(0, 0, dps=(1, -1)))
        for p in range(N_ROW):
            run(par, steps_of(0, 0, rows=(p, p + 1), dps=(0,)), epilogues(0, (p - 1,)) if p else ())
        for thunk in epilogues(0, (N_ROW - 1,)):
            thunk()
        finish_moments(nxt)

        @pl.when(c < N_CONV - 1)
        def _():
            for d in range(cp_size - 1):
                st_copy(nxt, d).start()

            @pl.when(jnp.logical_not(last))
            def _():
                for i in range(1, len(PIECES)):
                    halo_copy(nxt, nxt, i).start()

            @pl.when(first)
            def _():
                for i in range(len(PIECES)):
                    own_copy(nxt, nxt, i).start()

        @pl.when(jnp.logical_not(last))
        def _():
            for i in range(len(PIECES)):
                halo_copy(par, par, i).wait_send()

        return carry

    lax.fori_loop(0, N_CONV, conv, 0)

    out_ref[...] = raw[0]


def reorder(val_ref, out_hbm, tmp, buf, sem):
    copies = []
    for t in range(N_FR):
        for p in range(N_ROW):
            for j in range(4):
                cut = slice(j * 128, (j + 1) * 128)
                for v in range(N_TILE):
                    tmp[p % 2, j, pl.ds(v, TILE, stride=N_TILE), :] = val_ref[
                        t, p, v * TILE : (v + 1) * TILE, cut
                    ].astype(F32)
                buf[t, p, :, cut] = tmp[p % 2, j].astype(BF16)
            copies.append(pltpu.make_async_copy(buf.at[t, p], out_hbm.at[t, p], sem.at[t, p]))
            copies[-1].start()
    for copy in copies:
        copy.wait()


def solution(mesh):
    cp_size = mesh.shape["cp"]

    def local_decode(latent, conv_w, conv_b, in_scale, in_shift, mid_scale, mid_shift):
        any_spec, vmem = pl.BlockSpec(memory_space=pl.ANY), pl.BlockSpec(memory_space=pltpu.VMEM)
        dma = pltpu.SemaphoreType.DMA
        frame = (N_ROW, N_COL, N_CH)
        blocks = pl.pallas_call(
            functools.partial(kernel, cp_size),
            out_shape=jax.ShapeDtypeStruct(latent.shape, BF16),
            in_specs=[any_spec] * 7,
            out_specs=vmem,
            scratch_shapes=[
                pltpu.VMEM((N_CONV, N_CH), F32),
                pltpu.VMEM((2, N_CH), F32),
                pltpu.VMEM((2, N_CH), F32),
                pltpu.VMEM((2, N_FR, N_CH), F32),
                pltpu.VMEM((2, N_FR, N_CH), F32),
                pltpu.VMEM((N_FR, *frame), BF16),
                pltpu.VMEM((3, N_FR, *frame), BF16),
                pltpu.VMEM((2, N_FR, *frame), BF16),
                pltpu.VMEM((4, N_ROW, PAD_COL, N_CH), BF16),
                pltpu.VMEM((2, 3, 9 * N_CH, N_CH), BF16),
                pltpu.VMEM((N_FR, N_ROW, 2, N_COL, HALF), F32),
                pltpu.VMEM((2, 8, N_CH), F32),
                pltpu.VMEM((2, 8, 128), F32),
                pltpu.VMEM((2, cp_size - 1, 8, 128), F32),
                pltpu.VMEM((N_CONV, 4, N_CH), F32),
                pltpu.VMEM((N_CONV, 4, N_CH), F32),
                pltpu.VMEM((2, N_FR, N_CH), F32),
                pltpu.VMEM((2, N_FR, N_CH), F32),
                pltpu.VMEM((2, 4, N_CH), F32),
                pltpu.VMEM((2, 4, N_COL, 128), F32),
                dma((N_FR,)),
                dma((5,)),
                dma((2, 3)),
                dma((2, cp_size - 1)),
                dma((2, cp_size - 1)),
                dma((2, len(PIECES))),
                dma((2, len(PIECES))),
                dma((2,)),
                dma((2,)),
            ],
            compiler_params=pltpu.CompilerParams(
                collective_id=0, has_side_effects=True, vmem_limit_bytes=46 * 1024 * 1024
            ),
        )(*[
            pltpu.with_memory_space_constraint(arg, pltpu.HBM)
            for arg in (
                latent, conv_w.reshape(N_CONV, 3, 9 * N_CH, N_CH), conv_b, in_scale, in_shift, mid_scale, mid_shift
            )
        ])
        return pl.pallas_call(
            reorder,
            out_shape=jax.ShapeDtypeStruct(latent.shape, BF16),
            in_specs=[vmem],
            out_specs=any_spec,
            scratch_shapes=[
                pltpu.VMEM((2, 4, N_COL, 128), F32),
                pltpu.VMEM((N_FR, *frame), BF16),
                dma((N_FR, N_ROW)),
            ],
            compiler_params=pltpu.CompilerParams(vmem_limit_bytes=6 * 1024 * 1024),
        )(blocks)

    time_spec = P(("dp", "cp"))
    param_spec = P(None, ("dp", "cp"))
    return jax.shard_map(
        local_decode,
        mesh=mesh,
        in_specs=(time_spec, P(), P(), P(), P(), param_spec, param_spec),
        out_specs=time_spec,
        check_vma=False,
    )
```

```python
import functools

import jax
import jax.numpy as jnp
from jax import lax
from jax.experimental import pallas as pl
from jax.experimental.pallas import tpu as pltpu
from jax.sharding import PartitionSpec as P

NUM_GROUPS = 32
EPSILON = 1e-6
MESH = pl.DeviceIdType.MESH
F32 = jnp.float32
BF16 = jnp.bfloat16

N_CONV = 4
N_FR = 2
N_ROW = 4
N_COL = 128
N_CH = 512
TILE = 16
PIECES = ((1, slice(0, 2)), (1, slice(2, 4)), (0, slice(0, 2)), (0, slice(2, 4)))
N_TILE = N_COL // TILE
PAD_COL = N_COL + 2 * TILE
HALF = 256


def kernel(
    cp_size, x_hbm, w_hbm, bias_hbm, in_scale_hbm, in_shift_hbm, mid_scale_hbm, mid_shift_hbm, out_ref,
    bias_ref, in_scale, in_shift, mid_scale, mid_shift,
    x_in, raw, halo, act, wts, acc, part, tx, rx, gains, shifts, h_scale, h_shift, coef, tmp,
    x_sem, s_sem, w_sem, st_send, st_recv, h_send, h_recv, p_send, p_recv,
):
    cp = lax.axis_index("cp")
    count = float(N_FR * cp_size * N_ROW * N_COL * (N_CH // NUM_GROUPS))
    first, last = cp == 0, cp == cp_size - 1
    peers = [lax.rem(cp + d, cp_size) for d in range(1, cp_size)]
    right = lax.rem(cp + 1, cp_size)

    def mm_step(slot, t, k, low, high, dp, dq, kt):
        cut = slice(TILE * (1 + dq), TILE * (1 + dq) + N_COL)
        lhs = act[t + k, low + dp : high + dp, cut, kt * HALF : (kt + 1) * HALF].reshape((high - low) * N_COL, HALF)
        off = ((dp + 1) * 3 + dq + 1) * N_CH + kt * HALF
        for m in range(2):
            w = wts[slot, k, off : off + HALF, m * HALF : (m + 1) * HALF]
            out = jnp.dot(lhs, w, preferred_element_type=F32)
            for p in range(low, high):
                acc[t, p, m] += out[(p - low) * N_COL : (p - low + 1) * N_COL]

    def pop(m, t, p):
        val = acc[t, p, m]
        acc[t, p, m] = jnp.zeros((N_COL, HALF), F32)
        return val

    def steps_of(t, k, kts=(0, 1), rows=(0, N_ROW), dps=(0, 1, -1), size=N_ROW):
        return [
            (t, k, max(low, -dp), min(low + size, N_ROW - dp, rows[1]), dp, dq, kt)
            for kt in kts
            for low in range(rows[0], rows[1], size)
            for dp in dps
            if max(low, -dp) < min(low + size, N_ROW - dp, rows[1])
            for dq in (0, -1, 1)
        ]

    def run(slot, steps, thunks=(), upto=1.0):
        done, span = 0, max(1, int(len(steps) * upto))
        for i, step in enumerate(steps):
            mm_step(slot, *step)
            want = min(len(thunks), -(-len(thunks) * (i + 1) // span))
            for thunk in thunks[done:want]:
                thunk()
            done = want

    def add_moments(val, half):
        cut = slice(half * HALF, (half + 1) * HALF)
        rows = val.reshape(N_COL // 8, 8, HALF)
        part[0, :, cut] += jnp.sum(rows, axis=0)
        part[1, :, cut] += jnp.sum(rows * rows, axis=0)

    def norm(read, f, p, half):
        cut = slice(half * HALF, (half + 1) * HALF)
        val = read(p, cut).astype(F32) * coef[0, f : f + 1, cut] + coef[1, f : f + 1, cut]
        val = val.astype(BF16).astype(F32)
        val = val + val * jnp.tanh(val)
        act[f, p, TILE : TILE + N_COL, cut] = val.astype(BF16)
        row = lax.broadcasted_iota(jnp.int32, (TILE, HALF), 0)
        low = jnp.where(row == 0, 0.0, pltpu.roll(val[N_COL - TILE :], 1, 0))
        act[f, p, 0:TILE, cut] = low.astype(BF16)
        high = jnp.where(row == TILE - 1, 0.0, pltpu.roll(val[:TILE], TILE - 1, 0))
        act[f, p, TILE + N_COL :, cut] = high.astype(BF16)

    def epilogue(c, par, t, p, m):
        cut = slice(m * HALF, (m + 1) * HALF)
        conv = (pop(m, t, p) + bias_ref[pl.ds(c, 1), cut]).astype(BF16).astype(F32)
        val = (raw[2 - 2 * par, t, p, :, cut].astype(F32) + conv).astype(BF16)
        raw[1 - par, t, p, :, cut] = val
        add_moments(val.astype(F32), m)

    def finish_moments(slot):
        for i in range(2):
            total = jnp.sum(part[i], axis=0, keepdims=True)
            for j in range(4):
                tx[slot, 4 * i + j : 4 * i + j + 1, :] = total[:, j * 128 : (j + 1) * 128]
        part[...] = jnp.zeros_like(part)

    def statistics(slot):
        total = tx[slot]
        for d in range(cp_size - 1):
            total = total + rx[slot, d]
        lane = lax.broadcasted_iota(jnp.int32, total.shape, 1)
        size = N_CH // NUM_GROUPS
        spot = lane % size
        terms = [total]
        for d in range(1, size):
            terms.append(jnp.where(spot < size - d, pltpu.roll(total, 128 - d, 1), 0.0))
            terms.append(jnp.where(spot >= d, pltpu.roll(total, d, 1), 0.0))
        while len(terms) > 1:
            terms = [terms[i] + terms[i + 1] for i in range(0, len(terms) - 1, 2)] + terms[len(terms) & ~1 :]
        total = terms[0]
        mean = total[0:4] * (1.0 / count)
        var = total[4:8] * (1.0 / count) - mean * mean
        return mean, lax.rsqrt(var + EPSILON)

    def coefficients(c, mean, rstd, frames):
        for j in range(4):
            cut = slice(j * 128, (j + 1) * 128)
            for f in frames:
                gain = 0.5 * (rstd[j : j + 1] * gains[c, f : f + 1, cut])
                coef[0, f : f + 1, cut] = gain
                coef[1, f : f + 1, cut] = 0.5 * shifts[c, f : f + 1, cut] - mean[j : j + 1] * gain

    def w_copy(c, k):
        slot = lax.rem(c, 2)
        return pltpu.make_async_copy(w_hbm.at[c, k], wts.at[slot, k], w_sem.at[slot, k])

    def st_copy(slot, d):
        return pltpu.make_async_remote_copy(
            src_ref=tx.at[slot], dst_ref=rx.at[slot, d], send_sem=st_send.at[slot, d], recv_sem=st_recv.at[slot, d],
            device_id={"cp": peers[d]}, device_id_type=MESH,
        )

    def halo_copy(par, hs, i):
        t, rows = PIECES[i]
        return pltpu.make_async_remote_copy(
            src_ref=raw.at[par, t, rows], dst_ref=halo.at[hs, t, rows],
            send_sem=h_send.at[hs, i], recv_sem=h_recv.at[hs, i],
            device_id={"cp": right}, device_id_type=MESH,
        )

    def own_copy(par, hs, i):
        t, rows = PIECES[i]
        return pltpu.make_async_copy(raw.at[par, 0, rows], halo.at[hs, t, rows], h_recv.at[hs, i])

    def param_copy(i):
        src, dst = ((mid_scale, h_scale), (mid_shift, h_shift))[i]
        return pltpu.make_async_remote_copy(
            src_ref=src, dst_ref=dst, send_sem=p_send.at[i], recv_sem=p_recv.at[i],
            device_id={"cp": right}, device_id_type=MESH,
        )

    barrier = pltpu.get_barrier_semaphore()
    for peer in peers:
        pl.semaphore_signal(barrier, inc=1, device_id={"cp": peer}, device_id_type=MESH)
    x_copies = [pltpu.make_async_copy(x_hbm.at[t], x_in.at[t], x_sem.at[t]) for t in range(N_FR)]
    for t in (1, 0):
        x_copies[t].start()
    small = ((bias_hbm, bias_ref), (in_scale_hbm, in_scale), (in_shift_hbm, in_shift),
             (mid_scale_hbm, mid_scale), (mid_shift_hbm, mid_shift))
    small_copies = [pltpu.make_async_copy(src, dst, s_sem.at[i]) for i, (src, dst) in enumerate(small)]
    for copy in small_copies:
        copy.start()
    for k in (2, 1):
        w_copy(0, k).start()

    part[...] = jnp.zeros_like(part)
    acc[...] = jnp.zeros_like(acc)
    raw[2] = jnp.zeros((N_FR, N_ROW, N_COL, N_CH), BF16)
    for t in (1, 0):
        x_copies[t].wait()
        for p in range(N_ROW):
            val = x_in[t, p].astype(F32)
            for half in range(2):
                add_moments(val[:, half * HALF : (half + 1) * HALF], half)
    finish_moments(0)
    pl.semaphore_wait(barrier, cp_size - 1)
    for d in range(cp_size - 1):
        st_copy(0, d).start()

    for copy in small_copies:
        copy.wait()
    for b in range(2):
        for f in range(4):
            gains[2 * b, f : f + 1, :] = in_scale[b : b + 1, :]
            shifts[2 * b, f : f + 1, :] = in_shift[b : b + 1, :]
        gains[2 * b + 1, 2:4, :] = mid_scale[b]
        shifts[2 * b + 1, 2:4, :] = mid_shift[b]
    for t in (1, 0):
        for p in range(N_ROW):
            val = x_in[t, p].astype(F32)
            for j in range(4):
                tmp[p % 2, j] = val[:, j * 128 : (j + 1) * 128]
            for j in range(4):
                for v in range(N_TILE):
                    raw[0, t, p, v * TILE : (v + 1) * TILE, j * 128 : (j + 1) * 128] = tmp[
                        p % 2, j, pl.ds(v, TILE, stride=N_TILE), :
                    ].astype(BF16)
            if p % 2:
                piece = 2 * (1 - t) + p // 2

                @pl.when(jnp.logical_not(last))
                def _():
                    halo_copy(0, 0, piece).start()
                    if piece == len(PIECES) - 1:
                        for i in range(2):
                            param_copy(i).start()

    @pl.when(first)
    def _():
        for i in range(len(PIECES)):
            own_copy(0, 0, i).start()

    def conv(c, carry):
        par = lax.rem(c, 2)
        nxt = 1 - par

        for d in range(cp_size - 1):
            st_copy(par, d).wait()
        mean, rstd = statistics(par)
        coefficients(c, mean, rstd, (3,))

        def own(t):
            return lambda p, cut: raw[par, t, p, :, cut]

        def received(t):
            return lambda p, cut: halo[par, t, p, :, cut]

        def norms(read, f, halves=(0, 1), rows=range(N_ROW)):
            return [functools.partial(norm, read, f, p, h) for h in halves for p in rows]

        def epilogues(t, rows):
            return [functools.partial(epilogue, c, par, t, p, m) for p in rows for m in range(2)]

        for thunk in norms(own(1), 3, (0,), (0, 1)):
            thunk()

        @pl.when(c == 0)
        def _():
            w_copy(0, 0).start()

        @pl.when(c < N_CONV - 1)
        def _():
            for k in (2, 1, 0):
                w_copy(c + 1, k).start()

        @pl.when(c == 1)
        def _():
            @pl.when(jnp.logical_not(first))
            def _():
                for i in range(2):
                    param_copy(i).wait_recv()
                for b in range(2):
                    gains[2 * b + 1, 0:2, :] = h_scale[b]
                    shifts[2 * b + 1, 0:2, :] = h_shift[b]

            @pl.when(first)
            def _():
                for b in range(2):
                    for f in range(2):
                        gains[2 * b + 1, f : f + 1, :] = mid_scale[b, 0:1]
                        shifts[2 * b + 1, f : f + 1, :] = mid_shift[b, 0:1]

            @pl.when(jnp.logical_not(last))
            def _():
                for i in range(2):
                    param_copy(i).wait_send()

        coefficients(c, mean, rstd, (2, 1, 0))
        w_copy(c, 2).wait()
        w_copy(c, 1).wait()
        run(par, steps_of(1, 2, (0,), size=1), norms(own(1), 3, (0,), (2, 3)) + norms(own(1), 3, (1,)), 0.9)
        run(par, steps_of(1, 2, (1,)), norms(own(0), 2))
        run(par, steps_of(1, 1))
        steps = steps_of(0, 2)
        run(par, steps[:12])
        w_copy(c, 0).wait()
        own_copy(par, par, 0).wait()
        own_copy(par, par, 1).wait()
        run(par, steps[12:], norms(received(1), 1), 0.9)
        run(par, steps_of(1, 0, dps=(1, -1)))
        for p in range(N_ROW):
            run(par, steps_of(1, 0, rows=(p, p + 1), dps=(0,)), epilogues(1, (p - 1,)) if p else ())
        steps = steps_of(0, 1)
        run(par, steps[:3], epilogues(1, (3,)))

        @pl.when(jnp.logical_and(c < N_CONV - 1, jnp.logical_not(last)))
        def _():
            halo_copy(nxt, nxt, 0).start()

        own_copy(par, par, 2).wait()
        run(par, steps[3:15], norms(received(0), 0, rows=(0, 1)), 0.9)
        own_copy(par, par, 3).wait()
        run(par, steps[15:], norms(received(0), 0, rows=(2, 3)), 0.9)
        run(par, steps_of(0, 0, dps=(1, -1)))
        for p in range(N_ROW):
            run(par, steps_of(0, 0, rows=(p, p + 1), dps=(0,)), epilogues(0, (p - 1,)) if p else ())
        for thunk in epilogues(0, (N_ROW - 1,)):
            thunk()
        finish_moments(nxt)

        @pl.when(c < N_CONV - 1)
        def _():
            for d in range(cp_size - 1):
                st_copy(nxt, d).start()

            @pl.when(jnp.logical_not(last))
            def _():
                for i in range(1, len(PIECES)):
                    halo_copy(nxt, nxt, i).start()

            @pl.when(first)
            def _():
                for i in range(len(PIECES)):
                    own_copy(nxt, nxt, i).start()

        @pl.when(jnp.logical_not(last))
        def _():
            for i in range(len(PIECES)):
                halo_copy(par, par, i).wait_send()

        return carry

    lax.fori_loop(0, N_CONV, conv, 0)

    out_ref[...] = raw[0]


def reorder(val_ref, out_hbm, tmp, buf, sem):
    copies = []
    for t in range(N_FR):
        for p in range(N_ROW):
            for j in range(4):
                cut = slice(j * 128, (j + 1) * 128)
                for v in range(N_TILE):
                    tmp[p % 2, j, pl.ds(v, TILE, stride=N_TILE), :] = val_ref[
                        t, p, v * TILE : (v + 1) * TILE, cut
                    ].astype(F32)
                buf[t, p, :, cut] = tmp[p % 2, j].astype(BF16)
            copies.append(pltpu.make_async_copy(buf.at[t, p], out_hbm.at[t, p], sem.at[t, p]))
            copies[-1].start()
    for copy in copies:
        copy.wait()


def solution(mesh):
    cp_size = mesh.shape["cp"]

    def local_decode(latent, conv_w, conv_b, in_scale, in_shift, mid_scale, mid_shift):
        any_spec, vmem = pl.BlockSpec(memory_space=pl.ANY), pl.BlockSpec(memory_space=pltpu.VMEM)
        dma = pltpu.SemaphoreType.DMA
        frame = (N_ROW, N_COL, N_CH)
        blocks = pl.pallas_call(
            functools.partial(kernel, cp_size),
            out_shape=jax.ShapeDtypeStruct(latent.shape, BF16),
            in_specs=[any_spec] * 7,
            out_specs=vmem,
            scratch_shapes=[
                pltpu.VMEM((N_CONV, N_CH), F32),
                pltpu.VMEM((2, N_CH), F32),
                pltpu.VMEM((2, N_CH), F32),
                pltpu.VMEM((2, N_FR, N_CH), F32),
                pltpu.VMEM((2, N_FR, N_CH), F32),
                pltpu.VMEM((N_FR, *frame), BF16),
                pltpu.VMEM((3, N_FR, *frame), BF16),
                pltpu.VMEM((2, N_FR, *frame), BF16),
                pltpu.VMEM((4, N_ROW, PAD_COL, N_CH), BF16),
                pltpu.VMEM((2, 3, 9 * N_CH, N_CH), BF16),
                pltpu.VMEM((N_FR, N_ROW, 2, N_COL, HALF), F32),
                pltpu.VMEM((2, 8, N_CH), F32),
                pltpu.VMEM((2, 8, 128), F32),
                pltpu.VMEM((2, cp_size - 1, 8, 128), F32),
                pltpu.VMEM((N_CONV, 4, N_CH), F32),
                pltpu.VMEM((N_CONV, 4, N_CH), F32),
                pltpu.VMEM((2, N_FR, N_CH), F32),
                pltpu.VMEM((2, N_FR, N_CH), F32),
                pltpu.VMEM((2, 4, N_CH), F32),
                pltpu.VMEM((2, 4, N_COL, 128), F32),
                dma((N_FR,)),
                dma((5,)),
                dma((2, 3)),
                dma((2, cp_size - 1)),
                dma((2, cp_size - 1)),
                dma((2, len(PIECES))),
                dma((2, len(PIECES))),
                dma((2,)),
                dma((2,)),
            ],
            compiler_params=pltpu.CompilerParams(
                collective_id=0, has_side_effects=True, vmem_limit_bytes=46 * 1024 * 1024
            ),
        )(*[
            pltpu.with_memory_space_constraint(arg, pltpu.HBM)
            for arg in (
                latent, conv_w.reshape(N_CONV, 3, 9 * N_CH, N_CH), conv_b, in_scale, in_shift, mid_scale, mid_shift
            )
        ])
        return pl.pallas_call(
            reorder,
            out_shape=jax.ShapeDtypeStruct(latent.shape, BF16),
            in_specs=[vmem],
            out_specs=any_spec,
            scratch_shapes=[
                pltpu.VMEM((2, 4, N_COL, 128), F32),
                pltpu.VMEM((N_FR, *frame), BF16),
                dma((N_FR, N_ROW)),
            ],
            compiler_params=pltpu.CompilerParams(vmem_limit_bytes=6 * 1024 * 1024),
        )(blocks)

    time_spec = P(("dp", "cp"))
    param_spec = P(None, ("dp", "cp"))
    return jax.shard_map(
        local_decode,
        mesh=mesh,
        in_specs=(time_spec, P(), P(), P(), P(), param_spec, param_spec),
        out_specs=time_spec,
        check_vma=False,
    )
```

```python
import functools

import jax
import jax.numpy as jnp
from jax import lax
from jax.experimental import pallas as pl
from jax.experimental.pallas import tpu as pltpu
from jax.sharding import PartitionSpec as P

NUM_GROUPS = 32
EPSILON = 1e-6
MESH = pl.DeviceIdType.MESH
F32 = jnp.float32
BF16 = jnp.bfloat16

N_CONV = 4
N_FR = 2
N_ROW = 4
N_COL = 128
N_CH = 512
TILE = 16
PIECES = ((1, slice(0, 2)), (1, slice(2, 4)), (0, slice(0, 2)), (0, slice(2, 4)))
N_TILE = N_COL // TILE
PAD_COL = N_COL + 2 * TILE
HALF = 256


def kernel(
    cp_size, x_hbm, w_hbm, bias_hbm, in_scale_hbm, in_shift_hbm, mid_scale_hbm, mid_shift_hbm, out_ref,
    bias_ref, in_scale, in_shift, mid_scale, mid_shift,
    x_in, raw, halo, act, wts, acc, part, tx, rx, gains, shifts, h_scale, h_shift, coef, tmp,
    x_sem, s_sem, w_sem, st_send, st_recv, h_send, h_recv, p_send, p_recv,
):
    cp = lax.axis_index("cp")
    count = float(N_FR * cp_size * N_ROW * N_COL * (N_CH // NUM_GROUPS))
    first, last = cp == 0, cp == cp_size - 1
    peers = [lax.rem(cp + d, cp_size) for d in range(1, cp_size)]
    right = lax.rem(cp + 1, cp_size)

    def mm_step(slot, t, k, low, high, dp, dq, kt):
        cut = slice(TILE * (1 + dq), TILE * (1 + dq) + N_COL)
        lhs = act[t + k, low + dp : high + dp, cut, kt * HALF : (kt + 1) * HALF].reshape((high - low) * N_COL, HALF)
        off = ((dp + 1) * 3 + dq + 1) * N_CH + kt * HALF
        for m in range(2):
            w = wts[slot, k, off : off + HALF, m * HALF : (m + 1) * HALF]
            out = jnp.dot(lhs, w, preferred_element_type=F32)
            for p in range(low, high):
                acc[t, p, m] += out[(p - low) * N_COL : (p - low + 1) * N_COL]

    def pop(m, t, p):
        val = acc[t, p, m]
        acc[t, p, m] = jnp.zeros((N_COL, HALF), F32)
        return val

    def steps_of(t, k, kts=(0, 1), rows=(0, N_ROW), dps=(0, 1, -1), size=N_ROW):
        return [
            (t, k, max(low, -dp), min(low + size, N_ROW - dp, rows[1]), dp, dq, kt)
            for kt in kts
            for low in range(rows[0], rows[1], size)
            for dp in dps
            if max(low, -dp) < min(low + size, N_ROW - dp, rows[1])
            for dq in (0, -1, 1)
        ]

    def run(slot, steps, thunks=(), upto=1.0):
        done, span = 0, max(1, int(len(steps) * upto))
        for i, step in enumerate(steps):
            mm_step(slot, *step)
            want = min(len(thunks), -(-len(thunks) * (i + 1) // span))
            for thunk in thunks[done:want]:
                thunk()
            done = want

    def add_moments(val, half):
        cut = slice(half * HALF, (half + 1) * HALF)
        rows = val.reshape(N_COL // 8, 8, HALF)
        part[0, :, cut] += jnp.sum(rows, axis=0)
        part[1, :, cut] += jnp.sum(rows * rows, axis=0)

    def norm(read, f, p, half):
        cut = slice(half * HALF, (half + 1) * HALF)
        val = read(p, cut).astype(F32) * coef[0, f : f + 1, cut] + coef[1, f : f + 1, cut]
        val = val.astype(BF16).astype(F32)
        val = val + val * jnp.tanh(val)
        act[f, p, TILE : TILE + N_COL, cut] = val.astype(BF16)
        row = lax.broadcasted_iota(jnp.int32, (TILE, HALF), 0)
        low = jnp.where(row == 0, 0.0, pltpu.roll(val[N_COL - TILE :], 1, 0))
        act[f, p, 0:TILE, cut] = low.astype(BF16)
        high = jnp.where(row == TILE - 1, 0.0, pltpu.roll(val[:TILE], TILE - 1, 0))
        act[f, p, TILE + N_COL :, cut] = high.astype(BF16)

    def epilogue(c, par, t, p, m):
        cut = slice(m * HALF, (m + 1) * HALF)
        conv = (pop(m, t, p) + bias_ref[pl.ds(c, 1), cut]).astype(BF16).astype(F32)
        val = (raw[2 - 2 * par, t, p, :, cut].astype(F32) + conv).astype(BF16)
        raw[1 - par, t, p, :, cut] = val
        add_moments(val.astype(F32), m)

    def finish_moments(slot):
        for i in range(2):
            total = jnp.sum(part[i], axis=0, keepdims=True)
            for j in range(4):
                tx[slot, 4 * i + j : 4 * i + j + 1, :] = total[:, j * 128 : (j + 1) * 128]
        part[...] = jnp.zeros_like(part)

    def statistics(slot):
        total = tx[slot]
        for d in range(cp_size - 1):
            total = total + rx[slot, d]
        lane = lax.broadcasted_iota(jnp.int32, total.shape, 1)
        size = N_CH // NUM_GROUPS
        spot = lane % size
        terms = [total]
        for d in range(1, size):
            terms.append(jnp.where(spot < size - d, pltpu.roll(total, 128 - d, 1), 0.0))
            terms.append(jnp.where(spot >= d, pltpu.roll(total, d, 1), 0.0))
        while len(terms) > 1:
            terms = [terms[i] + terms[i + 1] for i in range(0, len(terms) - 1, 2)] + terms[len(terms) & ~1 :]
        total = terms[0]
        mean = total[0:4] * (1.0 / count)
        var = total[4:8] * (1.0 / count) - mean * mean
        return mean, lax.rsqrt(var + EPSILON)

    def coefficients(c, mean, rstd, frames):
        for j in range(4):
            cut = slice(j * 128, (j + 1) * 128)
            for f in frames:
                gain = 0.5 * (rstd[j : j + 1] * gains[c, f : f + 1, cut])
                coef[0, f : f + 1, cut] = gain
                coef[1, f : f + 1, cut] = 0.5 * shifts[c, f : f + 1, cut] - mean[j : j + 1] * gain

    def w_copy(c, k):
        slot = lax.rem(c, 2)
        return pltpu.make_async_copy(w_hbm.at[c, k], wts.at[slot, k], w_sem.at[slot, k])

    def st_copy(slot, d):
        return pltpu.make_async_remote_copy(
            src_ref=tx.at[slot], dst_ref=rx.at[slot, d], send_sem=st_send.at[slot, d], recv_sem=st_recv.at[slot, d],
            device_id={"cp": peers[d]}, device_id_type=MESH,
        )

    def halo_copy(par, hs, i):
        t, rows = PIECES[i]
        return pltpu.make_async_remote_copy(
            src_ref=raw.at[par, t, rows], dst_ref=halo.at[hs, t, rows],
            send_sem=h_send.at[hs, i], recv_sem=h_recv.at[hs, i],
            device_id={"cp": right}, device_id_type=MESH,
        )

    def own_copy(par, hs, i):
        t, rows = PIECES[i]
        return pltpu.make_async_copy(raw.at[par, 0, rows], halo.at[hs, t, rows], h_recv.at[hs, i])

    def param_copy(i):
        src, dst = ((mid_scale, h_scale), (mid_shift, h_shift))[i]
        return pltpu.make_async_remote_copy(
            src_ref=src, dst_ref=dst, send_sem=p_send.at[i], recv_sem=p_recv.at[i],
            device_id={"cp": right}, device_id_type=MESH,
        )

    barrier = pltpu.get_barrier_semaphore()
    for peer in peers:
        pl.semaphore_signal(barrier, inc=1, device_id={"cp": peer}, device_id_type=MESH)
    x_copies = [pltpu.make_async_copy(x_hbm.at[t], x_in.at[t], x_sem.at[t]) for t in range(N_FR)]
    for t in (1, 0):
        x_copies[t].start()
    small = ((bias_hbm, bias_ref), (in_scale_hbm, in_scale), (in_shift_hbm, in_shift),
             (mid_scale_hbm, mid_scale), (mid_shift_hbm, mid_shift))
    small_copies = [pltpu.make_async_copy(src, dst, s_sem.at[i]) for i, (src, dst) in enumerate(small)]
    for copy in small_copies:
        copy.start()

    part[...] = jnp.zeros_like(part)
    acc[...] = jnp.zeros_like(acc)
    raw[2] = jnp.zeros((N_FR, N_ROW, N_COL, N_CH), BF16)
    for t in (1, 0):
        x_copies[t].wait()
        for p in range(N_ROW):
            val = x_in[t, p].astype(F32)
            for half in range(2):
                add_moments(val[:, half * HALF : (half + 1) * HALF], half)
    finish_moments(0)
    pl.semaphore_wait(barrier, cp_size - 1)
    for d in range(cp_size - 1):
        st_copy(0, d).start()
    w_copy(0, 2).start()

    for copy in small_copies:
        copy.wait()
    for b in range(2):
        for f in range(4):
            gains[2 * b, f : f + 1, :] = in_scale[b : b + 1, :]
            shifts[2 * b, f : f + 1, :] = in_shift[b : b + 1, :]
        gains[2 * b + 1, 2:4, :] = mid_scale[b]
        shifts[2 * b + 1, 2:4, :] = mid_shift[b]
    for t in (1, 0):
        for p in range(N_ROW):
            val = x_in[t, p].astype(F32)
            for j in range(4):
                tmp[p % 2, j] = val[:, j * 128 : (j + 1) * 128]
            for j in range(4):
                for v in range(N_TILE):
                    raw[0, t, p, v * TILE : (v + 1) * TILE, j * 128 : (j + 1) * 128] = tmp[
                        p % 2, j, pl.ds(v, TILE, stride=N_TILE), :
                    ].astype(BF16)
            if p % 2:
                piece = 2 * (1 - t) + p // 2

                @pl.when(jnp.logical_not(last))
                def _():
                    halo_copy(0, 0, piece).start()
                    if piece == len(PIECES) - 1:
                        for i in range(2):
                            param_copy(i).start()

    @pl.when(first)
    def _():
        for i in range(len(PIECES)):
            own_copy(0, 0, i).start()

    def conv(c, carry):
        par = lax.rem(c, 2)
        nxt = 1 - par

        for d in range(cp_size - 1):
            st_copy(par, d).wait()
        mean, rstd = statistics(par)
        coefficients(c, mean, rstd, (3,))

        def own(t):
            return lambda p, cut: raw[par, t, p, :, cut]

        def received(t):
            return lambda p, cut: halo[par, t, p, :, cut]

        def norms(read, f, halves=(0, 1), rows=range(N_ROW)):
            return [functools.partial(norm, read, f, p, h) for h in halves for p in rows]

        def epilogues(t, rows):
            return [functools.partial(epilogue, c, par, t, p, m) for p in rows for m in range(2)]

        for thunk in norms(own(1), 3, (0,), (0, 1)):
            thunk()

        @pl.when(c == 0)
        def _():
            for k in (1, 0):
                w_copy(0, k).start()

        @pl.when(c < N_CONV - 1)
        def _():
            for k in (2, 1, 0):
                w_copy(c + 1, k).start()

        @pl.when(c == 1)
        def _():
            @pl.when(jnp.logical_not(first))
            def _():
                for i in range(2):
                    param_copy(i).wait_recv()
                for b in range(2):
                    gains[2 * b + 1, 0:2, :] = h_scale[b]
                    shifts[2 * b + 1, 0:2, :] = h_shift[b]

            @pl.when(first)
            def _():
                for b in range(2):
                    for f in range(2):
                        gains[2 * b + 1, f : f + 1, :] = mid_scale[b, 0:1]
                        shifts[2 * b + 1, f : f + 1, :] = mid_shift[b, 0:1]

            @pl.when(jnp.logical_not(last))
            def _():
                for i in range(2):
                    param_copy(i).wait_send()

        coefficients(c, mean, rstd, (2, 1, 0))
        w_copy(c, 2).wait()
        run(par, steps_of(1, 2, (0,), size=1), norms(own(1), 3, (0,), (2, 3)) + norms(own(1), 3, (1,)), 0.9)
        run(par, steps_of(1, 2, (1,)), norms(own(0), 2))
        w_copy(c, 1).wait()
        run(par, steps_of(1, 1))
        steps = steps_of(0, 2)
        run(par, steps[:12])
        w_copy(c, 0).wait()
        own_copy(par, par, 0).wait()
        own_copy(par, par, 1).wait()
        run(par, steps[12:], norms(received(1), 1), 0.9)
        run(par, steps_of(1, 0, dps=(1, -1)))
        for p in range(N_ROW):
            run(par, steps_of(1, 0, rows=(p, p + 1), dps=(0,)), epilogues(1, (p - 1,)) if p else ())
        steps = steps_of(0, 1)
        run(par, steps[:3], epilogues(1, (3,)))

        @pl.when(jnp.logical_and(c < N_CONV - 1, jnp.logical_not(last)))
        def _():
            halo_copy(nxt, nxt, 0).start()

        own_copy(par, par, 2).wait()
        run(par, steps[3:15], norms(received(0), 0, rows=(0, 1)), 0.9)
        own_copy(par, par, 3).wait()
        run(par, steps[15:], norms(received(0), 0, rows=(2, 3)), 0.9)
        run(par, steps_of(0, 0, dps=(1, -1)))
        for p in range(N_ROW):
            run(par, steps_of(0, 0, rows=(p, p + 1), dps=(0,)), epilogues(0, (p - 1,)) if p else ())
        for thunk in epilogues(0, (N_ROW - 1,)):
            thunk()
        finish_moments(nxt)

        @pl.when(c < N_CONV - 1)
        def _():
            for d in range(cp_size - 1):
                st_copy(nxt, d).start()

            @pl.when(jnp.logical_not(last))
            def _():
                for i in range(1, len(PIECES)):
                    halo_copy(nxt, nxt, i).start()

            @pl.when(first)
            def _():
                for i in range(len(PIECES)):
                    own_copy(nxt, nxt, i).start()

        @pl.when(jnp.logical_not(last))
        def _():
            for i in range(len(PIECES)):
                halo_copy(par, par, i).wait_send()

        return carry

    lax.fori_loop(0, N_CONV, conv, 0)

    out_ref[...] = raw[0]


def reorder(val_ref, out_hbm, tmp, buf, sem):
    copies = []
    for t in range(N_FR):
        for p in range(N_ROW):
            for j in range(4):
                cut = slice(j * 128, (j + 1) * 128)
                for v in range(N_TILE):
                    tmp[p % 2, j, pl.ds(v, TILE, stride=N_TILE), :] = val_ref[
                        t, p, v * TILE : (v + 1) * TILE, cut
                    ].astype(F32)
                buf[t, p, :, cut] = tmp[p % 2, j].astype(BF16)
            copies.append(pltpu.make_async_copy(buf.at[t, p], out_hbm.at[t, p], sem.at[t, p]))
            copies[-1].start()
    for copy in copies:
        copy.wait()


def solution(mesh):
    cp_size = mesh.shape["cp"]

    def local_decode(latent, conv_w, conv_b, in_scale, in_shift, mid_scale, mid_shift):
        any_spec, vmem = pl.BlockSpec(memory_space=pl.ANY), pl.BlockSpec(memory_space=pltpu.VMEM)
        dma = pltpu.SemaphoreType.DMA
        frame = (N_ROW, N_COL, N_CH)
        blocks = pl.pallas_call(
            functools.partial(kernel, cp_size),
            out_shape=jax.ShapeDtypeStruct(latent.shape, BF16),
            in_specs=[any_spec] * 7,
            out_specs=vmem,
            scratch_shapes=[
                pltpu.VMEM((N_CONV, N_CH), F32),
                pltpu.VMEM((2, N_CH), F32),
                pltpu.VMEM((2, N_CH), F32),
                pltpu.VMEM((2, N_FR, N_CH), F32),
                pltpu.VMEM((2, N_FR, N_CH), F32),
                pltpu.VMEM((N_FR, *frame), BF16),
                pltpu.VMEM((3, N_FR, *frame), BF16),
                pltpu.VMEM((2, N_FR, *frame), BF16),
                pltpu.VMEM((4, N_ROW, PAD_COL, N_CH), BF16),
                pltpu.VMEM((2, 3, 9 * N_CH, N_CH), BF16),
                pltpu.VMEM((N_FR, N_ROW, 2, N_COL, HALF), F32),
                pltpu.VMEM((2, 8, N_CH), F32),
                pltpu.VMEM((2, 8, 128), F32),
                pltpu.VMEM((2, cp_size - 1, 8, 128), F32),
                pltpu.VMEM((N_CONV, 4, N_CH), F32),
                pltpu.VMEM((N_CONV, 4, N_CH), F32),
                pltpu.VMEM((2, N_FR, N_CH), F32),
                pltpu.VMEM((2, N_FR, N_CH), F32),
                pltpu.VMEM((2, 4, N_CH), F32),
                pltpu.VMEM((2, 4, N_COL, 128), F32),
                dma((N_FR,)),
                dma((5,)),
                dma((2, 3)),
                dma((2, cp_size - 1)),
                dma((2, cp_size - 1)),
                dma((2, len(PIECES))),
                dma((2, len(PIECES))),
                dma((2,)),
                dma((2,)),
            ],
            compiler_params=pltpu.CompilerParams(
                collective_id=0, has_side_effects=True, vmem_limit_bytes=46 * 1024 * 1024
            ),
        )(*[
            pltpu.with_memory_space_constraint(arg, pltpu.HBM)
            for arg in (
                latent, conv_w.reshape(N_CONV, 3, 9 * N_CH, N_CH), conv_b, in_scale, in_shift, mid_scale, mid_shift
            )
        ])
        return pl.pallas_call(
            reorder,
            out_shape=jax.ShapeDtypeStruct(latent.shape, BF16),
            in_specs=[vmem],
            out_specs=any_spec,
            scratch_shapes=[
                pltpu.VMEM((2, 4, N_COL, 128), F32),
                pltpu.VMEM((N_FR, *frame), BF16),
                dma((N_FR, N_ROW)),
            ],
            compiler_params=pltpu.CompilerParams(vmem_limit_bytes=6 * 1024 * 1024),
        )(blocks)

    time_spec = P(("dp", "cp"))
    param_spec = P(None, ("dp", "cp"))
    return jax.shard_map(
        local_decode,
        mesh=mesh,
        in_specs=(time_spec, P(), P(), P(), P(), param_spec, param_spec),
        out_specs=time_spec,
        check_vma=False,
    )
```

```python
import functools

import jax
import jax.numpy as jnp
from jax import lax
from jax.experimental import pallas as pl
from jax.experimental.pallas import tpu as pltpu
from jax.sharding import PartitionSpec as P

NUM_GROUPS = 32
EPSILON = 1e-6
MESH = pl.DeviceIdType.MESH
F32 = jnp.float32
BF16 = jnp.bfloat16

N_CONV = 4
N_FR = 2
N_ROW = 4
N_COL = 128
N_CH = 512
TILE = 16
PIECES = ((1, slice(0, 2)), (1, slice(2, 4)), (0, slice(0, 2)), (0, slice(2, 4)))
N_TILE = N_COL // TILE
PAD_COL = N_COL + 2 * TILE
HALF = 256


def kernel(
    cp_size, x_hbm, w_hbm, bias_hbm, in_scale_hbm, in_shift_hbm, mid_scale_hbm, mid_shift_hbm, out_ref,
    bias_ref, in_scale, in_shift, mid_scale, mid_shift,
    x_in, raw, halo, act, wts, acc, part, tx, rx, gains, shifts, h_scale, h_shift, coef, tmp,
    x_sem, s_sem, w_sem, st_send, st_recv, h_send, h_recv, p_send, p_recv,
):
    cp = lax.axis_index("cp")
    count = float(N_FR * cp_size * N_ROW * N_COL * (N_CH // NUM_GROUPS))
    first, last = cp == 0, cp == cp_size - 1
    peers = [lax.rem(cp + d, cp_size) for d in range(1, cp_size)]
    right = lax.rem(cp + 1, cp_size)

    def mm_step(slot, t, k, low, high, dp, dq, kt):
        cut = slice(TILE * (1 + dq), TILE * (1 + dq) + N_COL)
        lhs = act[t + k, low + dp : high + dp, cut, kt * HALF : (kt + 1) * HALF].reshape((high - low) * N_COL, HALF)
        off = ((dp + 1) * 3 + dq + 1) * N_CH + kt * HALF
        for m in range(2):
            w = wts[slot, k, off : off + HALF, m * HALF : (m + 1) * HALF]
            out = jnp.dot(lhs, w, preferred_element_type=F32)
            for p in range(low, high):
                acc[t, p, m] += out[(p - low) * N_COL : (p - low + 1) * N_COL]

    def pop(m, t, p):
        val = acc[t, p, m]
        acc[t, p, m] = jnp.zeros((N_COL, HALF), F32)
        return val

    def steps_of(t, k, kts=(0, 1), rows=(0, N_ROW), dps=(0, 1, -1), size=N_ROW):
        return [
            (t, k, max(low, -dp), min(low + size, N_ROW - dp, rows[1]), dp, dq, kt)
            for kt in kts
            for low in range(rows[0], rows[1], size)
            for dp in dps
            if max(low, -dp) < min(low + size, N_ROW - dp, rows[1])
            for dq in (0, -1, 1)
        ]

    def run(slot, steps, thunks=(), upto=1.0):
        done, span = 0, max(1, int(len(steps) * upto))
        for i, step in enumerate(steps):
            mm_step(slot, *step)
            want = min(len(thunks), -(-len(thunks) * (i + 1) // span))
            for thunk in thunks[done:want]:
                thunk()
            done = want

    def add_moments(val, half):
        cut = slice(half * HALF, (half + 1) * HALF)
        rows = val.reshape(N_COL // 8, 8, HALF)
        part[0, :, cut] += jnp.sum(rows, axis=0)
        part[1, :, cut] += jnp.sum(rows * rows, axis=0)

    def norm(read, f, p, half):
        cut = slice(half * HALF, (half + 1) * HALF)
        val = read(p, cut).astype(F32) * coef[0, f : f + 1, cut] + coef[1, f : f + 1, cut]
        val = val.astype(BF16).astype(F32)
        val = val + val * jnp.tanh(val)
        act[f, p, TILE : TILE + N_COL, cut] = val.astype(BF16)
        row = lax.broadcasted_iota(jnp.int32, (TILE, HALF), 0)
        low = jnp.where(row == 0, 0.0, pltpu.roll(val[N_COL - TILE :], 1, 0))
        act[f, p, 0:TILE, cut] = low.astype(BF16)
        high = jnp.where(row == TILE - 1, 0.0, pltpu.roll(val[:TILE], TILE - 1, 0))
        act[f, p, TILE + N_COL :, cut] = high.astype(BF16)

    def epilogue(c, par, t, p, m):
        cut = slice(m * HALF, (m + 1) * HALF)
        conv = (pop(m, t, p) + bias_ref[pl.ds(c, 1), cut]).astype(BF16).astype(F32)
        val = (raw[2 - 2 * par, t, p, :, cut].astype(F32) + conv).astype(BF16)
        raw[1 - par, t, p, :, cut] = val
        add_moments(val.astype(F32), m)

    def finish_moments(slot):
        for i in range(2):
            total = jnp.sum(part[i], axis=0, keepdims=True)
            for j in range(4):
                tx[slot, 4 * i + j : 4 * i + j + 1, :] = total[:, j * 128 : (j + 1) * 128]
        part[...] = jnp.zeros_like(part)

    def statistics(slot):
        total = tx[slot]
        for d in range(cp_size - 1):
            total = total + rx[slot, d]
        lane = lax.broadcasted_iota(jnp.int32, total.shape, 1)
        size = N_CH // NUM_GROUPS
        spot = lane % size
        terms = [total]
        for d in range(1, size):
            terms.append(jnp.where(spot < size - d, pltpu.roll(total, 128 - d, 1), 0.0))
            terms.append(jnp.where(spot >= d, pltpu.roll(total, d, 1), 0.0))
        while len(terms) > 1:
            terms = [terms[i] + terms[i + 1] for i in range(0, len(terms) - 1, 2)] + terms[len(terms) & ~1 :]
        total = terms[0]
        mean = total[0:4] * (1.0 / count)
        var = total[4:8] * (1.0 / count) - mean * mean
        return mean, lax.rsqrt(var + EPSILON)

    def coefficients(c, mean, rstd, frames):
        for j in range(4):
            cut = slice(j * 128, (j + 1) * 128)
            for f in frames:
                gain = 0.5 * (rstd[j : j + 1] * gains[c, f : f + 1, cut])
                coef[0, f : f + 1, cut] = gain
                coef[1, f : f + 1, cut] = 0.5 * shifts[c, f : f + 1, cut] - mean[j : j + 1] * gain

    def w_copy(c, k):
        slot = lax.rem(c, 2)
        return pltpu.make_async_copy(w_hbm.at[c, k], wts.at[slot, k], w_sem.at[slot, k])

    def st_copy(slot, d):
        return pltpu.make_async_remote_copy(
            src_ref=tx.at[slot], dst_ref=rx.at[slot, d], send_sem=st_send.at[slot, d], recv_sem=st_recv.at[slot, d],
            device_id={"cp": peers[d]}, device_id_type=MESH,
        )

    def halo_copy(par, hs, i):
        t, rows = PIECES[i]
        return pltpu.make_async_remote_copy(
            src_ref=raw.at[par, t, rows], dst_ref=halo.at[hs, t, rows],
            send_sem=h_send.at[hs, i], recv_sem=h_recv.at[hs, i],
            device_id={"cp": right}, device_id_type=MESH,
        )

    def own_copy(par, hs, i):
        t, rows = PIECES[i]
        return pltpu.make_async_copy(raw.at[par, 0, rows], halo.at[hs, t, rows], h_recv.at[hs, i])

    def param_copy(i):
        src, dst = ((mid_scale, h_scale), (mid_shift, h_shift))[i]
        return pltpu.make_async_remote_copy(
            src_ref=src, dst_ref=dst, send_sem=p_send.at[i], recv_sem=p_recv.at[i],
            device_id={"cp": right}, device_id_type=MESH,
        )

    barrier = pltpu.get_barrier_semaphore()
    for peer in peers:
        pl.semaphore_signal(barrier, inc=1, device_id={"cp": peer}, device_id_type=MESH)
    x_copies = [pltpu.make_async_copy(x_hbm.at[t], x_in.at[t], x_sem.at[t]) for t in range(N_FR)]
    for t in (1, 0):
        x_copies[t].start()
    small = ((bias_hbm, bias_ref), (in_scale_hbm, in_scale), (in_shift_hbm, in_shift),
             (mid_scale_hbm, mid_scale), (mid_shift_hbm, mid_shift))
    small_copies = [pltpu.make_async_copy(src, dst, s_sem.at[i]) for i, (src, dst) in enumerate(small)]
    for copy in small_copies:
        copy.start()

    part[...] = jnp.zeros_like(part)
    acc[...] = jnp.zeros_like(acc)
    raw[2] = jnp.zeros((N_FR, N_ROW, N_COL, N_CH), BF16)
    for t in (1, 0):
        x_copies[t].wait()
        for p in range(N_ROW):
            val = x_in[t, p].astype(F32)
            for half in range(2):
                add_moments(val[:, half * HALF : (half + 1) * HALF], half)
    finish_moments(0)
    pl.semaphore_wait(barrier, cp_size - 1)
    for d in range(cp_size - 1):
        st_copy(0, d).start()
    w_copy(0, 2).start()

    for copy in small_copies:
        copy.wait()
    for b in range(2):
        for f in range(4):
            gains[2 * b, f : f + 1, :] = in_scale[b : b + 1, :]
            shifts[2 * b, f : f + 1, :] = in_shift[b : b + 1, :]
        gains[2 * b + 1, 2:4, :] = mid_scale[b]
        shifts[2 * b + 1, 2:4, :] = mid_shift[b]
    for t in (1, 0):
        for p in range(N_ROW):
            val = x_in[t, p].astype(F32)
            for j in range(4):
                tmp[p % 2, j] = val[:, j * 128 : (j + 1) * 128]
            for j in range(4):
                for v in range(N_TILE):
                    raw[0, t, p, v * TILE : (v + 1) * TILE, j * 128 : (j + 1) * 128] = tmp[
                        p % 2, j, pl.ds(v, TILE, stride=N_TILE), :
                    ].astype(BF16)
            if p % 2:
                piece = 2 * (1 - t) + p // 2

                @pl.when(jnp.logical_not(last))
                def _():
                    halo_copy(0, 0, piece).start()
                    if piece == len(PIECES) - 1:
                        for i in range(2):
                            param_copy(i).start()

    @pl.when(first)
    def _():
        for i in range(len(PIECES)):
            own_copy(0, 0, i).start()

    def conv(c, carry):
        par = lax.rem(c, 2)
        nxt = 1 - par

        for d in range(cp_size - 1):
            st_copy(par, d).wait()
        mean, rstd = statistics(par)
        coefficients(c, mean, rstd, (3,))

        def own(t):
            return lambda p, cut: raw[par, t, p, :, cut]

        def received(t):
            return lambda p, cut: halo[par, t, p, :, cut]

        def norms(read, f, halves=(0, 1), rows=range(N_ROW)):
            return [functools.partial(norm, read, f, p, h) for h in halves for p in rows]

        def epilogues(t, rows):
            return [functools.partial(epilogue, c, par, t, p, m) for p in rows for m in range(2)]

        for thunk in norms(own(1), 3, (0,), (0, 1)):
            thunk()

        @pl.when(c == 0)
        def _():
            for k in (1, 0):
                w_copy(0, k).start()

        @pl.when(c == 1)
        def _():
            @pl.when(jnp.logical_not(first))
            def _():
                for i in range(2):
                    param_copy(i).wait_recv()
                for b in range(2):
                    gains[2 * b + 1, 0:2, :] = h_scale[b]
                    shifts[2 * b + 1, 0:2, :] = h_shift[b]

            @pl.when(first)
            def _():
                for b in range(2):
                    for f in range(2):
                        gains[2 * b + 1, f : f + 1, :] = mid_scale[b, 0:1]
                        shifts[2 * b + 1, f : f + 1, :] = mid_shift[b, 0:1]

            @pl.when(jnp.logical_not(last))
            def _():
                for i in range(2):
                    param_copy(i).wait_send()

        coefficients(c, mean, rstd, (2, 1, 0))
        w_copy(c, 2).wait()
        run(par, steps_of(1, 2, (0,), size=1), norms(own(1), 3, (0,), (2, 3)) + norms(own(1), 3, (1,)), 0.9)
        run(par, steps_of(1, 2, (1,)), norms(own(0), 2))
        w_copy(c, 1).wait()

        @pl.when(c < N_CONV - 1)
        def _():
            for k in (2, 1, 0):
                w_copy(c + 1, k).start()

        run(par, steps_of(1, 1))
        steps = steps_of(0, 2)
        run(par, steps[:12])
        w_copy(c, 0).wait()
        own_copy(par, par, 0).wait()
        own_copy(par, par, 1).wait()
        run(par, steps[12:], norms(received(1), 1), 0.9)
        run(par, steps_of(1, 0, dps=(1, -1)))
        for p in range(N_ROW):
            run(par, steps_of(1, 0, rows=(p, p + 1), dps=(0,)), epilogues(1, (p - 1,)) if p else ())
        steps = steps_of(0, 1)
        run(par, steps[:3], epilogues(1, (3,)))

        @pl.when(jnp.logical_and(c < N_CONV - 1, jnp.logical_not(last)))
        def _():
            halo_copy(nxt, nxt, 0).start()

        own_copy(par, par, 2).wait()
        run(par, steps[3:15], norms(received(0), 0, rows=(0, 1)), 0.9)
        own_copy(par, par, 3).wait()
        run(par, steps[15:], norms(received(0), 0, rows=(2, 3)), 0.9)
        run(par, steps_of(0, 0, dps=(1, -1)))
        for p in range(N_ROW):
            run(par, steps_of(0, 0, rows=(p, p + 1), dps=(0,)), epilogues(0, (p - 1,)) if p else ())
        for thunk in epilogues(0, (N_ROW - 1,)):
            thunk()
        finish_moments(nxt)

        @pl.when(c < N_CONV - 1)
        def _():
            for d in range(cp_size - 1):
                st_copy(nxt, d).start()

            @pl.when(jnp.logical_not(last))
            def _():
                for i in range(1, len(PIECES)):
                    halo_copy(nxt, nxt, i).start()

            @pl.when(first)
            def _():
                for i in range(len(PIECES)):
                    own_copy(nxt, nxt, i).start()

        @pl.when(jnp.logical_not(last))
        def _():
            for i in range(len(PIECES)):
                halo_copy(par, par, i).wait_send()

        return carry

    lax.fori_loop(0, N_CONV, conv, 0)

    out_ref[...] = raw[0]


def reorder(val_ref, out_hbm, tmp, buf, sem):
    copies = []
    for t in range(N_FR):
        for p in range(N_ROW):
            for j in range(4):
                cut = slice(j * 128, (j + 1) * 128)
                for v in range(N_TILE):
                    tmp[p % 2, j, pl.ds(v, TILE, stride=N_TILE), :] = val_ref[
                        t, p, v * TILE : (v + 1) * TILE, cut
                    ].astype(F32)
                buf[t, p, :, cut] = tmp[p % 2, j].astype(BF16)
            copies.append(pltpu.make_async_copy(buf.at[t, p], out_hbm.at[t, p], sem.at[t, p]))
            copies[-1].start()
    for copy in copies:
        copy.wait()


def solution(mesh):
    cp_size = mesh.shape["cp"]

    def local_decode(latent, conv_w, conv_b, in_scale, in_shift, mid_scale, mid_shift):
        any_spec, vmem = pl.BlockSpec(memory_space=pl.ANY), pl.BlockSpec(memory_space=pltpu.VMEM)
        dma = pltpu.SemaphoreType.DMA
        frame = (N_ROW, N_COL, N_CH)
        blocks = pl.pallas_call(
            functools.partial(kernel, cp_size),
            out_shape=jax.ShapeDtypeStruct(latent.shape, BF16),
            in_specs=[any_spec] * 7,
            out_specs=vmem,
            scratch_shapes=[
                pltpu.VMEM((N_CONV, N_CH), F32),
                pltpu.VMEM((2, N_CH), F32),
                pltpu.VMEM((2, N_CH), F32),
                pltpu.VMEM((2, N_FR, N_CH), F32),
                pltpu.VMEM((2, N_FR, N_CH), F32),
                pltpu.VMEM((N_FR, *frame), BF16),
                pltpu.VMEM((3, N_FR, *frame), BF16),
                pltpu.VMEM((2, N_FR, *frame), BF16),
                pltpu.VMEM((4, N_ROW, PAD_COL, N_CH), BF16),
                pltpu.VMEM((2, 3, 9 * N_CH, N_CH), BF16),
                pltpu.VMEM((N_FR, N_ROW, 2, N_COL, HALF), F32),
                pltpu.VMEM((2, 8, N_CH), F32),
                pltpu.VMEM((2, 8, 128), F32),
                pltpu.VMEM((2, cp_size - 1, 8, 128), F32),
                pltpu.VMEM((N_CONV, 4, N_CH), F32),
                pltpu.VMEM((N_CONV, 4, N_CH), F32),
                pltpu.VMEM((2, N_FR, N_CH), F32),
                pltpu.VMEM((2, N_FR, N_CH), F32),
                pltpu.VMEM((2, 4, N_CH), F32),
                pltpu.VMEM((2, 4, N_COL, 128), F32),
                dma((N_FR,)),
                dma((5,)),
                dma((2, 3)),
                dma((2, cp_size - 1)),
                dma((2, cp_size - 1)),
                dma((2, len(PIECES))),
                dma((2, len(PIECES))),
                dma((2,)),
                dma((2,)),
            ],
            compiler_params=pltpu.CompilerParams(
                collective_id=0, has_side_effects=True, vmem_limit_bytes=46 * 1024 * 1024
            ),
        )(*[
            pltpu.with_memory_space_constraint(arg, pltpu.HBM)
            for arg in (
                latent, conv_w.reshape(N_CONV, 3, 9 * N_CH, N_CH), conv_b, in_scale, in_shift, mid_scale, mid_shift
            )
        ])
        return pl.pallas_call(
            reorder,
            out_shape=jax.ShapeDtypeStruct(latent.shape, BF16),
            in_specs=[vmem],
            out_specs=any_spec,
            scratch_shapes=[
                pltpu.VMEM((2, 4, N_COL, 128), F32),
                pltpu.VMEM((N_FR, *frame), BF16),
                dma((N_FR, N_ROW)),
            ],
            compiler_params=pltpu.CompilerParams(vmem_limit_bytes=6 * 1024 * 1024),
        )(blocks)

    time_spec = P(("dp", "cp"))
    param_spec = P(None, ("dp", "cp"))
    return jax.shard_map(
        local_decode,
        mesh=mesh,
        in_specs=(time_spec, P(), P(), P(), P(), param_spec, param_spec),
        out_specs=time_spec,
        check_vma=False,
    )
```

```python
import functools

import jax
import jax.numpy as jnp
from jax import lax
from jax.experimental import pallas as pl
from jax.experimental.pallas import tpu as pltpu
from jax.sharding import PartitionSpec as P

NUM_GROUPS = 32
EPSILON = 1e-6
MESH = pl.DeviceIdType.MESH
F32 = jnp.float32
BF16 = jnp.bfloat16

N_CONV = 4
N_FR = 2
N_ROW = 4
N_COL = 128
N_CH = 512
TILE = 16
PIECES = ((1, slice(0, 2)), (1, slice(2, 4)), (0, slice(0, 2)), (0, slice(2, 4)))
N_TILE = N_COL // TILE
PAD_COL = N_COL + 2 * TILE
HALF = 256


def kernel(
    cp_size, x_hbm, w_hbm, bias_hbm, in_scale_hbm, in_shift_hbm, mid_scale_hbm, mid_shift_hbm, out_ref,
    bias_ref, in_scale, in_shift, mid_scale, mid_shift,
    x_in, raw, halo, act, wts, acc, part, tx, rx, gains, shifts, h_scale, h_shift, coef, tmp,
    x_sem, s_sem, w_sem, st_send, st_recv, h_send, h_recv, p_send, p_recv,
):
    cp = lax.axis_index("cp")
    count = float(N_FR * cp_size * N_ROW * N_COL * (N_CH // NUM_GROUPS))
    first, last = cp == 0, cp == cp_size - 1
    peers = [lax.rem(cp + d, cp_size) for d in range(1, cp_size)]
    right = lax.rem(cp + 1, cp_size)

    def mm_step(slot, t, k, low, high, dp, dq, kt):
        cut = slice(TILE * (1 + dq), TILE * (1 + dq) + N_COL)
        lhs = act[t + k, low + dp : high + dp, cut, kt * HALF : (kt + 1) * HALF].reshape((high - low) * N_COL, HALF)
        off = ((dp + 1) * 3 + dq + 1) * N_CH + kt * HALF
        for m in range(2):
            w = wts[slot, k, off : off + HALF, m * HALF : (m + 1) * HALF]
            out = jnp.dot(lhs, w, preferred_element_type=F32)
            for p in range(low, high):
                acc[t, p, m] += out[(p - low) * N_COL : (p - low + 1) * N_COL]

    def pop(m, t, p):
        val = acc[t, p, m]
        acc[t, p, m] = jnp.zeros((N_COL, HALF), F32)
        return val

    def steps_of(t, k, kts=(0, 1), rows=(0, N_ROW), dps=(0, 1, -1), size=N_ROW):
        return [
            (t, k, max(low, -dp), min(low + size, N_ROW - dp, rows[1]), dp, dq, kt)
            for kt in kts
            for low in range(rows[0], rows[1], size)
            for dp in dps
            if max(low, -dp) < min(low + size, N_ROW - dp, rows[1])
            for dq in (0, -1, 1)
        ]

    def run(slot, steps, thunks=(), upto=1.0):
        done, span = 0, max(1, int(len(steps) * upto))
        for i, step in enumerate(steps):
            mm_step(slot, *step)
            want = min(len(thunks), -(-len(thunks) * (i + 1) // span))
            for thunk in thunks[done:want]:
                thunk()
            done = want

    def add_moments(val, half):
        cut = slice(half * HALF, (half + 1) * HALF)
        rows = val.reshape(N_COL // 8, 8, HALF)
        part[0, :, cut] += jnp.sum(rows, axis=0)
        part[1, :, cut] += jnp.sum(rows * rows, axis=0)

    def norm(read, f, p, half):
        cut = slice(half * HALF, (half + 1) * HALF)
        val = read(p, cut).astype(F32) * coef[0, f : f + 1, cut] + coef[1, f : f + 1, cut]
        val = val.astype(BF16).astype(F32)
        val = val + val * jnp.tanh(val)
        act[f, p, TILE : TILE + N_COL, cut] = val.astype(BF16)
        row = lax.broadcasted_iota(jnp.int32, (TILE, HALF), 0)
        low = jnp.where(row == 0, 0.0, pltpu.roll(val[N_COL - TILE :], 1, 0))
        act[f, p, 0:TILE, cut] = low.astype(BF16)
        high = jnp.where(row == TILE - 1, 0.0, pltpu.roll(val[:TILE], TILE - 1, 0))
        act[f, p, TILE + N_COL :, cut] = high.astype(BF16)

    def epilogue(c, par, t, p, m):
        cut = slice(m * HALF, (m + 1) * HALF)
        conv = (pop(m, t, p) + bias_ref[pl.ds(c, 1), cut]).astype(BF16).astype(F32)
        val = (raw[2 - 2 * par, t, p, :, cut].astype(F32) + conv).astype(BF16)
        raw[1 - par, t, p, :, cut] = val
        add_moments(val.astype(F32), m)

    def finish_moments(slot):
        for i in range(2):
            total = jnp.sum(part[i], axis=0, keepdims=True)
            for j in range(4):
                tx[slot, 4 * i + j : 4 * i + j + 1, :] = total[:, j * 128 : (j + 1) * 128]
        part[...] = jnp.zeros_like(part)

    def statistics(slot):
        total = tx[slot]
        for d in range(cp_size - 1):
            total = total + rx[slot, d]
        lane = lax.broadcasted_iota(jnp.int32, total.shape, 1)
        size = N_CH // NUM_GROUPS
        spot = lane % size
        terms = [total]
        for d in range(1, size):
            terms.append(jnp.where(spot < size - d, pltpu.roll(total, 128 - d, 1), 0.0))
            terms.append(jnp.where(spot >= d, pltpu.roll(total, d, 1), 0.0))
        while len(terms) > 1:
            terms = [terms[i] + terms[i + 1] for i in range(0, len(terms) - 1, 2)] + terms[len(terms) & ~1 :]
        total = terms[0]
        mean = total[0:4] * (1.0 / count)
        var = total[4:8] * (1.0 / count) - mean * mean
        return mean, lax.rsqrt(var + EPSILON)

    def coefficients(c, mean, rstd, frames):
        for j in range(4):
            cut = slice(j * 128, (j + 1) * 128)
            for f in frames:
                gain = 0.5 * (rstd[j : j + 1] * gains[c, f : f + 1, cut])
                coef[0, f : f + 1, cut] = gain
                coef[1, f : f + 1, cut] = 0.5 * shifts[c, f : f + 1, cut] - mean[j : j + 1] * gain

    def w_copy(c, k):
        slot = lax.rem(c, 2)
        return pltpu.make_async_copy(w_hbm.at[c, k], wts.at[slot, k], w_sem.at[slot, k])

    def st_copy(slot, d):
        return pltpu.make_async_remote_copy(
            src_ref=tx.at[slot], dst_ref=rx.at[slot, d], send_sem=st_send.at[slot, d], recv_sem=st_recv.at[slot, d],
            device_id={"cp": peers[d]}, device_id_type=MESH,
        )

    def halo_copy(par, hs, i):
        t, rows = PIECES[i]
        return pltpu.make_async_remote_copy(
            src_ref=raw.at[par, t, rows], dst_ref=halo.at[hs, t, rows],
            send_sem=h_send.at[hs, i], recv_sem=h_recv.at[hs, i],
            device_id={"cp": right}, device_id_type=MESH,
        )

    def own_copy(par, hs, i):
        t, rows = PIECES[i]
        return pltpu.make_async_copy(raw.at[par, 0, rows], halo.at[hs, t, rows], h_recv.at[hs, i])

    def param_copy(i):
        src, dst = ((mid_scale, h_scale), (mid_shift, h_shift))[i]
        return pltpu.make_async_remote_copy(
            src_ref=src, dst_ref=dst, send_sem=p_send.at[i], recv_sem=p_recv.at[i],
            device_id={"cp": right}, device_id_type=MESH,
        )

    barrier = pltpu.get_barrier_semaphore()
    for peer in peers:
        pl.semaphore_signal(barrier, inc=1, device_id={"cp": peer}, device_id_type=MESH)
    x_copies = [pltpu.make_async_copy(x_hbm.at[t], x_in.at[t], x_sem.at[t]) for t in range(N_FR)]
    for t in (1, 0):
        x_copies[t].start()
    small = ((bias_hbm, bias_ref), (in_scale_hbm, in_scale), (in_shift_hbm, in_shift),
             (mid_scale_hbm, mid_scale), (mid_shift_hbm, mid_shift))
    small_copies = [pltpu.make_async_copy(src, dst, s_sem.at[i]) for i, (src, dst) in enumerate(small)]
    for copy in small_copies:
        copy.start()
    w_copy(0, 2).start()

    part[...] = jnp.zeros_like(part)
    acc[...] = jnp.zeros_like(acc)
    raw[2] = jnp.zeros((N_FR, N_ROW, N_COL, N_CH), BF16)
    for t in (1, 0):
        x_copies[t].wait()
        for p in range(N_ROW):
            val = x_in[t, p].astype(F32)
            for half in range(2):
                add_moments(val[:, half * HALF : (half + 1) * HALF], half)
    finish_moments(0)
    pl.semaphore_wait(barrier, cp_size - 1)
    for d in range(cp_size - 1):
        st_copy(0, d).start()

    for copy in small_copies:
        copy.wait()
    for b in range(2):
        for f in range(4):
            gains[2 * b, f : f + 1, :] = in_scale[b : b + 1, :]
            shifts[2 * b, f : f + 1, :] = in_shift[b : b + 1, :]
        gains[2 * b + 1, 2:4, :] = mid_scale[b]
        shifts[2 * b + 1, 2:4, :] = mid_shift[b]
    for t in (1, 0):
        for p in range(N_ROW):
            val = x_in[t, p].astype(F32)
            for j in range(4):
                tmp[p % 2, j] = val[:, j * 128 : (j + 1) * 128]
            for j in range(4):
                for v in range(N_TILE):
                    raw[0, t, p, v * TILE : (v + 1) * TILE, j * 128 : (j + 1) * 128] = tmp[
                        p % 2, j, pl.ds(v, TILE, stride=N_TILE), :
                    ].astype(BF16)
            if p % 2:
                piece = 2 * (1 - t) + p // 2

                @pl.when(jnp.logical_not(last))
                def _():
                    halo_copy(0, 0, piece).start()
                    if piece == len(PIECES) - 1:
                        for i in range(2):
                            param_copy(i).start()

    @pl.when(first)
    def _():
        for i in range(len(PIECES)):
            own_copy(0, 0, i).start()

    def conv(c, carry):
        par = lax.rem(c, 2)
        nxt = 1 - par

        for d in range(cp_size - 1):
            st_copy(par, d).wait()
        mean, rstd = statistics(par)
        coefficients(c, mean, rstd, (3,))

        def own(t):
            return lambda p, cut: raw[par, t, p, :, cut]

        def received(t):
            return lambda p, cut: halo[par, t, p, :, cut]

        def norms(read, f, halves=(0, 1), rows=range(N_ROW)):
            return [functools.partial(norm, read, f, p, h) for h in halves for p in rows]

        def epilogues(t, rows):
            return [functools.partial(epilogue, c, par, t, p, m) for p in rows for m in range(2)]

        for thunk in norms(own(1), 3, (0,), (0, 1)):
            thunk()

        @pl.when(c == 0)
        def _():
            for k in (1, 0):
                w_copy(0, k).start()

        @pl.when(c == 1)
        def _():
            @pl.when(jnp.logical_not(first))
            def _():
                for i in range(2):
                    param_copy(i).wait_recv()
                for b in range(2):
                    gains[2 * b + 1, 0:2, :] = h_scale[b]
                    shifts[2 * b + 1, 0:2, :] = h_shift[b]

            @pl.when(first)
            def _():
                for b in range(2):
                    for f in range(2):
                        gains[2 * b + 1, f : f + 1, :] = mid_scale[b, 0:1]
                        shifts[2 * b + 1, f : f + 1, :] = mid_shift[b, 0:1]

            @pl.when(jnp.logical_not(last))
            def _():
                for i in range(2):
                    param_copy(i).wait_send()

        coefficients(c, mean, rstd, (2, 1, 0))
        w_copy(c, 2).wait()
        run(par, steps_of(1, 2, (0,), size=1), norms(own(1), 3, (0,), (2, 3)) + norms(own(1), 3, (1,)), 0.9)
        run(par, steps_of(1, 2, (1,)), norms(own(0), 2))
        w_copy(c, 1).wait()

        @pl.when(c < N_CONV - 1)
        def _():
            for k in (2, 1, 0):
                w_copy(c + 1, k).start()

        run(par, steps_of(1, 1))
        steps = steps_of(0, 2)
        run(par, steps[:12])
        w_copy(c, 0).wait()
        own_copy(par, par, 0).wait()
        own_copy(par, par, 1).wait()
        run(par, steps[12:], norms(received(1), 1), 0.9)
        run(par, steps_of(1, 0, dps=(1, -1)))
        for p in range(N_ROW):
            run(par, steps_of(1, 0, rows=(p, p + 1), dps=(0,)), epilogues(1, (p - 1,)) if p else ())
        steps = steps_of(0, 1)
        run(par, steps[:3], epilogues(1, (3,)))

        @pl.when(jnp.logical_and(c < N_CONV - 1, jnp.logical_not(last)))
        def _():
            halo_copy(nxt, nxt, 0).start()

        own_copy(par, par, 2).wait()
        run(par, steps[3:15], norms(received(0), 0, rows=(0, 1)), 0.9)
        own_copy(par, par, 3).wait()
        run(par, steps[15:], norms(received(0), 0, rows=(2, 3)), 0.9)
        run(par, steps_of(0, 0, dps=(1, -1)))
        for p in range(N_ROW):
            run(par, steps_of(0, 0, rows=(p, p + 1), dps=(0,)), epilogues(0, (p - 1,)) if p else ())
        for thunk in epilogues(0, (N_ROW - 1,)):
            thunk()
        finish_moments(nxt)

        @pl.when(c < N_CONV - 1)
        def _():
            for d in range(cp_size - 1):
                st_copy(nxt, d).start()

            @pl.when(jnp.logical_not(last))
            def _():
                for i in range(1, len(PIECES)):
                    halo_copy(nxt, nxt, i).start()

            @pl.when(first)
            def _():
                for i in range(len(PIECES)):
                    own_copy(nxt, nxt, i).start()

        @pl.when(jnp.logical_not(last))
        def _():
            for i in range(len(PIECES)):
                halo_copy(par, par, i).wait_send()

        return carry

    lax.fori_loop(0, N_CONV, conv, 0)

    out_ref[...] = raw[0]


def reorder(val_ref, out_hbm, tmp, buf, sem):
    copies = []
    for t in range(N_FR):
        for p in range(N_ROW):
            for j in range(4):
                cut = slice(j * 128, (j + 1) * 128)
                for v in range(N_TILE):
                    tmp[p % 2, j, pl.ds(v, TILE, stride=N_TILE), :] = val_ref[
                        t, p, v * TILE : (v + 1) * TILE, cut
                    ].astype(F32)
                buf[t, p, :, cut] = tmp[p % 2, j].astype(BF16)
            copies.append(pltpu.make_async_copy(buf.at[t, p], out_hbm.at[t, p], sem.at[t, p]))
            copies[-1].start()
    for copy in copies:
        copy.wait()


def solution(mesh):
    cp_size = mesh.shape["cp"]

    def local_decode(latent, conv_w, conv_b, in_scale, in_shift, mid_scale, mid_shift):
        any_spec, vmem = pl.BlockSpec(memory_space=pl.ANY), pl.BlockSpec(memory_space=pltpu.VMEM)
        dma = pltpu.SemaphoreType.DMA
        frame = (N_ROW, N_COL, N_CH)
        blocks = pl.pallas_call(
            functools.partial(kernel, cp_size),
            out_shape=jax.ShapeDtypeStruct(latent.shape, BF16),
            in_specs=[any_spec] * 7,
            out_specs=vmem,
            scratch_shapes=[
                pltpu.VMEM((N_CONV, N_CH), F32),
                pltpu.VMEM((2, N_CH), F32),
                pltpu.VMEM((2, N_CH), F32),
                pltpu.VMEM((2, N_FR, N_CH), F32),
                pltpu.VMEM((2, N_FR, N_CH), F32),
                pltpu.VMEM((N_FR, *frame), BF16),
                pltpu.VMEM((3, N_FR, *frame), BF16),
                pltpu.VMEM((2, N_FR, *frame), BF16),
                pltpu.VMEM((4, N_ROW, PAD_COL, N_CH), BF16),
                pltpu.VMEM((2, 3, 9 * N_CH, N_CH), BF16),
                pltpu.VMEM((N_FR, N_ROW, 2, N_COL, HALF), F32),
                pltpu.VMEM((2, 8, N_CH), F32),
                pltpu.VMEM((2, 8, 128), F32),
                pltpu.VMEM((2, cp_size - 1, 8, 128), F32),
                pltpu.VMEM((N_CONV, 4, N_CH), F32),
                pltpu.VMEM((N_CONV, 4, N_CH), F32),
                pltpu.VMEM((2, N_FR, N_CH), F32),
                pltpu.VMEM((2, N_FR, N_CH), F32),
                pltpu.VMEM((2, 4, N_CH), F32),
                pltpu.VMEM((2, 4, N_COL, 128), F32),
                dma((N_FR,)),
                dma((5,)),
                dma((2, 3)),
                dma((2, cp_size - 1)),
                dma((2, cp_size - 1)),
                dma((2, len(PIECES))),
                dma((2, len(PIECES))),
                dma((2,)),
                dma((2,)),
            ],
            compiler_params=pltpu.CompilerParams(
                collective_id=0, has_side_effects=True, vmem_limit_bytes=46 * 1024 * 1024
            ),
        )(*[
            pltpu.with_memory_space_constraint(arg, pltpu.HBM)
            for arg in (
                latent, conv_w.reshape(N_CONV, 3, 9 * N_CH, N_CH), conv_b, in_scale, in_shift, mid_scale, mid_shift
            )
        ])
        return pl.pallas_call(
            reorder,
            out_shape=jax.ShapeDtypeStruct(latent.shape, BF16),
            in_specs=[vmem],
            out_specs=any_spec,
            scratch_shapes=[
                pltpu.VMEM((2, 4, N_COL, 128), F32),
                pltpu.VMEM((N_FR, *frame), BF16),
                dma((N_FR, N_ROW)),
            ],
            compiler_params=pltpu.CompilerParams(vmem_limit_bytes=6 * 1024 * 1024),
        )(blocks)

    time_spec = P(("dp", "cp"))
    param_spec = P(None, ("dp", "cp"))
    return jax.shard_map(
        local_decode,
        mesh=mesh,
        in_specs=(time_spec, P(), P(), P(), P(), param_spec, param_spec),
        out_specs=time_spec,
        check_vma=False,
    )
```

```python
import functools

import jax
import jax.numpy as jnp
from jax import lax
from jax.experimental import pallas as pl
from jax.experimental.pallas import tpu as pltpu
from jax.sharding import PartitionSpec as P

NUM_GROUPS = 32
EPSILON = 1e-6
MESH = pl.DeviceIdType.MESH
F32 = jnp.float32
BF16 = jnp.bfloat16

N_CONV = 4
N_FR = 2
N_ROW = 4
N_COL = 128
N_CH = 512
TILE = 16
PIECES = ((1, slice(0, 2)), (1, slice(2, 4)), (0, slice(0, 2)), (0, slice(2, 4)))
N_TILE = N_COL // TILE
PAD_COL = N_COL + 2 * TILE
HALF = 256


def kernel(
    cp_size, x_hbm, w_hbm, bias_hbm, in_scale_hbm, in_shift_hbm, mid_scale_hbm, mid_shift_hbm, out_ref,
    bias_ref, in_scale, in_shift, mid_scale, mid_shift,
    x_in, raw, halo, act, wts, acc, part, tx, rx, gains, shifts, h_scale, h_shift, coef, tmp,
    x_sem, s_sem, w_sem, st_send, st_recv, h_send, h_recv, p_send, p_recv,
):
    cp = lax.axis_index("cp")
    count = float(N_FR * cp_size * N_ROW * N_COL * (N_CH // NUM_GROUPS))
    first, last = cp == 0, cp == cp_size - 1
    peers = [lax.rem(cp + d, cp_size) for d in range(1, cp_size)]
    right = lax.rem(cp + 1, cp_size)

    def mm_step(slot, t, k, low, high, dp, dq, kt):
        cut = slice(TILE * (1 + dq), TILE * (1 + dq) + N_COL)
        lhs = act[t + k, low + dp : high + dp, cut, kt * HALF : (kt + 1) * HALF].reshape((high - low) * N_COL, HALF)
        off = ((dp + 1) * 3 + dq + 1) * N_CH + kt * HALF
        for m in range(2):
            w = wts[slot, k, off : off + HALF, m * HALF : (m + 1) * HALF]
            out = jnp.dot(lhs, w, preferred_element_type=F32)
            for p in range(low, high):
                acc[t, p, m] += out[(p - low) * N_COL : (p - low + 1) * N_COL]

    def pop(m, t, p):
        val = acc[t, p, m]
        acc[t, p, m] = jnp.zeros((N_COL, HALF), F32)
        return val

    def steps_of(t, k, kts=(0, 1), rows=(0, N_ROW), dps=(0, 1, -1), size=N_ROW):
        return [
            (t, k, max(low, -dp), min(low + size, N_ROW - dp, rows[1]), dp, dq, kt)
            for kt in kts
            for low in range(rows[0], rows[1], size)
            for dp in dps
            if max(low, -dp) < min(low + size, N_ROW - dp, rows[1])
            for dq in (0, -1, 1)
        ]

    def run(slot, steps, thunks=(), upto=1.0):
        done, span = 0, max(1, int(len(steps) * upto))
        for i, step in enumerate(steps):
            mm_step(slot, *step)
            want = min(len(thunks), -(-len(thunks) * (i + 1) // span))
            for thunk in thunks[done:want]:
                thunk()
            done = want

    def add_moments(val, half):
        cut = slice(half * HALF, (half + 1) * HALF)
        rows = val.reshape(N_COL // 8, 8, HALF)
        part[0, :, cut] += jnp.sum(rows, axis=0)
        part[1, :, cut] += jnp.sum(rows * rows, axis=0)

    def norm(read, f, p, half):
        cut = slice(half * HALF, (half + 1) * HALF)
        val = read(p, cut).astype(F32) * coef[0, f : f + 1, cut] + coef[1, f : f + 1, cut]
        val = val.astype(BF16).astype(F32)
        val = val + val * jnp.tanh(val)
        act[f, p, TILE : TILE + N_COL, cut] = val.astype(BF16)
        row = lax.broadcasted_iota(jnp.int32, (TILE, HALF), 0)
        low = jnp.where(row == 0, 0.0, pltpu.roll(val[N_COL - TILE :], 1, 0))
        act[f, p, 0:TILE, cut] = low.astype(BF16)
        high = jnp.where(row == TILE - 1, 0.0, pltpu.roll(val[:TILE], TILE - 1, 0))
        act[f, p, TILE + N_COL :, cut] = high.astype(BF16)

    def epilogue(c, par, t, p, m):
        cut = slice(m * HALF, (m + 1) * HALF)
        conv = (pop(m, t, p) + bias_ref[pl.ds(c, 1), cut]).astype(BF16).astype(F32)
        val = (raw[2 - 2 * par, t, p, :, cut].astype(F32) + conv).astype(BF16)
        raw[1 - par, t, p, :, cut] = val
        add_moments(val.astype(F32), m)

    def finish_moments(slot):
        for i in range(2):
            total = jnp.sum(part[i], axis=0, keepdims=True)
            for j in range(4):
                tx[slot, 4 * i + j : 4 * i + j + 1, :] = total[:, j * 128 : (j + 1) * 128]
        part[...] = jnp.zeros_like(part)

    def statistics(slot):
        total = tx[slot]
        for d in range(cp_size - 1):
            total = total + rx[slot, d]
        lane = lax.broadcasted_iota(jnp.int32, total.shape, 1)
        size = N_CH // NUM_GROUPS
        spot = lane % size
        terms = [total]
        for d in range(1, size):
            terms.append(jnp.where(spot < size - d, pltpu.roll(total, 128 - d, 1), 0.0))
            terms.append(jnp.where(spot >= d, pltpu.roll(total, d, 1), 0.0))
        while len(terms) > 1:
            terms = [terms[i] + terms[i + 1] for i in range(0, len(terms) - 1, 2)] + terms[len(terms) & ~1 :]
        total = terms[0]
        mean = total[0:4] * (1.0 / count)
        var = total[4:8] * (1.0 / count) - mean * mean
        return mean, lax.rsqrt(var + EPSILON)

    def coefficients(c, mean, rstd, frames):
        for j in range(4):
            cut = slice(j * 128, (j + 1) * 128)
            for f in frames:
                gain = 0.5 * (rstd[j : j + 1] * gains[c, f : f + 1, cut])
                coef[0, f : f + 1, cut] = gain
                coef[1, f : f + 1, cut] = 0.5 * shifts[c, f : f + 1, cut] - mean[j : j + 1] * gain

    def w_copy(c, k):
        slot = lax.rem(c, 2)
        return pltpu.make_async_copy(w_hbm.at[c, k], wts.at[slot, k], w_sem.at[slot, k])

    def st_copy(slot, d):
        return pltpu.make_async_remote_copy(
            src_ref=tx.at[slot], dst_ref=rx.at[slot, d], send_sem=st_send.at[slot, d], recv_sem=st_recv.at[slot, d],
            device_id={"cp": peers[d]}, device_id_type=MESH,
        )

    def halo_copy(par, hs, i):
        t, rows = PIECES[i]
        return pltpu.make_async_remote_copy(
            src_ref=raw.at[par, t, rows], dst_ref=halo.at[hs, t, rows],
            send_sem=h_send.at[hs, i], recv_sem=h_recv.at[hs, i],
            device_id={"cp": right}, device_id_type=MESH,
        )

    def own_copy(par, hs, i):
        t, rows = PIECES[i]
        return pltpu.make_async_copy(raw.at[par, 0, rows], halo.at[hs, t, rows], h_recv.at[hs, i])

    def param_copy(i):
        src, dst = ((mid_scale, h_scale), (mid_shift, h_shift))[i]
        return pltpu.make_async_remote_copy(
            src_ref=src, dst_ref=dst, send_sem=p_send.at[i], recv_sem=p_recv.at[i],
            device_id={"cp": right}, device_id_type=MESH,
        )

    barrier = pltpu.get_barrier_semaphore()
    for peer in peers:
        pl.semaphore_signal(barrier, inc=1, device_id={"cp": peer}, device_id_type=MESH)
    x_copies = [pltpu.make_async_copy(x_hbm.at[t], x_in.at[t], x_sem.at[t]) for t in range(N_FR)]
    for t in (1, 0):
        x_copies[t].start()
    small = ((bias_hbm, bias_ref), (in_scale_hbm, in_scale), (in_shift_hbm, in_shift),
             (mid_scale_hbm, mid_scale), (mid_shift_hbm, mid_shift))
    small_copies = [pltpu.make_async_copy(src, dst, s_sem.at[i]) for i, (src, dst) in enumerate(small)]
    for copy in small_copies:
        copy.start()
    for k in (2, 1):
        w_copy(0, k).start()

    part[...] = jnp.zeros_like(part)
    acc[...] = jnp.zeros_like(acc)
    raw[2] = jnp.zeros((N_FR, N_ROW, N_COL, N_CH), BF16)
    for t in (1, 0):
        x_copies[t].wait()
        for p in range(N_ROW):
            val = x_in[t, p].astype(F32)
            for half in range(2):
                add_moments(val[:, half * HALF : (half + 1) * HALF], half)
    finish_moments(0)
    pl.semaphore_wait(barrier, cp_size - 1)
    for d in range(cp_size - 1):
        st_copy(0, d).start()

    for copy in small_copies:
        copy.wait()
    for b in range(2):
        for f in range(4):
            gains[2 * b, f : f + 1, :] = in_scale[b : b + 1, :]
            shifts[2 * b, f : f + 1, :] = in_shift[b : b + 1, :]
        gains[2 * b + 1, 2:4, :] = mid_scale[b]
        shifts[2 * b + 1, 2:4, :] = mid_shift[b]
    for t in (1, 0):
        for p in range(N_ROW):
            val = x_in[t, p].astype(F32)
            for j in range(4):
                tmp[p % 2, j] = val[:, j * 128 : (j + 1) * 128]
            for j in range(4):
                for v in range(N_TILE):
                    raw[0, t, p, v * TILE : (v + 1) * TILE, j * 128 : (j + 1) * 128] = tmp[
                        p % 2, j, pl.ds(v, TILE, stride=N_TILE), :
                    ].astype(BF16)
            if p % 2:
                piece = 2 * (1 - t) + p // 2

                @pl.when(jnp.logical_not(last))
                def _():
                    halo_copy(0, 0, piece).start()
                    if piece == len(PIECES) - 1:
                        for i in range(2):
                            param_copy(i).start()

    @pl.when(first)
    def _():
        for i in range(len(PIECES)):
            own_copy(0, 0, i).start()

    def conv(c, carry):
        par = lax.rem(c, 2)
        nxt = 1 - par

        for d in range(cp_size - 1):
            st_copy(par, d).wait()
        mean, rstd = statistics(par)
        coefficients(c, mean, rstd, (3,))

        def own(t):
            return lambda p, cut: raw[par, t, p, :, cut]

        def received(t):
            return lambda p, cut: halo[par, t, p, :, cut]

        def norms(read, f, halves=(0, 1), rows=range(N_ROW)):
            return [functools.partial(norm, read, f, p, h) for h in halves for p in rows]

        def epilogues(t, rows):
            return [functools.partial(epilogue, c, par, t, p, m) for p in rows for m in range(2)]

        for thunk in norms(own(1), 3, (0,), (0, 1)):
            thunk()

        @pl.when(c == 0)
        def _():
            w_copy(0, 0).start()

        @pl.when(c == 1)
        def _():
            @pl.when(jnp.logical_not(first))
            def _():
                for i in range(2):
                    param_copy(i).wait_recv()
                for b in range(2):
                    gains[2 * b + 1, 0:2, :] = h_scale[b]
                    shifts[2 * b + 1, 0:2, :] = h_shift[b]

            @pl.when(first)
            def _():
                for b in range(2):
                    for f in range(2):
                        gains[2 * b + 1, f : f + 1, :] = mid_scale[b, 0:1]
                        shifts[2 * b + 1, f : f + 1, :] = mid_shift[b, 0:1]

            @pl.when(jnp.logical_not(last))
            def _():
                for i in range(2):
                    param_copy(i).wait_send()

        coefficients(c, mean, rstd, (2, 1, 0))
        w_copy(c, 2).wait()
        w_copy(c, 1).wait()
        run(par, steps_of(1, 2, (0,), size=1), norms(own(1), 3, (0,), (2, 3)) + norms(own(1), 3, (1,)), 0.9)
        run(par, steps_of(1, 2, (1,)), norms(own(0), 2))
        run(par, steps_of(1, 1))
        steps = steps_of(0, 2)
        run(par, steps[:12])
        w_copy(c, 0).wait()
        own_copy(par, par, 0).wait()
        own_copy(par, par, 1).wait()

        @pl.when(c < N_CONV - 1)
        def _():
            for k in (2, 1, 0):
                w_copy(c + 1, k).start()

        run(par, steps[12:], norms(received(1), 1), 0.9)
        run(par, steps_of(1, 0, dps=(1, -1)))
        for p in range(N_ROW):
            run(par, steps_of(1, 0, rows=(p, p + 1), dps=(0,)), epilogues(1, (p - 1,)) if p else ())
        steps = steps_of(0, 1)
        run(par, steps[:3], epilogues(1, (3,)))

        @pl.when(jnp.logical_and(c < N_CONV - 1, jnp.logical_not(last)))
        def _():
            halo_copy(nxt, nxt, 0).start()

        own_copy(par, par, 2).wait()
        run(par, steps[3:15], norms(received(0), 0, rows=(0, 1)), 0.9)
        own_copy(par, par, 3).wait()
        run(par, steps[15:], norms(received(0), 0, rows=(2, 3)), 0.9)
        run(par, steps_of(0, 0, dps=(1, -1)))
        for p in range(N_ROW):
            run(par, steps_of(0, 0, rows=(p, p + 1), dps=(0,)), epilogues(0, (p - 1,)) if p else ())
        for thunk in epilogues(0, (N_ROW - 1,)):
            thunk()
        finish_moments(nxt)

        @pl.when(c < N_CONV - 1)
        def _():
            for d in range(cp_size - 1):
                st_copy(nxt, d).start()

            @pl.when(jnp.logical_not(last))
            def _():
                for i in range(1, len(PIECES)):
                    halo_copy(nxt, nxt, i).start()

            @pl.when(first)
            def _():
                for i in range(len(PIECES)):
                    own_copy(nxt, nxt, i).start()

        @pl.when(jnp.logical_not(last))
        def _():
            for i in range(len(PIECES)):
                halo_copy(par, par, i).wait_send()

        return carry

    lax.fori_loop(0, N_CONV, conv, 0)

    out_ref[...] = raw[0]


def reorder(val_ref, out_hbm, tmp, buf, sem):
    copies = []
    for t in range(N_FR):
        for p in range(N_ROW):
            for j in range(4):
                cut = slice(j * 128, (j + 1) * 128)
                for v in range(N_TILE):
                    tmp[p % 2, j, pl.ds(v, TILE, stride=N_TILE), :] = val_ref[
                        t, p, v * TILE : (v + 1) * TILE, cut
                    ].astype(F32)
                buf[t, p, :, cut] = tmp[p % 2, j].astype(BF16)
            copies.append(pltpu.make_async_copy(buf.at[t, p], out_hbm.at[t, p], sem.at[t, p]))
            copies[-1].start()
    for copy in copies:
        copy.wait()


def solution(mesh):
    cp_size = mesh.shape["cp"]

    def local_decode(latent, conv_w, conv_b, in_scale, in_shift, mid_scale, mid_shift):
        any_spec, vmem = pl.BlockSpec(memory_space=pl.ANY), pl.BlockSpec(memory_space=pltpu.VMEM)
        dma = pltpu.SemaphoreType.DMA
        frame = (N_ROW, N_COL, N_CH)
        blocks = pl.pallas_call(
            functools.partial(kernel, cp_size),
            out_shape=jax.ShapeDtypeStruct(latent.shape, BF16),
            in_specs=[any_spec] * 7,
            out_specs=vmem,
            scratch_shapes=[
                pltpu.VMEM((N_CONV, N_CH), F32),
                pltpu.VMEM((2, N_CH), F32),
                pltpu.VMEM((2, N_CH), F32),
                pltpu.VMEM((2, N_FR, N_CH), F32),
                pltpu.VMEM((2, N_FR, N_CH), F32),
                pltpu.VMEM((N_FR, *frame), BF16),
                pltpu.VMEM((3, N_FR, *frame), BF16),
                pltpu.VMEM((2, N_FR, *frame), BF16),
                pltpu.VMEM((4, N_ROW, PAD_COL, N_CH), BF16),
                pltpu.VMEM((2, 3, 9 * N_CH, N_CH), BF16),
                pltpu.VMEM((N_FR, N_ROW, 2, N_COL, HALF), F32),
                pltpu.VMEM((2, 8, N_CH), F32),
                pltpu.VMEM((2, 8, 128), F32),
                pltpu.VMEM((2, cp_size - 1, 8, 128), F32),
                pltpu.VMEM((N_CONV, 4, N_CH), F32),
                pltpu.VMEM((N_CONV, 4, N_CH), F32),
                pltpu.VMEM((2, N_FR, N_CH), F32),
                pltpu.VMEM((2, N_FR, N_CH), F32),
                pltpu.VMEM((2, 4, N_CH), F32),
                pltpu.VMEM((2, 4, N_COL, 128), F32),
                dma((N_FR,)),
                dma((5,)),
                dma((2, 3)),
                dma((2, cp_size - 1)),
                dma((2, cp_size - 1)),
                dma((2, len(PIECES))),
                dma((2, len(PIECES))),
                dma((2,)),
                dma((2,)),
            ],
            compiler_params=pltpu.CompilerParams(
                collective_id=0, has_side_effects=True, vmem_limit_bytes=46 * 1024 * 1024
            ),
        )(*[
            pltpu.with_memory_space_constraint(arg, pltpu.HBM)
            for arg in (
                latent, conv_w.reshape(N_CONV, 3, 9 * N_CH, N_CH), conv_b, in_scale, in_shift, mid_scale, mid_shift
            )
        ])
        return pl.pallas_call(
            reorder,
            out_shape=jax.ShapeDtypeStruct(latent.shape, BF16),
            in_specs=[vmem],
            out_specs=any_spec,
            scratch_shapes=[
                pltpu.VMEM((2, 4, N_COL, 128), F32),
                pltpu.VMEM((N_FR, *frame), BF16),
                dma((N_FR, N_ROW)),
            ],
            compiler_params=pltpu.CompilerParams(vmem_limit_bytes=6 * 1024 * 1024),
        )(blocks)

    time_spec = P(("dp", "cp"))
    param_spec = P(None, ("dp", "cp"))
    return jax.shard_map(
        local_decode,
        mesh=mesh,
        in_specs=(time_spec, P(), P(), P(), P(), param_spec, param_spec),
        out_specs=time_spec,
        check_vma=False,
    )
```

```python
import functools

import jax
import jax.numpy as jnp
from jax import lax
from jax.experimental import pallas as pl
from jax.experimental.pallas import tpu as pltpu
from jax.sharding import PartitionSpec as P

NUM_GROUPS = 32
EPSILON = 1e-6
MESH = pl.DeviceIdType.MESH
F32 = jnp.float32
BF16 = jnp.bfloat16

N_CONV = 4
N_FR = 2
N_ROW = 4
N_COL = 128
N_CH = 512
TILE = 16
PIECES = ((1, slice(0, 2)), (1, slice(2, 4)), (0, slice(0, 2)), (0, slice(2, 4)))
N_TILE = N_COL // TILE
PAD_COL = N_COL + 2 * TILE
HALF = 256


def kernel(
    cp_size, x_hbm, w_hbm, bias_hbm, in_scale_hbm, in_shift_hbm, mid_scale_hbm, mid_shift_hbm, out_ref,
    bias_ref, in_scale, in_shift, mid_scale, mid_shift,
    x_in, raw, halo, act, wts, acc, part, tx, rx, gains, shifts, h_scale, h_shift, coef, tmp,
    x_sem, s_sem, w_sem, st_send, st_recv, h_send, h_recv, p_send, p_recv,
):
    cp = lax.axis_index("cp")
    count = float(N_FR * cp_size * N_ROW * N_COL * (N_CH // NUM_GROUPS))
    first, last = cp == 0, cp == cp_size - 1
    peers = [lax.rem(cp + d, cp_size) for d in range(1, cp_size)]
    right = lax.rem(cp + 1, cp_size)

    def mm_step(slot, t, k, low, high, dp, dq, kt):
        cut = slice(TILE * (1 + dq), TILE * (1 + dq) + N_COL)
        lhs = act[t + k, low + dp : high + dp, cut, kt * HALF : (kt + 1) * HALF].reshape((high - low) * N_COL, HALF)
        off = ((dp + 1) * 3 + dq + 1) * N_CH + kt * HALF
        for m in range(2):
            w = wts[slot, k, off : off + HALF, m * HALF : (m + 1) * HALF]
            out = jnp.dot(lhs, w, preferred_element_type=F32)
            for p in range(low, high):
                acc[t, p, m] += out[(p - low) * N_COL : (p - low + 1) * N_COL]

    def pop(m, t, p):
        val = acc[t, p, m]
        acc[t, p, m] = jnp.zeros((N_COL, HALF), F32)
        return val

    def steps_of(t, k, kts=(0, 1), rows=(0, N_ROW), dps=(0, 1, -1), size=N_ROW):
        return [
            (t, k, max(low, -dp), min(low + size, N_ROW - dp, rows[1]), dp, dq, kt)
            for kt in kts
            for low in range(rows[0], rows[1], size)
            for dp in dps
            if max(low, -dp) < min(low + size, N_ROW - dp, rows[1])
            for dq in (0, -1, 1)
        ]

    def run(slot, steps, thunks=(), upto=1.0):
        done, span = 0, max(1, int(len(steps) * upto))
        for i, step in enumerate(steps):
            mm_step(slot, *step)
            want = min(len(thunks), -(-len(thunks) * (i + 1) // span))
            for thunk in thunks[done:want]:
                thunk()
            done = want

    def add_moments(val, half):
        cut = slice(half * HALF, (half + 1) * HALF)
        rows = val.reshape(N_COL // 8, 8, HALF)
        part[0, :, cut] += jnp.sum(rows, axis=0)
        part[1, :, cut] += jnp.sum(rows * rows, axis=0)

    def norm(read, f, p, half):
        cut = slice(half * HALF, (half + 1) * HALF)
        val = read(p, cut).astype(F32) * coef[0, f : f + 1, cut] + coef[1, f : f + 1, cut]
        val = val.astype(BF16).astype(F32)
        val = val + val * jnp.tanh(val)
        act[f, p, TILE : TILE + N_COL, cut] = val.astype(BF16)
        row = lax.broadcasted_iota(jnp.int32, (TILE, HALF), 0)
        low = jnp.where(row == 0, 0.0, pltpu.roll(val[N_COL - TILE :], 1, 0))
        act[f, p, 0:TILE, cut] = low.astype(BF16)
        high = jnp.where(row == TILE - 1, 0.0, pltpu.roll(val[:TILE], TILE - 1, 0))
        act[f, p, TILE + N_COL :, cut] = high.astype(BF16)

    def epilogue(c, par, t, p, m):
        cut = slice(m * HALF, (m + 1) * HALF)
        conv = (pop(m, t, p) + bias_ref[pl.ds(c, 1), cut]).astype(BF16).astype(F32)
        val = (raw[2 - 2 * par, t, p, :, cut].astype(F32) + conv).astype(BF16)
        raw[1 - par, t, p, :, cut] = val
        out_ref[t, p, :, cut] = val
        add_moments(val.astype(F32), m)

    def finish_moments(slot):
        for i in range(2):
            total = jnp.sum(part[i], axis=0, keepdims=True)
            for j in range(4):
                tx[slot, 4 * i + j : 4 * i + j + 1, :] = total[:, j * 128 : (j + 1) * 128]
        part[...] = jnp.zeros_like(part)

    def statistics(slot):
        total = tx[slot]
        for d in range(cp_size - 1):
            total = total + rx[slot, d]
        lane = lax.broadcasted_iota(jnp.int32, total.shape, 1)
        size = N_CH // NUM_GROUPS
        spot = lane % size
        terms = [total]
        for d in range(1, size):
            terms.append(jnp.where(spot < size - d, pltpu.roll(total, 128 - d, 1), 0.0))
            terms.append(jnp.where(spot >= d, pltpu.roll(total, d, 1), 0.0))
        while len(terms) > 1:
            terms = [terms[i] + terms[i + 1] for i in range(0, len(terms) - 1, 2)] + terms[len(terms) & ~1 :]
        total = terms[0]
        mean = total[0:4] * (1.0 / count)
        var = total[4:8] * (1.0 / count) - mean * mean
        return mean, lax.rsqrt(var + EPSILON)

    def coefficients(c, mean, rstd, frames):
        for j in range(4):
            cut = slice(j * 128, (j + 1) * 128)
            for f in frames:
                gain = 0.5 * (rstd[j : j + 1] * gains[c, f : f + 1, cut])
                coef[0, f : f + 1, cut] = gain
                coef[1, f : f + 1, cut] = 0.5 * shifts[c, f : f + 1, cut] - mean[j : j + 1] * gain

    def w_copy(c, k):
        slot = lax.rem(c, 2)
        return pltpu.make_async_copy(w_hbm.at[c, k], wts.at[slot, k], w_sem.at[slot, k])

    def st_copy(slot, d):
        return pltpu.make_async_remote_copy(
            src_ref=tx.at[slot], dst_ref=rx.at[slot, d], send_sem=st_send.at[slot, d], recv_sem=st_recv.at[slot, d],
            device_id={"cp": peers[d]}, device_id_type=MESH,
        )

    def halo_copy(par, hs, i):
        t, rows = PIECES[i]
        return pltpu.make_async_remote_copy(
            src_ref=raw.at[par, t, rows], dst_ref=halo.at[hs, t, rows],
            send_sem=h_send.at[hs, i], recv_sem=h_recv.at[hs, i],
            device_id={"cp": right}, device_id_type=MESH,
        )

    def own_copy(par, hs, i):
        t, rows = PIECES[i]
        return pltpu.make_async_copy(raw.at[par, 0, rows], halo.at[hs, t, rows], h_recv.at[hs, i])

    def param_copy(i):
        src, dst = ((mid_scale, h_scale), (mid_shift, h_shift))[i]
        return pltpu.make_async_remote_copy(
            src_ref=src, dst_ref=dst, send_sem=p_send.at[i], recv_sem=p_recv.at[i],
            device_id={"cp": right}, device_id_type=MESH,
        )

    barrier = pltpu.get_barrier_semaphore()
    for peer in peers:
        pl.semaphore_signal(barrier, inc=1, device_id={"cp": peer}, device_id_type=MESH)
    x_copies = [pltpu.make_async_copy(x_hbm.at[t], x_in.at[t], x_sem.at[t]) for t in range(N_FR)]
    for t in (1, 0):
        x_copies[t].start()
    small = ((bias_hbm, bias_ref), (in_scale_hbm, in_scale), (in_shift_hbm, in_shift),
             (mid_scale_hbm, mid_scale), (mid_shift_hbm, mid_shift))
    small_copies = [pltpu.make_async_copy(src, dst, s_sem.at[i]) for i, (src, dst) in enumerate(small)]
    for copy in small_copies:
        copy.start()
    for k in (2, 1):
        w_copy(0, k).start()

    part[...] = jnp.zeros_like(part)
    acc[...] = jnp.zeros_like(acc)
    raw[2] = jnp.zeros((N_FR, N_ROW, N_COL, N_CH), BF16)
    for t in (1, 0):
        x_copies[t].wait()
        for p in range(N_ROW):
            val = x_in[t, p].astype(F32)
            for half in range(2):
                add_moments(val[:, half * HALF : (half + 1) * HALF], half)
    finish_moments(0)
    pl.semaphore_wait(barrier, cp_size - 1)
    for d in range(cp_size - 1):
        st_copy(0, d).start()

    for copy in small_copies:
        copy.wait()
    for b in range(2):
        for f in range(4):
            gains[2 * b, f : f + 1, :] = in_scale[b : b + 1, :]
            shifts[2 * b, f : f + 1, :] = in_shift[b : b + 1, :]
        gains[2 * b + 1, 2:4, :] = mid_scale[b]
        shifts[2 * b + 1, 2:4, :] = mid_shift[b]
    for t in (1, 0):
        for p in range(N_ROW):
            val = x_in[t, p].astype(F32)
            for j in range(4):
                tmp[p % 2, j] = val[:, j * 128 : (j + 1) * 128]
            for j in range(4):
                for v in range(N_TILE):
                    raw[0, t, p, v * TILE : (v + 1) * TILE, j * 128 : (j + 1) * 128] = tmp[
                        p % 2, j, pl.ds(v, TILE, stride=N_TILE), :
                    ].astype(BF16)
            if p % 2:
                piece = 2 * (1 - t) + p // 2

                @pl.when(jnp.logical_not(last))
                def _():
                    halo_copy(0, 0, piece).start()
                    if piece == len(PIECES) - 1:
                        for i in range(2):
                            param_copy(i).start()

    @pl.when(first)
    def _():
        for i in range(len(PIECES)):
            own_copy(0, 0, i).start()

    def conv(c, carry):
        par = lax.rem(c, 2)
        nxt = 1 - par

        for d in range(cp_size - 1):
            st_copy(par, d).wait()
        mean, rstd = statistics(par)
        coefficients(c, mean, rstd, (3,))

        def own(t):
            return lambda p, cut: raw[par, t, p, :, cut]

        def received(t):
            return lambda p, cut: halo[par, t, p, :, cut]

        def norms(read, f, halves=(0, 1), rows=range(N_ROW)):
            return [functools.partial(norm, read, f, p, h) for h in halves for p in rows]

        def epilogues(t, rows):
            return [functools.partial(epilogue, c, par, t, p, m) for p in rows for m in range(2)]

        for thunk in norms(own(1), 3, (0,), (0, 1)):
            thunk()

        @pl.when(c == 0)
        def _():
            w_copy(0, 0).start()

        @pl.when(c < N_CONV - 1)
        def _():
            for k in (2, 1, 0):
                w_copy(c + 1, k).start()

        @pl.when(c == 1)
        def _():
            @pl.when(jnp.logical_not(first))
            def _():
                for i in range(2):
                    param_copy(i).wait_recv()
                for b in range(2):
                    gains[2 * b + 1, 0:2, :] = h_scale[b]
                    shifts[2 * b + 1, 0:2, :] = h_shift[b]

            @pl.when(first)
            def _():
                for b in range(2):
                    for f in range(2):
                        gains[2 * b + 1, f : f + 1, :] = mid_scale[b, 0:1]
                        shifts[2 * b + 1, f : f + 1, :] = mid_shift[b, 0:1]

            @pl.when(jnp.logical_not(last))
            def _():
                for i in range(2):
                    param_copy(i).wait_send()

        coefficients(c, mean, rstd, (2, 1, 0))
        w_copy(c, 2).wait()
        w_copy(c, 1).wait()
        run(par, steps_of(1, 2, (0,), size=1), norms(own(1), 3, (0,), (2, 3)) + norms(own(1), 3, (1,)), 0.9)
        run(par, steps_of(1, 2, (1,)), norms(own(0), 2))
        run(par, steps_of(1, 1))
        steps = steps_of(0, 2)
        run(par, steps[:12])
        w_copy(c, 0).wait()
        own_copy(par, par, 0).wait()
        own_copy(par, par, 1).wait()
        run(par, steps[12:], norms(received(1), 1), 0.9)
        run(par, steps_of(1, 0, dps=(1, -1)))
        for p in range(N_ROW):
            run(par, steps_of(1, 0, rows=(p, p + 1), dps=(0,)), epilogues(1, (p - 1,)) if p else ())
        steps = steps_of(0, 1)
        run(par, steps[:3], epilogues(1, (3,)))

        @pl.when(jnp.logical_and(c < N_CONV - 1, jnp.logical_not(last)))
        def _():
            halo_copy(nxt, nxt, 0).start()

        own_copy(par, par, 2).wait()
        run(par, steps[3:15], norms(received(0), 0, rows=(0, 1)), 0.9)
        own_copy(par, par, 3).wait()
        run(par, steps[15:], norms(received(0), 0, rows=(2, 3)), 0.9)
        run(par, steps_of(0, 0, dps=(1, -1)))
        for p in range(N_ROW):
            run(par, steps_of(0, 0, rows=(p, p + 1), dps=(0,)), epilogues(0, (p - 1,)) if p else ())
        for thunk in epilogues(0, (N_ROW - 1,)):
            thunk()
        finish_moments(nxt)

        @pl.when(c < N_CONV - 1)
        def _():
            for d in range(cp_size - 1):
                st_copy(nxt, d).start()

            @pl.when(jnp.logical_not(last))
            def _():
                for i in range(1, len(PIECES)):
                    halo_copy(nxt, nxt, i).start()

            @pl.when(first)
            def _():
                for i in range(len(PIECES)):
                    own_copy(nxt, nxt, i).start()

        @pl.when(jnp.logical_not(last))
        def _():
            for i in range(len(PIECES)):
                halo_copy(par, par, i).wait_send()

        return carry

    lax.fori_loop(0, N_CONV, conv, 0)


def reorder(val_ref, out_hbm, tmp, buf, sem):
    copies = []
    for t in range(N_FR):
        for p in range(N_ROW):
            for j in range(4):
                cut = slice(j * 128, (j + 1) * 128)
                for v in range(N_TILE):
                    tmp[p % 2, j, pl.ds(v, TILE, stride=N_TILE), :] = val_ref[
                        t, p, v * TILE : (v + 1) * TILE, cut
                    ].astype(F32)
                buf[t, p, :, cut] = tmp[p % 2, j].astype(BF16)
            copies.append(pltpu.make_async_copy(buf.at[t, p], out_hbm.at[t, p], sem.at[t, p]))
            copies[-1].start()
    for copy in copies:
        copy.wait()


def solution(mesh):
    cp_size = mesh.shape["cp"]

    def local_decode(latent, conv_w, conv_b, in_scale, in_shift, mid_scale, mid_shift):
        any_spec, vmem = pl.BlockSpec(memory_space=pl.ANY), pl.BlockSpec(memory_space=pltpu.VMEM)
        dma = pltpu.SemaphoreType.DMA
        frame = (N_ROW, N_COL, N_CH)
        blocks = pl.pallas_call(
            functools.partial(kernel, cp_size),
            out_shape=jax.ShapeDtypeStruct(latent.shape, BF16),
            in_specs=[any_spec] * 7,
            out_specs=vmem,
            scratch_shapes=[
                pltpu.VMEM((N_CONV, N_CH), F32),
                pltpu.VMEM((2, N_CH), F32),
                pltpu.VMEM((2, N_CH), F32),
                pltpu.VMEM((2, N_FR, N_CH), F32),
                pltpu.VMEM((2, N_FR, N_CH), F32),
                pltpu.VMEM((N_FR, *frame), BF16),
                pltpu.VMEM((3, N_FR, *frame), BF16),
                pltpu.VMEM((2, N_FR, *frame), BF16),
                pltpu.VMEM((4, N_ROW, PAD_COL, N_CH), BF16),
                pltpu.VMEM((2, 3, 9 * N_CH, N_CH), BF16),
                pltpu.VMEM((N_FR, N_ROW, 2, N_COL, HALF), F32),
                pltpu.VMEM((2, 8, N_CH), F32),
                pltpu.VMEM((2, 8, 128), F32),
                pltpu.VMEM((2, cp_size - 1, 8, 128), F32),
                pltpu.VMEM((N_CONV, 4, N_CH), F32),
                pltpu.VMEM((N_CONV, 4, N_CH), F32),
                pltpu.VMEM((2, N_FR, N_CH), F32),
                pltpu.VMEM((2, N_FR, N_CH), F32),
                pltpu.VMEM((2, 4, N_CH), F32),
                pltpu.VMEM((2, 4, N_COL, 128), F32),
                dma((N_FR,)),
                dma((5,)),
                dma((2, 3)),
                dma((2, cp_size - 1)),
                dma((2, cp_size - 1)),
                dma((2, len(PIECES))),
                dma((2, len(PIECES))),
                dma((2,)),
                dma((2,)),
            ],
            compiler_params=pltpu.CompilerParams(
                collective_id=0, has_side_effects=True, vmem_limit_bytes=46 * 1024 * 1024
            ),
        )(*[
            pltpu.with_memory_space_constraint(arg, pltpu.HBM)
            for arg in (
                latent, conv_w.reshape(N_CONV, 3, 9 * N_CH, N_CH), conv_b, in_scale, in_shift, mid_scale, mid_shift
            )
        ])
        return pl.pallas_call(
            reorder,
            out_shape=jax.ShapeDtypeStruct(latent.shape, BF16),
            in_specs=[vmem],
            out_specs=any_spec,
            scratch_shapes=[
                pltpu.VMEM((2, 4, N_COL, 128), F32),
                pltpu.VMEM((N_FR, *frame), BF16),
                dma((N_FR, N_ROW)),
            ],
            compiler_params=pltpu.CompilerParams(vmem_limit_bytes=6 * 1024 * 1024),
        )(blocks)

    time_spec = P(("dp", "cp"))
    param_spec = P(None, ("dp", "cp"))
    return jax.shard_map(
        local_decode,
        mesh=mesh,
        in_specs=(time_spec, P(), P(), P(), P(), param_spec, param_spec),
        out_specs=time_spec,
        check_vma=False,
    )
```
